128 devices in a mesh: gx: 16 (over y, x_hi, core), gy: 8 (over z, x_lo).
Axes of the slice: x: 4 (x_hi: 2, x_lo: 2; x = x_hi * 2 + x_lo), y: 4, z: 4, core: 2. Of those that a mesh axis runs over, the one named last changes fastest.
Arguments:
- velocity: float32 [2, 640, 2048], P(None, 'gy', 'gx'), may hold values from -4 to 4
- stress: float32 [3, 640, 2048], P(None, 'gy', 'gx'), may hold values from -6 to 6
- wind: float32 [2, 640, 2048], P(None, 'gy', 'gx'), may hold values from -4 to 4
- strength: float32 [640, 2048], P('gy', 'gx'), may hold values from 0.5 to 2
- mass: float32 [640, 2048], P('gy', 'gx'), may hold values from 0.5 to 2
- land_mask: int32 [640, 2048], P('gy', 'gx'), may hold values 0 or 1
- region_mask: int32 [640, 2048], P('gy', 'gx'), may hold values 0 or 1
- observed: float32 [2, 640, 2048], P(None, 'gy', 'gx'), may hold values from -4 to 4
- start_index: int32 [1], replicated, may hold values from 0 to 112
Outputs:
- state_adjoint: float32 [5, 640, 2048], P(None, 'gy', 'gx')
- wind_direction: float32 [2, 640, 2048], P(None, 'gy', 'gx')
The draws below stay inside these ranges and needn't reach their ends.
All inputs are finite; a program needn't handle non-finite values. No bound on the sum of `land_mask` or of `region_mask` on one device may be relied on, other than what follows from the above.
Results may differ from the reference program's by a relative error of at most 0.00002.
Values sent between devices are 32-bit elements; how exact they have to be, the bound alone decides.
A program may use at most 64 MiB of HBM per device.

```python
import math
import jax
import jax.numpy as jnp

STEPS = 8
SUBTOTAL = 120
NY = 640
NX = 2048


def with_ends(result, rng, low, high):
    longest = result.shape.index(max(result.shape))
    spots = []
    for shift in (0, 1):
        where = [jax.random.randint(jax.random.fold_in(rng, axis), (), 0, length) for axis, length in enumerate(result.shape)]
        where[longest] = (where[longest] + shift) % result.shape[longest]
        spots.append(tuple(where))
    return result.at[spots[0]].set(low).at[spots[1]].set(high)


def block_scale(stream_key, extent, pieces, least, top_value):
    gain = 1.0
    for dim, shards_of in pieces:
        heights = jax.random.uniform(jax.random.fold_in(jax.random.fold_in(stream_key, 6), dim), (shards_of,), jnp.float32, least / len(pieces), top_value / len(pieces))
        gain = gain * jnp.repeat(jnp.exp(heights), extent[dim] // shards_of).reshape((-1,) + (1,) * (len(extent) - 1 - dim))
    return gain


def noise(rng, extent, deviation, limit, cuts=(), kind=jnp.bfloat16):
    drawn = deviation * jax.random.normal(rng, extent, jnp.float32)
    if cuts:
        drawn = drawn * block_scale(rng, extent, cuts, -0.22, 0.18)
    return jnp.clip(drawn, -limit, limit).astype(kind)


def setup_inputs(seed: int = 0) -> dict:
    keys = jax.random.split(jax.random.key(seed), 10)
    velocity = noise(keys[0], (2, NY, NX), 0.5, 4.0, ((1, 8), (2, 16)), jnp.float32)
    stress = noise(keys[1], (3, NY, NX), 1.0, 6.0, ((1, 8), (2, 16)), jnp.float32)
    wind = noise(keys[2], (2, NY, NX), 0.5, 4.0, ((1, 8), (2, 16)), jnp.float32)
    strength = jnp.clip(jnp.exp(math.log(2.0) - 1.3862944 * jax.random.uniform(keys[3], (NY, NX), jnp.float32) ** block_scale(keys[3], (NY, NX), ((0, 8), (1, 16)), -0.2, 0.2)), 0.5, 2.0)
    mass = jnp.clip(jnp.exp(math.log(2.0) - 1.3862944 * jax.random.uniform(keys[4], (NY, NX), jnp.float32) ** block_scale(keys[4], (NY, NX), ((0, 8), (1, 16)), -0.2, 0.2)), 0.5, 2.0)
    land_mask = with_ends((jax.random.randint(keys[5], (NY, NX), 0, 10) < 9).astype(jnp.int32), jax.random.fold_in(keys[5], 1), 0, 1)
    region_mask = with_ends((jax.random.randint(keys[6], (NY, NX), 0, 2) < 1).astype(jnp.int32), jax.random.fold_in(keys[6], 1), 0, 1)
    observed = noise(keys[7], (2, NY, NX), 0.5, 4.0, ((1, 8), (2, 16)), jnp.float32)
    start_index = jax.random.randint(keys[8], (1,), 0, SUBTOTAL - STEPS + 1).astype(jnp.int32)
    return dict(velocity=velocity, stress=stress, wind=wind, strength=strength, mass=mass, land_mask=land_mask, region_mask=region_mask, observed=observed, start_index=start_index)


ellipse_sq = 4.0
delta_floor = 0.04
time_step = 0.5
drag_rate = 1.0
norm_eps = 1e-06

def extend(field, signs):
    north = signs[:, None] * field[:, -1, ::-1]
    zero = jnp.zeros_like(field[:, :1, :])
    rows = jnp.concatenate([zero, field, north[:, None, :]], axis=1)
    return jnp.concatenate([rows[:, :, -1:], rows, rows[:, :, :1]], axis=2)

def centred_x(field):
    return 0.5 * (field[1:-1, 2:] - field[1:-1, :-2])

def centred_y(field):
    return 0.5 * (field[2:, 1:-1] - field[:-2, 1:-1])

def stress_update(vel_pad, stress, strength, coef):
    east = vel_pad[0]
    north = vel_pad[1]
    dudx = centred_x(east)
    dudy = centred_y(east)
    dvdx = centred_x(north)
    dvdy = centred_y(north)
    diverge = dudx + dvdy
    tension = dudx - dvdy
    shearing = dudy + dvdx
    delta = jnp.sqrt(diverge * diverge + (tension * tension + shearing * shearing) / ellipse_sq + delta_floor)
    ratio = coef * strength / delta
    denom = 1.0 + coef
    first = (stress[0] + ratio * diverge - coef * strength) / denom
    second = (stress[1] + ratio * tension / ellipse_sq) / denom
    third = (stress[2] + ratio * shearing / ellipse_sq) / denom
    return jnp.stack([first, second, third], axis=0)

def velocity_update(stress_pad, velocity, wind, mass, land):
    first = stress_pad[0]
    second = stress_pad[1]
    third = stress_pad[2]
    force_x = 0.5 * centred_x(first + second) + centred_y(third)
    force_y = 0.5 * centred_y(first - second) + centred_x(third)
    scaled = land / (mass + time_step * drag_rate)
    east = scaled * (mass * velocity[0] + time_step * (force_x + wind[0]))
    north = scaled * (mass * velocity[1] + time_step * (force_y + wind[1]))
    return jnp.stack([east, north], axis=0)

def coefficient(start_index, step):
    return 0.2 + 0.8 * (start_index[0].astype(jnp.float32) + (step + 1)) / SUBTOTAL

def reference(velocity, stress, wind, strength, mass, land_mask, region_mask, observed, start_index):
    land = land_mask.astype(jnp.float32)
    region = region_mask.astype(jnp.float32)
    vel_signs = jnp.array([-1.0, -1.0], dtype=jnp.float32)
    stress_signs = jnp.array([1.0, 1.0, 1.0], dtype=jnp.float32)

    def subcycle(vel, sts, forcing, coef):
        sts = stress_update(extend(vel, vel_signs), sts, strength, coef)
        vel = velocity_update(extend(sts, stress_signs), vel, forcing, mass, land)
        return (vel, sts)
    stepper = jax.checkpoint(subcycle)

    def forward(vel, sts, forcing):
        for step in range(STEPS):
            vel, sts = stepper(vel, sts, forcing, coefficient(start_index, step))
        return vel
    final, pullback = jax.vjp(forward, velocity, stress, wind)
    vel_bar, stress_bar, wind_bar = pullback(region * (final - observed))
    state_adjoint = jnp.concatenate([vel_bar, stress_bar], axis=0)
    spread = jnp.sqrt(jnp.mean(wind_bar * wind_bar) + norm_eps)
    return (state_adjoint, wind_bar / spread)
```

```python
import functools

import jax
import jax.numpy as jnp
from jax import lax
from jax.experimental import pallas as pl
from jax.experimental.pallas import tpu as pltpu
from jax.sharding import PartitionSpec as P

STEPS = 8
SUBTOTAL = 120
HALO = 2 * STEPS
LANES = 128
PAD = 8
CHUNK = 16
NORM_EPS = 1e-06
F32 = jnp.float32
MESH = pl.DeviceIdType.MESH

ROWS = 80
NORTH = slice(80, 96)
GAP = slice(96, 112)
SOUTH = slice(112, 128)
FIRST = PAD + HALO
LAST = FIRST + LANES
TALL = LAST + HALO + PAD
SIGNS = (-1.0, -1.0, 1.0, 1.0, 1.0, -1.0, -1.0, 1.0, 1.0)

N, S, E, W, NE, NW, SE, SW = range(8)


def flip_lanes(x, index):
    return jnp.take_along_axis(x, index, axis=1)


def flip_strip(strip, lane_index, sign):
    row_index = 7 - lax.broadcasted_iota(jnp.int32, (8, LANES), 0)
    upper = jnp.take_along_axis(strip[8:16], row_index, axis=0)
    lower = jnp.take_along_axis(strip[0:8], row_index, axis=0)
    upper = flip_lanes(upper, lane_index)
    lower = flip_lanes(lower, lane_index)
    return sign * upper, sign * lower


def kernel(
    nx,
    ny,
    start_ref,
    velocity,
    stress,
    wind,
    strength,
    mass,
    land,
    region,
    observed,
    state_out,
    wind_out,
    raw,
    mass_v,
    land_v,
    region_v,
    target,
    pack_e,
    pack_w,
    got_e,
    got_w,
    rev_n,
    rev_e,
    rev_w,
    field,
    static,
    saved,
    back,
    fin,
    fin_e,
    fin_w,
    got_n_f,
    got_s_f,
    got_e_f,
    got_w_f,
    got_c_f,
    red_x,
    red_y,
    load_sem,
    send_sem,
    recv_sem,
    fsend_sem,
    frecv_sem,
    self_sem,
    xs_sem,
    xr_sem,
    ys_sem,
    yr_sem,
):
    gx = lax.axis_index("gx")
    gy = lax.axis_index("gy")
    top = gy == ny - 1
    bottom = gy == 0
    not_top = gy < ny - 1
    not_bottom = gy > 0
    east = lax.rem(gx + 1, nx)
    west = lax.rem(gx + nx - 1, nx)
    fold = nx - 1 - gx
    fold_e = lax.rem(2 * nx - 2 - gx, nx)
    fold_w = lax.rem(nx - gx, nx)

    def at(x, y):
        return {"gx": x, "gy": y}

    barrier = pltpu.get_barrier_semaphore()
    for d in range(1, nx):
        pl.semaphore_signal(
            barrier, inc=1, device_id=at(lax.rem(gx + d, nx), gy), device_id_type=MESH
        )
    for d in range(1, ny):
        pl.semaphore_signal(
            barrier, inc=1, device_id=at(gx, lax.rem(gy + d, ny)), device_id_type=MESH
        )

    @pl.when(not_top)
    def _():
        for x in (east, west):
            pl.semaphore_signal(barrier, inc=1, device_id=at(x, gy + 1), device_id_type=MESH)

    @pl.when(not_bottom)
    def _():
        for x in (east, west):
            pl.semaphore_signal(barrier, inc=1, device_id=at(x, gy - 1), device_id_type=MESH)

    loads = [
        pltpu.make_async_copy(velocity, raw.at[0:2, 0:ROWS], load_sem.at[0]),
        pltpu.make_async_copy(stress, raw.at[2:5, 0:ROWS], load_sem.at[1]),
        pltpu.make_async_copy(wind, raw.at[5:7, 0:ROWS], load_sem.at[2]),
        pltpu.make_async_copy(strength, raw.at[7, 0:ROWS], load_sem.at[3]),
        pltpu.make_async_copy(mass, mass_v, load_sem.at[4]),
        pltpu.make_async_copy(land, land_v, load_sem.at[5]),
        pltpu.make_async_copy(region, region_v, load_sem.at[6]),
        pltpu.make_async_copy(observed, target.at[1:3, 0:ROWS], load_sem.at[7]),
    ]
    for copy in loads:
        copy.start()

    zero_gap = jnp.zeros((HALO, LANES), F32)
    for f in range(9):
        raw[f, GAP] = zero_gap
    for i in range(2):
        got_e[i, GAP] = zero_gap
        got_w[i, GAP] = zero_gap
    for f in range(3):
        target[f, ROWS:LANES] = jnp.zeros((LANES - ROWS, LANES), F32)
    zero_pad = jnp.zeros((PAD, LANES), F32)
    for f in range(5):
        field[f, 0:PAD] = zero_pad
        field[f, TALL - PAD : TALL] = zero_pad
    for f in range(12):
        back[f, 0:PAD] = zero_pad
        back[f, TALL - PAD : TALL] = zero_pad

    @pl.when(bottom)
    def _():
        for f in range(9):
            raw[f, SOUTH] = zero_gap
        for i in range(2):
            got_e[i, SOUTH] = zero_gap
            got_w[i, SOUTH] = zero_gap
        for f in range(7):
            got_s_f[f] = zero_gap
        got_c_f[2] = zero_gap
        got_c_f[3] = zero_gap

    for copy in loads:
        copy.wait()

    lane = lax.broadcasted_iota(jnp.int32, (ROWS, LANES), 1)
    raw[8, 0:ROWS] = land_v[...].astype(F32) * (0.5 / (mass_v[...] + 0.5))
    target[0, 0:ROWS] = region_v[...].astype(F32)
    packed_e = jnp.zeros((ROWS, LANES), F32)
    packed_w = jnp.zeros((ROWS, LANES), F32)
    for f in range(8):
        here = (lane >= HALO * f) & (lane < HALO * (f + 1))
        value = raw[f, 0:ROWS]
        packed_e = jnp.where(here, pltpu.roll(value, (HALO * f + HALO) % LANES, 1), packed_e)
        packed_w = jnp.where(here, value if f == 0 else pltpu.roll(value, HALO * f, 1), packed_w)
    pack_e[0] = packed_e
    pack_w[0] = packed_w
    pack_e[1] = pltpu.roll(raw[8, 0:ROWS], HALO, 1)
    pack_w[1] = raw[8, 0:ROWS]

    lane8 = lax.broadcasted_iota(jnp.int32, (8, LANES), 1)
    whole_flip = LANES - 1 - lane8
    group_flip = lane8 + (HALO - 1) - 2 * lax.rem(lane8, HALO)
    group = lane8 // HALO
    group_sign = jnp.where((group < 2) | ((group >= 5) & (group < 7)), -1.0, 1.0)

    @pl.when(top)
    def _():
        for f in range(9):
            rev_n[f, 0:8], rev_n[f, 8:16] = flip_strip(raw[f, 64:80], whole_flip, SIGNS[f])
        for src, dst in ((pack_e, rev_e), (pack_w, rev_w)):
            for i, sign in ((0, group_sign), (1, 1.0)):
                dst[i, 0:8], dst[i, 8:16] = flip_strip(src[i, 64:80], group_flip, sign)

    def remote(src, dst, send, recv, slot, x, y):
        return pltpu.make_async_remote_copy(
            src_ref=src,
            dst_ref=dst,
            send_sem=send.at[slot],
            recv_sem=recv.at[slot],
            device_id=at(x, y),
            device_id_type=MESH,
        )

    def exchange(send, recv, ns, e, w, corners, folded, slots):
        to_n, to_s = ns
        corner = {
            SW: (corners[0], east, gy + 1),
            SE: (corners[1], west, gy + 1),
            NW: (corners[2], east, gy - 1),
            NE: (corners[3], west, gy - 1),
        }

        def side_copies():
            return [
                remote(e, slots[W], send, recv, W, east, gy),
                remote(w, slots[E], send, recv, E, west, gy),
            ]

        def north_copies():
            return [
                remote(to_n, slots[S], send, recv, S, gx, gy + 1),
                *[remote(corner[k][0], slots[k], send, recv, k, *corner[k][1:]) for k in (SW, SE)],
            ]

        def south_copies():
            return [
                remote(to_s, slots[N], send, recv, N, gx, gy - 1),
                *[remote(corner[k][0], slots[k], send, recv, k, *corner[k][1:]) for k in (NW, NE)],
            ]

        def fold_copy(k, src, slot, x):
            return pltpu.make_async_remote_copy(
                src_ref=src,
                dst_ref=slots[slot],
                send_sem=send.at[k],
                recv_sem=recv.at[slot],
                device_id=at(x, gy),
                device_id_type=MESH,
            )

        def local_copy(i, src, slot):
            return pltpu.make_async_copy(src, slots[slot], self_sem.at[i])

        fold_n = lambda: fold_copy(S, folded[0], N, fold)
        fold_ne = lambda: fold_copy(SW, folded[1], NE, fold_e)
        fold_nw = lambda: fold_copy(SE, folded[2], NW, fold_w)
        self_ne = lambda: local_copy(0, folded[1], NE)
        self_nw = lambda: local_copy(1, folded[2], NW)

        @pl.when(not_top)
        def _():
            for copy in north_copies():
                copy.start()

        @pl.when(top)
        def _():
            fold_n().start()

        @pl.when(top & (fold_e != gx))
        def _():
            fold_ne().start()

        @pl.when(top & (fold_e == gx))
        def _():
            self_ne().start()

        @pl.when(top & (fold_w != gx))
        def _():
            fold_nw().start()

        @pl.when(top & (fold_w == gx))
        def _():
            self_nw().start()

        @pl.when(not_bottom)
        def _():
            for copy in south_copies():
                copy.start()

        for copy in side_copies():
            copy.start()

        def finish_recv():
            for copy in side_copies():
                copy.wait_recv()

            @pl.when(not_bottom)
            def _():
                for copy in north_copies():
                    copy.wait_recv()

            @pl.when(not_top)
            def _():
                for copy in south_copies():
                    copy.wait_recv()

            @pl.when(top)
            def _():
                fold_n().wait_recv()

            @pl.when(top & (fold_e != gx))
            def _():
                fold_ne().wait_recv()

            @pl.when(top & (fold_e == gx))
            def _():
                self_ne().wait()

            @pl.when(top & (fold_w != gx))
            def _():
                fold_nw().wait_recv()

            @pl.when(top & (fold_w == gx))
            def _():
                self_nw().wait()

        def finish_send():
            for copy in side_copies():
                copy.wait_send()

            @pl.when(not_top)
            def _():
                for copy in north_copies():
                    copy.wait_send()

            @pl.when(not_bottom)
            def _():
                for copy in south_copies():
                    copy.wait_send()

            @pl.when(top)
            def _():
                fold_n().wait_send()

            @pl.when(top & (fold_e != gx))
            def _():
                fold_ne().wait_send()

            @pl.when(top & (fold_w != gx))
            def _():
                fold_nw().wait_send()

        return finish_recv, finish_send

    peers = (nx - 1) + (ny - 1)
    pl.semaphore_wait(
        barrier,
        peers + 2 * not_top.astype(jnp.int32) + 2 * not_bottom.astype(jnp.int32),
    )

    finish_recv, finish_send = exchange(
        send_sem,
        recv_sem,
        (raw.at[:, 64:80], raw.at[:, 0:16]),
        pack_e,
        pack_w,
        (pack_e.at[:, 64:80], pack_w.at[:, 64:80], pack_e.at[:, 0:16], pack_w.at[:, 0:16]),
        (rev_n, rev_e, rev_w),
        {
            N: raw.at[:, NORTH],
            S: raw.at[:, SOUTH],
            E: got_e.at[:, 0:ROWS],
            W: got_w.at[:, 0:ROWS],
            NE: got_e.at[:, NORTH],
            NW: got_w.at[:, NORTH],
            SE: got_e.at[:, SOUTH],
            SW: got_w.at[:, SOUTH],
        },
    )
    finish_recv()

    centre = slice(FIRST, LAST)
    low = slice(PAD, FIRST)
    high = slice(LAST, LAST + HALO)
    whole = [jnp.transpose(raw[f]) for f in range(9)]
    halo_e = jnp.transpose(got_e[0])
    halo_w = jnp.transpose(got_w[0])
    last_e = jnp.transpose(got_e[1])[0:HALO]
    last_w = jnp.transpose(got_w[1])[0:HALO]

    def place(rows, parts):
        u, v, s1, s2, s12, wu, wv, strong, b = parts
        field[0, rows] = u
        field[1, rows] = v
        field[2, rows] = s1 + s2
        field[3, rows] = s1 - s2
        field[4, rows] = 2.0 * s12
        static[0, rows] = jnp.where(b > 0.0, 1.0, 0.0) - b
        static[1, rows] = 0.25 * b
        static[2, rows] = b * wu
        static[3, rows] = b * wv
        static[4, rows] = strong

    def split(packed, last):
        return [packed[HALO * f : HALO * (f + 1)] for f in range(8)] + [last]

    place(centre, whole)
    place(low, split(halo_w, last_w))
    place(high, split(halo_e, last_e))

    begin = start_ref[0].astype(F32)

    def coefs(k):
        step = jnp.full((CHUNK, LANES), begin + (k + 1).astype(F32), F32)
        coef = 0.2 + 0.8 * step / SUBTOTAL
        keep = 1.0 / (1.0 + coef)
        return coef, keep

    to_n = lambda x: pltpu.roll(x, LANES - 1, 1)
    to_s = lambda x: pltpu.roll(x, 1, 1)
    chunks = range(PAD, TALL - PAD, CHUNK)

    def forward(k, carry):
        coef, keep = coefs(k)
        gain = coef * keep
        for r in chunks:
            rows = slice(r, r + CHUNK)
            up = slice(r + 1, r + 1 + CHUNK)
            down = slice(r - 1, r - 1 + CHUNK)
            u = field[0, rows]
            v = field[1, rows]
            x1 = field[0, up] - field[0, down]
            x2 = field[1, up] - field[1, down]
            y1 = to_n(u) - to_s(u)
            y2 = to_n(v) - to_s(v)
            div = x1 + y2
            ten = x1 - y2
            quarter = 0.25 * ten
            half = 0.5 * (y1 + x2)
            inv = lax.rsqrt(div * div + quarter * ten + half * half + 0.16)
            rate = gain * static[4, rows]
            un = (div + quarter) * inv
            vn = (div - quarter) * inv
            sn = half * inv
            saved[k, 0, rows] = un
            saved[k, 1, rows] = vn
            saved[k, 2, rows] = sn
            saved[k, 3, rows] = rate * inv
            field[2, rows] = keep * field[2, rows] + rate * (un - 1.0)
            field[3, rows] = keep * field[3, rows] + rate * (vn - 1.0)
            field[4, rows] = keep * field[4, rows] + rate * sn
        for r in chunks:
            rows = slice(r, r + CHUNK)
            up = slice(r + 1, r + 1 + CHUNK)
            down = slice(r - 1, r - 1 + CHUNK)
            m = field[3, rows]
            q = field[4, rows]
            fx = (field[2, up] - field[2, down]) + (to_n(q) - to_s(q))
            fy = (field[4, up] - field[4, down]) + (to_n(m) - to_s(m))
            field[0, rows] = static[0, rows] * field[0, rows] + (static[2, rows] + static[1, rows] * fx)
            field[1, rows] = static[0, rows] * field[1, rows] + (static[3, rows] + static[1, rows] * fy)
        return carry

    lax.fori_loop(0, STEPS, forward, 0)

    for f in range(12):
        if f not in (7, 8, 9):
            back[f, low] = jnp.zeros((HALO, LANES), F32)
            back[f, high] = jnp.zeros((HALO, LANES), F32)
    for f in (4, 5, 6, 10, 11):
        back[f, centre] = jnp.zeros((LANES, LANES), F32)
    where_cost = jnp.transpose(target[0])
    for i in range(2):
        miss = where_cost * (field[i, centre] - jnp.transpose(target[1 + i]))
        back[i, centre] = miss
        back[2 + i, centre] = static[1, centre] * miss

    def backward(i, carry):
        k = STEPS - 1 - i
        _, keep = coefs(k)
        for r in chunks:
            rows = slice(r, r + CHUNK)
            up = slice(r + 1, r + 1 + CHUNK)
            down = slice(r - 1, r - 1 + CHUNK)
            mu = back[2, rows]
            mv = back[3, rows]
            tp = back[4, rows] + (back[2, down] - back[2, up])
            tm = back[5, rows] + (to_s(mv) - to_n(mv))
            tq = back[6, rows] + ((to_s(mu) - to_n(mu)) + (back[3, down] - back[3, up]))
            un = saved[k, 0, rows]
            vn = saved[k, 1, rows]
            sn = saved[k, 2, rows]
            g = saved[k, 3, rows]
            along = tp * un + tm * vn + tq * sn
            total = tp + tm
            quarter = 0.25 * (tp - tm)
            back[7, rows] = g * ((total + quarter) - along * un)
            back[8, rows] = g * ((total - quarter) - along * vn)
            back[9, rows] = (0.5 * g) * (tq - along * sn)
            back[4, rows] = keep * tp
            back[5, rows] = keep * tm
            back[6, rows] = keep * tq
        for r in chunks:
            rows = slice(r, r + CHUNK)
            up = slice(r + 1, r + 1 + CHUNK)
            down = slice(r - 1, r - 1 + CHUNK)
            yb = back[8, rows]
            sb = back[9, rows]
            lu = back[0, rows]
            lv = back[1, rows]
            back[10, rows] = back[10, rows] + lu
            back[11, rows] = back[11, rows] + lv
            new_u = static[0, rows] * lu + ((back[7, down] - back[7, up]) + (to_s(sb) - to_n(sb)))
            new_v = static[0, rows] * lv + ((back[9, down] - back[9, up]) + (to_s(yb) - to_n(yb)))
            back[0, rows] = new_u
            back[1, rows] = new_v
            back[2, rows] = static[1, rows] * new_u
            back[3, rows] = static[1, rows] * new_v
        return carry

    lax.fori_loop(0, STEPS, backward, 0)
    finish_send()

    def result(rows):
        b = 4.0 * static[1, rows]
        p = back[4, rows]
        m = back[5, rows]
        return [
            back[0, rows],
            back[1, rows],
            p + m,
            p - m,
            2.0 * back[6, rows],
            b * back[10, rows],
            b * back[11, rows],
        ]

    for f, value in enumerate(result(centre)):
        fin[f] = jnp.transpose(value)
    spare = [jnp.zeros((HALO, LANES), F32)]
    fin_e[...] = jnp.transpose(jnp.concatenate(result(high) + spare, axis=0))
    fin_w[...] = jnp.transpose(jnp.concatenate(result(low) + spare, axis=0))

    @pl.when(top)
    def _():
        for f in range(7):
            rev_n[f, 0:8], rev_n[f, 8:16] = flip_strip(fin[f, NORTH], whole_flip, SIGNS[f])
        for src, dst in ((fin_e, rev_e), (fin_w, rev_w)):
            dst[0, 0:8], dst[0, 8:16] = flip_strip(src[NORTH], group_flip, group_sign)

    finish_recv, finish_send = exchange(
        fsend_sem,
        frecv_sem,
        (fin.at[:, NORTH], fin.at[:, SOUTH]),
        fin_e.at[0:ROWS],
        fin_w.at[0:ROWS],
        (fin_e.at[NORTH], fin_w.at[NORTH], fin_e.at[SOUTH], fin_w.at[SOUTH]),
        (rev_n.at[0:7], rev_e.at[0], rev_w.at[0]),
        {
            N: got_n_f,
            S: got_s_f,
            E: got_e_f,
            W: got_w_f,
            NE: got_c_f.at[0],
            NW: got_c_f.at[1],
            SE: got_c_f.at[2],
            SW: got_c_f.at[3],
        },
    )
    finish_recv()
    got_e_f[64:80] = got_e_f[64:80] + got_c_f[0]
    got_w_f[64:80] = got_w_f[64:80] + got_c_f[1]
    got_e_f[0:16] = got_e_f[0:16] + got_c_f[2]
    got_w_f[0:16] = got_w_f[0:16] + got_c_f[3]

    def finished(f):
        packed_e = got_e_f[...]
        packed_w = got_w_f[...]
        side_e = pltpu.roll(packed_e, LANES - HALO - HALO * f, 1)
        side_w = packed_w if f == 0 else pltpu.roll(packed_w, LANES - HALO * f, 1)
        value = fin[f, 0:ROWS]
        value = value + jnp.where(lane >= LANES - HALO, side_e, 0.0)
        value = value + jnp.where(lane < HALO, side_w, 0.0)
        return jnp.concatenate(
            [value[0:16] + got_s_f[f], value[16:64], value[64:80] + got_n_f[f]], axis=0
        )

    grads = [finished(5), finished(6)]
    squares = grads[0] * grads[0] + grads[1] * grads[1]
    part = jnp.sum(squares, axis=0, keepdims=True)

    def all_sum(part, buf, send, recv, count, me, where):
        buf[me] = part

        def copies():
            return [
                pltpu.make_async_remote_copy(
                    src_ref=buf.at[me],
                    dst_ref=buf.at[me],
                    send_sem=send.at[d],
                    recv_sem=recv.at[d],
                    device_id=where(lax.rem(me + d, count)),
                    device_id_type=MESH,
                )
                for d in range(1, count)
            ]

        def arrivals():
            return [
                pltpu.make_async_remote_copy(
                    src_ref=buf.at[me],
                    dst_ref=buf.at[lax.rem(me + count - d, count)],
                    send_sem=send.at[d],
                    recv_sem=recv.at[d],
                    device_id=where(lax.rem(me + d, count)),
                    device_id_type=MESH,
                )
                for d in range(1, count)
            ]

        for copy in copies():
            copy.start()
        for copy in arrivals():
            copy.wait_recv()
        for copy in copies():
            copy.wait_send()
        return jnp.sum(buf[...], axis=0)

    part = all_sum(part, red_x, xs_sem, xr_sem, nx, gx, lambda j: at(j, gy))
    part = all_sum(part, red_y, ys_sem, yr_sem, ny, gy, lambda j: at(gx, j))
    for f in range(5):
        state_out[f] = finished(f)
    finish_send()
    total = jnp.sum(jnp.broadcast_to(part, (8, LANES)), axis=1, keepdims=True)[0:1]
    entries = 2 * ROWS * LANES * nx * ny
    inv = lax.rsqrt(total / entries + NORM_EPS)
    for i in range(2):
        wind_out[i] = grads[i] * inv


def solution(mesh):
    nx, ny = mesh.shape["gx"], mesh.shape["gy"]

    def per_device(velocity, stress, wind, strength, mass, land, region, observed, start):
        vm = lambda *shape: pltpu.VMEM(shape, F32)
        dma = pltpu.SemaphoreType.DMA
        any_spec = pl.BlockSpec(memory_space=pl.ANY)
        return pl.pallas_call(
            functools.partial(kernel, nx, ny),
            out_shape=(
                jax.ShapeDtypeStruct((5, ROWS, LANES), F32),
                jax.ShapeDtypeStruct((2, ROWS, LANES), F32),
            ),
            in_specs=[pl.BlockSpec(memory_space=pltpu.SMEM)] + [any_spec] * 8,
            out_specs=(
                pl.BlockSpec(memory_space=pltpu.VMEM),
                pl.BlockSpec(memory_space=pltpu.VMEM),
            ),
            scratch_shapes=[
                vm(9, LANES, LANES),
                vm(ROWS, LANES),
                pltpu.VMEM((ROWS, LANES), jnp.int32),
                pltpu.VMEM((ROWS, LANES), jnp.int32),
                vm(3, LANES, LANES),
                vm(2, ROWS, LANES),
                vm(2, ROWS, LANES),
                vm(2, LANES, LANES),
                vm(2, LANES, LANES),
                vm(9, HALO, LANES),
                vm(2, HALO, LANES),
                vm(2, HALO, LANES),
                vm(5, TALL, LANES),
                vm(5, TALL, LANES),
                vm(STEPS, 4, TALL, LANES),
                vm(12, TALL, LANES),
                vm(7, LANES, LANES),
                vm(LANES, LANES),
                vm(LANES, LANES),
                vm(7, HALO, LANES),
                vm(7, HALO, LANES),
                vm(ROWS, LANES),
                vm(ROWS, LANES),
                vm(4, HALO, LANES),
                vm(nx, 1, LANES),
                vm(ny, 1, LANES),
                dma((8,)),
                dma((8,)),
                dma((8,)),
                dma((8,)),
                dma((8,)),
                dma((2,)),
                dma((nx,)),
                dma((nx,)),
                dma((ny,)),
                dma((ny,)),
            ],
            compiler_params=pltpu.CompilerParams(
                collective_id=0, has_side_effects=True, vmem_limit_bytes=32 * 1024 * 1024
            ),
        )(start, velocity, stress, wind, strength, mass, land, region, observed)

    tri, two = P(None, "gy", "gx"), P("gy", "gx")
    return jax.shard_map(
        per_device,
        mesh=mesh,
        in_specs=(tri, tri, tri, two, two, two, two, tri, P()),
        out_specs=(tri, tri),
        check_vma=False,
    )
```

```python
import functools

import jax
import jax.numpy as jnp
from jax import lax
from jax.experimental import pallas as pl
from jax.experimental.pallas import tpu as pltpu
from jax.sharding import PartitionSpec as P

STEPS = 8
SUBTOTAL = 120
HALO = 2 * STEPS
LANES = 128
PAD = 8
CHUNK = 16
NORM_EPS = 1e-06
F32 = jnp.float32
MESH = pl.DeviceIdType.MESH

ROWS = 80
NORTH = slice(80, 96)
GAP = slice(96, 112)
SOUTH = slice(112, 128)
FIRST = PAD + HALO
LAST = FIRST + LANES
TALL = LAST + HALO + PAD
SIGNS = (-1.0, -1.0, 1.0, 1.0, 1.0, -1.0, -1.0, 1.0, 1.0)

N, S, E, W, NE, NW, SE, SW = range(8)


def flip_lanes(x, index):
    return jnp.take_along_axis(x, index, axis=1)


def flip_strip(strip, lane_index, sign):
    row_index = 7 - lax.broadcasted_iota(jnp.int32, (8, LANES), 0)
    upper = jnp.take_along_axis(strip[8:16], row_index, axis=0)
    lower = jnp.take_along_axis(strip[0:8], row_index, axis=0)
    upper = flip_lanes(upper, lane_index)
    lower = flip_lanes(lower, lane_index)
    return sign * upper, sign * lower


def kernel(
    nx,
    ny,
    start_ref,
    velocity,
    stress,
    wind,
    strength,
    mass,
    land,
    region,
    observed,
    state_out,
    wind_out,
    raw,
    mass_v,
    land_v,
    region_v,
    target,
    bundle_e,
    bundle_w,
    corner_out,
    got_e,
    got_w,
    got_c,
    rev_n,
    rev_c,
    field,
    static,
    saved,
    back,
    fin,
    fin_e,
    fin_w,
    got_n_f,
    got_s_f,
    got_e_f,
    got_w_f,
    got_c_f,
    gust,
    gust_ns,
    got_n_w,
    got_s_w,
    got_e_w,
    got_w_w,
    got_c_w,
    rev_n_w,
    rev_c_w,
    red_x,
    red_y,
    load_sem,
    send_sem,
    recv_sem,
    wsend_sem,
    wrecv_sem,
    fsend_sem,
    frecv_sem,
    self_sem,
    xs_sem,
    xr_sem,
    ys_sem,
    yr_sem,
):
    gx = lax.axis_index("gx")
    gy = lax.axis_index("gy")
    top = gy == ny - 1
    bottom = gy == 0
    not_top = gy < ny - 1
    not_bottom = gy > 0
    east = lax.rem(gx + 1, nx)
    west = lax.rem(gx + nx - 1, nx)
    fold = nx - 1 - gx
    fold_e = lax.rem(2 * nx - 2 - gx, nx)
    fold_w = lax.rem(nx - gx, nx)

    def at(x, y):
        return {"gx": x, "gy": y}

    cross = lax.rem(gx // 2, 2)
    near = (gx // 4) * 2 + lax.rem(gx, 2)
    far = cross * ny + gy
    nears, fars = nx // 2, 2 * ny

    def near_at(j):
        return at((j // 2) * 4 + cross * 2 + lax.rem(j, 2), gy)

    def far_at(j):
        return at(gx + 2 * (j // ny - cross), lax.rem(j, ny))

    barrier = pltpu.get_barrier_semaphore()

    def greet(where):
        pl.semaphore_signal(barrier, inc=1, device_id=where, device_id_type=MESH)

    with jax.named_scope("greet"):
        for d in range(1, fars):
            greet(far_at(lax.rem(far + d, fars)))
        for d in range(1, nears):
            greet(near_at(lax.rem(near + d, nears)))

        @pl.when(not_top)
        def _():
            for x in (east, west, gx):
                greet(at(x, gy + 1))

        @pl.when(not_bottom)
        def _():
            for x in (east, west, gx):
                greet(at(x, gy - 1))

        @pl.when(top)
        def _():
            greet(at(fold, gy))

        @pl.when(top & (fold_e != gx))
        def _():
            greet(at(fold_e, gy))

        @pl.when(top & (fold_w != gx))
        def _():
            greet(at(fold_w, gy))

        greet(at(east, gy))
        greet(at(west, gy))

    loads = [
        pltpu.make_async_copy(velocity, raw.at[0:2, 0:ROWS], load_sem.at[0]),
        pltpu.make_async_copy(stress, raw.at[2:5, 0:ROWS], load_sem.at[1]),
        pltpu.make_async_copy(wind, raw.at[5:7, 0:ROWS], load_sem.at[2]),
        pltpu.make_async_copy(strength, raw.at[7, 0:ROWS], load_sem.at[3]),
        pltpu.make_async_copy(mass, mass_v, load_sem.at[4]),
        pltpu.make_async_copy(land, land_v, load_sem.at[5]),
        pltpu.make_async_copy(region, region_v, load_sem.at[6]),
        pltpu.make_async_copy(observed, target.at[1:3, 0:ROWS], load_sem.at[7]),
    ]
    for copy in loads:
        copy.start()

    zero_gap = jnp.zeros((HALO, LANES), F32)
    for f in range(9):
        raw[f, GAP] = zero_gap
    for f in range(3):
        target[f, ROWS:LANES] = jnp.zeros((LANES - ROWS, LANES), F32)
    zero_pad = jnp.zeros((PAD, LANES), F32)
    for f in range(5):
        field[f, 0:PAD] = zero_pad
        field[f, TALL - PAD : TALL] = zero_pad
    for f in range(12):
        back[f, 0:FIRST] = jnp.zeros((FIRST, LANES), F32)
        back[f, LAST:TALL] = jnp.zeros((FIRST, LANES), F32)
    for f in (4, 5, 6, 10, 11):
        back[f, FIRST:LAST] = jnp.zeros((LANES, LANES), F32)

    @pl.when(bottom)
    def _():
        for f in range(9):
            raw[f, SOUTH] = zero_gap
        for f in range(5):
            got_s_f[f] = zero_gap
        for i in (2, 3):
            got_c[i] = jnp.zeros((2 * HALO, LANES), F32)
            got_c_f[i] = zero_gap
            got_c_w[i] = jnp.zeros((2, HALO, LANES), F32)
        got_s_w[...] = jnp.zeros((2 * HALO, LANES), F32)

    for copy in loads:
        copy.wait()

    lane = lax.broadcasted_iota(jnp.int32, (ROWS, LANES), 1)
    lane16 = lax.broadcasted_iota(jnp.int32, (HALO, LANES), 1)
    lane8 = lax.broadcasted_iota(jnp.int32, (8, LANES), 1)
    whole_flip = LANES - 1 - lane8
    group_flip = lane8 + (HALO - 1) - 2 * lax.rem(lane8, HALO)
    group = lane8 // HALO
    group_sign = jnp.where((group < 2) | ((group >= 5) & (group < 7)), -1.0, 1.0)
    spare_rows = jnp.zeros((LANES - ROWS, LANES), F32)

    with jax.named_scope("pack"):
        drag = land_v[...].astype(F32) * (0.5 / (mass_v[...] + 0.5))
        raw[8, 0:ROWS] = drag
        drag_t = jnp.transpose(jnp.concatenate([drag, spare_rows], axis=0))
        target[0, 0:ROWS] = region_v[...].astype(F32)
        packed_e = pltpu.roll(raw[0, 0:ROWS], HALO, 1)
        packed_w = raw[0, 0:ROWS]
        for f in range(1, 8):
            here = (lane >= HALO * f) & (lane < HALO * (f + 1))
            value = raw[f, 0:ROWS]
            packed_e = jnp.where(here, pltpu.roll(value, (HALO * f + HALO) % LANES, 1), packed_e)
            packed_w = jnp.where(here, pltpu.roll(value, HALO * f, 1), packed_w)
        sides = ((bundle_e, packed_e, drag_t[LANES - HALO :]), (bundle_w, packed_w, drag_t[:HALO]))
        for i, (bundle, packed, strip) in enumerate(sides):
            bundle[0:ROWS] = packed
            bundle[ROWS:] = strip
            corner_out[i, 0:HALO] = packed[64:80]
            corner_out[i, HALO:] = pltpu.roll(strip, 48, 1)
            corner_out[2 + i, 0:HALO] = packed[0:16]
            corner_out[2 + i, HALO:] = pltpu.roll(strip, 80, 1)

        @pl.when(top)
        def _():
            for f in range(9):
                rev_n[f, 0:8], rev_n[f, 8:16] = flip_strip(raw[f, 64:80], whole_flip, SIGNS[f])
            for i in range(2):
                rev_c[i, 0:8], rev_c[i, 8:16] = flip_strip(
                    corner_out[i, 0:HALO], group_flip, group_sign
                )
                upper, lower = flip_strip(corner_out[i, HALO:], whole_flip, 1.0)
                rev_c[i, 16:24] = pltpu.roll(upper, 80, 1)
                rev_c[i, 24:32] = pltpu.roll(lower, 80, 1)

    def remote(src, dst, send, recv, slot, x, y):
        return pltpu.make_async_remote_copy(
            src_ref=src,
            dst_ref=dst,
            send_sem=send.at[slot],
            recv_sem=recv.at[slot],
            device_id=at(x, y),
            device_id_type=MESH,
        )

    def exchange(turn, send, recv, ns, e, w, corners, folded, slots):
        to_n, to_s = ns
        corner = {
            SW: (corners[0], east, gy + 1),
            SE: (corners[1], west, gy + 1),
            NW: (corners[2], east, gy - 1),
            NE: (corners[3], west, gy - 1),
        }

        def side_copies():
            return [
                remote(e, slots[W], send, recv, W, east, gy),
                remote(w, slots[E], send, recv, E, west, gy),
            ]

        def corner_copy(k):
            return remote(corner[k][0], slots[k], send, recv, k, *corner[k][1:])

        def corner_copies(kinds):
            return [corner_copy(k) for k in kinds]

        def north_copy():
            return remote(to_n, slots[S], send, recv, S, gx, gy + 1)

        def south_copy():
            return remote(to_s, slots[N], send, recv, N, gx, gy - 1)

        def north_copies():
            return [*corner_copies((SW, SE)), north_copy()]

        def south_copies():
            return [*corner_copies((NW, NE)), south_copy()]

        def fold_copy(k, src, slot, x):
            return pltpu.make_async_remote_copy(
                src_ref=src,
                dst_ref=slots[slot],
                send_sem=send.at[k],
                recv_sem=recv.at[slot],
                device_id=at(x, gy),
                device_id_type=MESH,
            )

        def local_copy(i, src, slot):
            return pltpu.make_async_copy(src, slots[slot], self_sem.at[2 * turn + i])

        fold_n = lambda: fold_copy(S, folded[0], N, fold)
        fold_ne = lambda: fold_copy(SW, folded[1], NE, fold_e)
        fold_nw = lambda: fold_copy(SE, folded[2], NW, fold_w)
        self_ne = lambda: local_copy(0, folded[1], NE)
        self_nw = lambda: local_copy(1, folded[2], NW)

        @pl.when(not_top)
        def _():
            for copy in corner_copies((SW, SE)):
                copy.start()

        @pl.when(not_bottom)
        def _():
            for copy in corner_copies((NW, NE)):
                copy.start()

        @pl.when(top & (fold_e != gx))
        def _():
            fold_ne().start()

        @pl.when(top & (fold_e == gx))
        def _():
            self_ne().start()

        @pl.when(top & (fold_w != gx))
        def _():
            fold_nw().start()

        @pl.when(top & (fold_w == gx))
        def _():
            self_nw().start()

        for copy in side_copies():
            copy.start()

        @pl.when(top)
        def _():
            fold_n().start()

        @pl.when(not_top)
        def _():
            north_copy().start()

        @pl.when(not_bottom)
        def _():
            south_copy().start()

        def finish_recv():
            for copy in side_copies():
                copy.wait_recv()

            @pl.when(not_bottom)
            def _():
                for copy in north_copies():
                    copy.wait_recv()

            @pl.when(not_top)
            def _():
                for copy in south_copies():
                    copy.wait_recv()

            @pl.when(top)
            def _():
                fold_n().wait_recv()

            @pl.when(top & (fold_e != gx))
            def _():
                fold_ne().wait_recv()

            @pl.when(top & (fold_e == gx))
            def _():
                self_ne().wait()

            @pl.when(top & (fold_w != gx))
            def _():
                fold_nw().wait_recv()

            @pl.when(top & (fold_w == gx))
            def _():
                self_nw().wait()

        def finish_send():
            for copy in side_copies():
                copy.wait_send()

            @pl.when(not_top)
            def _():
                for copy in north_copies():
                    copy.wait_send()

            @pl.when(not_bottom)
            def _():
                for copy in south_copies():
                    copy.wait_send()

            @pl.when(top)
            def _():
                fold_n().wait_send()

            @pl.when(top & (fold_e != gx))
            def _():
                fold_ne().wait_send()

            @pl.when(top & (fold_w != gx))
            def _():
                fold_nw().wait_send()

        return finish_recv, finish_send

    peers = (nears - 1) + (fars - 1) + 2
    as_int = lambda flag: flag.astype(jnp.int32)
    peers = peers + 3 * as_int(not_top) + 3 * as_int(not_bottom) + as_int(top)
    peers = peers + as_int(top & (fold_e != gx)) + as_int(top & (fold_w != gx))
    with jax.named_scope("barrier"):
        pl.semaphore_wait(barrier, peers)

    finish_recv, finish_send = exchange(
        0,
        send_sem,
        recv_sem,
        (raw.at[:, 64:80], raw.at[:, 0:16]),
        bundle_e,
        bundle_w,
        tuple(corner_out.at[i] for i in range(4)),
        (rev_n, rev_c.at[0], rev_c.at[1]),
        {
            N: raw.at[:, NORTH],
            S: raw.at[:, SOUTH],
            E: got_e,
            W: got_w,
            NE: got_c.at[0],
            NW: got_c.at[1],
            SE: got_c.at[2],
            SW: got_c.at[3],
        },
    )
    with jax.named_scope("recv_first"):
        finish_recv()

    centre = slice(FIRST, LAST)
    low = slice(PAD, FIRST)
    high = slice(LAST, LAST + HALO)
    whole = [jnp.transpose(raw[f]) for f in range(9)]

    def side(bundle, upper, lower):
        packed = [bundle[0:ROWS], upper[0:HALO], zero_gap, lower[0:HALO]]
        packed = jnp.transpose(jnp.concatenate(packed, axis=0))
        strip = jnp.where(lane16 < 96, upper[HALO:], jnp.where(lane16 >= 112, lower[HALO:], 0.0))
        strip = jnp.where(lane16 < ROWS, bundle[ROWS:], strip)
        return [packed[HALO * f : HALO * (f + 1)] for f in range(8)] + [strip]

    def place(rows, parts):
        u, v, s1, s2, s12, wu, wv, strong, b = parts
        field[0, rows] = u
        field[1, rows] = v
        field[2, rows] = s1 + s2
        field[3, rows] = s1 - s2
        field[4, rows] = 2.0 * s12
        static[0, rows] = jnp.where(b > 0.0, 1.0, 0.0) - b
        static[1, rows] = 0.25 * b
        static[2, rows] = b * wu
        static[3, rows] = b * wv
        static[4, rows] = strong

    place(centre, whole)
    place(low, side(got_w, got_c.at[1], got_c.at[3]))
    place(high, side(got_e, got_c.at[0], got_c.at[2]))

    begin = start_ref[0].astype(F32)

    def coefs(k):
        step = jnp.full((CHUNK, LANES), begin + (k + 1).astype(F32), F32)
        coef = 0.2 + 0.8 * step / SUBTOTAL
        keep = 1.0 / (1.0 + coef)
        return coef, keep

    to_n = lambda x: pltpu.roll(x, LANES - 1, 1)
    to_s = lambda x: pltpu.roll(x, 1, 1)
    wide = range(PAD, TALL - PAD, CHUNK)
    narrow = range(PAD + 8, TALL - PAD - 8, CHUNK)

    def forward(chunks, k, carry):
        coef, keep = coefs(k)
        gain = coef * keep
        for r in chunks:
            rows = slice(r, r + CHUNK)
            up = slice(r + 1, r + 1 + CHUNK)
            down = slice(r - 1, r - 1 + CHUNK)
            u = field[0, rows]
            v = field[1, rows]
            x1 = field[0, up] - field[0, down]
            x2 = field[1, up] - field[1, down]
            y1 = to_n(u) - to_s(u)
            y2 = to_n(v) - to_s(v)
            div = x1 + y2
            ten = x1 - y2
            quarter = 0.25 * ten
            half = 0.5 * (y1 + x2)
            inv = lax.rsqrt(div * div + quarter * ten + half * half + 0.16)
            rate = gain * static[4, rows]
            un = (div + quarter) * inv
            vn = (div - quarter) * inv
            sn = half * inv
            saved[k, 0, rows] = un
            saved[k, 1, rows] = vn
            saved[k, 2, rows] = sn
            saved[k, 3, rows] = rate * inv
            field[2, rows] = keep * field[2, rows] + rate * (un - 1.0)
            field[3, rows] = keep * field[3, rows] + rate * (vn - 1.0)
            field[4, rows] = keep * field[4, rows] + rate * sn
        for r in chunks:
            rows = slice(r, r + CHUNK)
            up = slice(r + 1, r + 1 + CHUNK)
            down = slice(r - 1, r - 1 + CHUNK)
            m = field[3, rows]
            q = field[4, rows]
            fx = (field[2, up] - field[2, down]) + (to_n(q) - to_s(q))
            fy = (field[4, up] - field[4, down]) + (to_n(m) - to_s(m))
            field[0, rows] = static[0, rows] * field[0, rows] + (static[2, rows] + static[1, rows] * fx)
            field[1, rows] = static[0, rows] * field[1, rows] + (static[3, rows] + static[1, rows] * fy)
        return carry

    with jax.named_scope("forward"):
        lax.fori_loop(0, STEPS // 2, functools.partial(forward, wide), 0)
        lax.fori_loop(STEPS // 2, STEPS, functools.partial(forward, narrow), 0)

    where_cost = jnp.transpose(target[0])
    for i in range(2):
        miss = where_cost * (field[i, centre] - jnp.transpose(target[1 + i]))
        back[i, centre] = miss
        back[2 + i, centre] = static[1, centre] * miss

    def backward(chunks, i, carry):
        k = STEPS - 1 - i
        _, keep = coefs(k)
        for r in chunks:
            rows = slice(r, r + CHUNK)
            up = slice(r + 1, r + 1 + CHUNK)
            down = slice(r - 1, r - 1 + CHUNK)
            mu = back[2, rows]
            mv = back[3, rows]
            tp = back[4, rows] + (back[2, down] - back[2, up])
            tm = back[5, rows] + (to_s(mv) - to_n(mv))
            tq = back[6, rows] + ((to_s(mu) - to_n(mu)) + (back[3, down] - back[3, up]))
            un = saved[k, 0, rows]
            vn = saved[k, 1, rows]
            sn = saved[k, 2, rows]
            g = saved[k, 3, rows]
            along = tp * un + tm * vn + tq * sn
            total = tp + tm
            quarter = 0.25 * (tp - tm)
            back[7, rows] = g * ((total + quarter) - along * un)
            back[8, rows] = g * ((total - quarter) - along * vn)
            back[9, rows] = (0.5 * g) * (tq - along * sn)
            back[4, rows] = keep * tp
            back[5, rows] = keep * tm
            back[6, rows] = keep * tq
        for r in chunks:
            rows = slice(r, r + CHUNK)
            up = slice(r + 1, r + 1 + CHUNK)
            down = slice(r - 1, r - 1 + CHUNK)
            yb = back[8, rows]
            sb = back[9, rows]
            lu = back[0, rows]
            lv = back[1, rows]
            back[10, rows] = back[10, rows] + lu
            back[11, rows] = back[11, rows] + lv
            new_u = static[0, rows] * lu + ((back[7, down] - back[7, up]) + (to_s(sb) - to_n(sb)))
            new_v = static[0, rows] * lv + ((back[9, down] - back[9, up]) + (to_s(yb) - to_n(yb)))
            back[0, rows] = new_u
            back[1, rows] = new_v
            back[2, rows] = static[1, rows] * new_u
            back[3, rows] = static[1, rows] * new_v
        return carry

    with jax.named_scope("backward"):
        lax.fori_loop(0, STEPS // 2, functools.partial(backward, narrow), 0)
        lax.fori_loop(STEPS // 2, STEPS, functools.partial(backward, wide), 0)

    lane_all = lax.broadcasted_iota(jnp.int32, (LANES, LANES), 1)
    with jax.named_scope("wind_pack"):
        for i in range(2):
            gust[i] = 4.0 * static[1] * back[10 + i]
        here = ((lane_all >= 80) & (lane_all < 96)) | (lane_all >= 112)
        both = jnp.where(here, gust[0, centre], pltpu.roll(gust[1, centre], LANES - HALO, 1))
        gust_ns[...] = jnp.transpose(both)[64:LANES]

        @pl.when(top)
        def _():
            for i in range(2):
                part = slice(HALO * i, HALO * (i + 1))
                upper, lower = flip_strip(gust_ns[part], whole_flip, -1.0)
                rev_n_w[16 * i : 16 * i + 8] = upper
                rev_n_w[16 * i + 8 : 16 * i + 16] = lower
                for j, rows in ((0, high), (1, low)):
                    upper, lower = flip_strip(gust[i, rows], whole_flip, -1.0)
                    rev_c_w[j, i, 0:8] = pltpu.roll(upper, 80, 1)
                    rev_c_w[j, i, 8:16] = pltpu.roll(lower, 80, 1)

    finish_wind, finish_wind_send = exchange(
        1,
        wsend_sem,
        wrecv_sem,
        (gust_ns.at[0:32], gust_ns.at[32:64]),
        gust.at[:, high],
        gust.at[:, low],
        (gust.at[:, high], gust.at[:, low], gust.at[:, high], gust.at[:, low]),
        (rev_n_w, rev_c_w.at[0], rev_c_w.at[1]),
        {
            N: got_n_w,
            S: got_s_w,
            E: got_e_w,
            W: got_w_w,
            NE: got_c_w.at[0],
            NW: got_c_w.at[1],
            SE: got_c_w.at[2],
            SW: got_c_w.at[3],
        },
    )
    finish_send()

    def result(rows):
        p = back[4, rows]
        m = back[5, rows]
        return [back[0, rows], back[1, rows], p + m, p - m, 2.0 * back[6, rows]]

    with jax.named_scope("state_pack"):
        for f, value in enumerate(result(centre)):
            fin[f] = jnp.transpose(value)
        for rows, dst in ((high, fin_e), (low, fin_w)):
            dst[...] = jnp.transpose(jnp.concatenate(result(rows) + [spare_rows], axis=0))

        @pl.when(top)
        def _():
            for f in range(5):
                rev_n[f, 0:8], rev_n[f, 8:16] = flip_strip(fin[f, NORTH], whole_flip, SIGNS[f])
            for i, src in ((0, fin_e), (1, fin_w)):
                rev_c[i, 0:8], rev_c[i, 8:16] = flip_strip(src[NORTH], group_flip, group_sign)

    finish_state, finish_state_send = exchange(
        2,
        fsend_sem,
        frecv_sem,
        (fin.at[:, NORTH], fin.at[:, SOUTH]),
        fin_e.at[0:ROWS],
        fin_w.at[0:ROWS],
        (fin_e.at[NORTH], fin_w.at[NORTH], fin_e.at[SOUTH], fin_w.at[SOUTH]),
        (rev_n.at[0:5], rev_c.at[0, 0:HALO], rev_c.at[1, 0:HALO]),
        {
            N: got_n_f,
            S: got_s_f,
            E: got_e_f,
            W: got_w_f,
            NE: got_c_f.at[0],
            NW: got_c_f.at[1],
            SE: got_c_f.at[2],
            SW: got_c_f.at[3],
        },
    )
    with jax.named_scope("recv_wind"):
        finish_wind()

    def with_sides(i):
        value = gust[i, centre]

        def ends(straight, upper, lower):
            extra = jnp.where(lane16 < ROWS, straight[i], 0.0)
            upper = pltpu.roll(upper[i], 80, 1)
            extra = extra + jnp.where((lane16 >= 64) & (lane16 < ROWS), upper, 0.0)
            return extra + jnp.where(lane16 < HALO, pltpu.roll(lower[i], 48, 1), 0.0)

        at_w = ends(got_w_w, got_c_w.at[1], got_c_w.at[3])
        at_e = ends(got_e_w, got_c_w.at[0], got_c_w.at[2])
        parts = [value[:HALO] + at_w, value[HALO:-HALO], value[-HALO:] + at_e]
        value = jnp.transpose(jnp.concatenate(parts, axis=0))
        rows = slice(HALO * (1 - i), HALO * (2 - i))
        return jnp.concatenate(
            [value[0:16] + got_s_w[rows], value[16:64], value[64:80] + got_n_w[rows]], axis=0
        )

    with jax.named_scope("wind_add"):
        for i in range(2):
            wind_out[i] = with_sides(i)
        squares = wind_out[0] * wind_out[0] + wind_out[1] * wind_out[1]
        part = jnp.sum(squares, axis=0, keepdims=True)

    def all_sum(buf, send, recv, count, me, where):
        def copies():
            return [
                pltpu.make_async_remote_copy(
                    src_ref=buf.at[me],
                    dst_ref=buf.at[me],
                    send_sem=send.at[d],
                    recv_sem=recv.at[d],
                    device_id=where(lax.rem(me + d, count)),
                    device_id_type=MESH,
                )
                for d in range(1, count)
            ]

        def arrivals():
            return [
                pltpu.make_async_remote_copy(
                    src_ref=buf.at[me],
                    dst_ref=buf.at[lax.rem(me + count - d, count)],
                    send_sem=send.at[d],
                    recv_sem=recv.at[d],
                    device_id=where(lax.rem(me + d, count)),
                    device_id_type=MESH,
                )
                for d in range(1, count)
            ]

        def begin_sum(part):
            buf[me] = part
            for copy in copies():
                copy.start()

        def end_sum():
            for copy in arrivals():
                copy.wait_recv()
            for copy in copies():
                copy.wait_send()
            return jnp.sum(buf[...], axis=0)

        return begin_sum, end_sum

    begin_near, end_near = all_sum(red_x, xs_sem, xr_sem, nears, near, near_at)
    begin_far, end_far = all_sum(red_y, ys_sem, yr_sem, fars, far, far_at)
    begin_near(part)
    with jax.named_scope("recv_state"):
        finish_state()
    with jax.named_scope("state_add"):
        got_e_f[64:80] = got_e_f[64:80] + got_c_f[0]
        got_w_f[64:80] = got_w_f[64:80] + got_c_f[1]
        got_e_f[0:16] = got_e_f[0:16] + got_c_f[2]
        got_w_f[0:16] = got_w_f[0:16] + got_c_f[3]
        packed_e = got_e_f[...]
        packed_w = got_w_f[...]
        for f in range(5):
            side_e = pltpu.roll(packed_e, LANES - HALO - HALO * f, 1)
            side_w = packed_w if f == 0 else pltpu.roll(packed_w, LANES - HALO * f, 1)
            value = fin[f, 0:ROWS]
            value = value + jnp.where(lane >= LANES - HALO, side_e, 0.0)
            value = value + jnp.where(lane < HALO, side_w, 0.0)
            state_out[f] = value
            state_out[f, 0:16] = state_out[f, 0:16] + got_s_f[f]
            state_out[f, 64:80] = state_out[f, 64:80] + got_n_f[f]
    with jax.named_scope("sum_near"):
        part = end_near()
    begin_far(part)
    finish_wind_send()
    finish_state_send()
    with jax.named_scope("sum_far"):
        part = end_far()
    total = jnp.sum(jnp.broadcast_to(part, (8, LANES)), axis=1, keepdims=True)[0:1]
    entries = 2 * ROWS * LANES * nx * ny
    inv = lax.rsqrt(total / entries + NORM_EPS)
    for i in range(2):
        wind_out[i] = wind_out[i] * inv


def writer(state, wind, state_hbm, wind_hbm, sem):
    copies = [
        pltpu.make_async_copy(state, state_hbm, sem.at[0]),
        pltpu.make_async_copy(wind, wind_hbm, sem.at[1]),
    ]
    for copy in copies:
        copy.start()
    for copy in copies:
        copy.wait()


def solution(mesh):
    nx, ny = mesh.shape["gx"], mesh.shape["gy"]

    def per_device(velocity, stress, wind, strength, mass, land, region, observed, start):
        vm = lambda *shape: pltpu.VMEM(shape, F32)
        dma = pltpu.SemaphoreType.DMA
        any_spec = pl.BlockSpec(memory_space=pl.ANY)
        args = (velocity, stress, wind, strength, mass, land, region, observed)
        args = [pltpu.with_memory_space_constraint(z, pltpu.HBM) for z in args]
        shapes = (
            jax.ShapeDtypeStruct((5, ROWS, LANES), F32),
            jax.ShapeDtypeStruct((2, ROWS, LANES), F32),
        )
        vmem_spec = pl.BlockSpec(memory_space=pltpu.VMEM)
        state, gusts = pl.pallas_call(
            functools.partial(kernel, nx, ny),
            out_shape=shapes,
            in_specs=[pl.BlockSpec(memory_space=pltpu.SMEM)] + [any_spec] * 8,
            out_specs=(vmem_spec, vmem_spec),
            scratch_shapes=[
                vm(9, LANES, LANES),
                vm(ROWS, LANES),
                pltpu.VMEM((ROWS, LANES), jnp.int32),
                pltpu.VMEM((ROWS, LANES), jnp.int32),
                vm(3, LANES, LANES),
                vm(ROWS + HALO, LANES),
                vm(ROWS + HALO, LANES),
                vm(4, 2 * HALO, LANES),
                vm(ROWS + HALO, LANES),
                vm(ROWS + HALO, LANES),
                vm(4, 2 * HALO, LANES),
                vm(9, HALO, LANES),
                vm(2, 2 * HALO, LANES),
                vm(5, TALL, LANES),
                vm(5, TALL, LANES),
                vm(STEPS, 4, TALL, LANES),
                vm(12, TALL, LANES),
                vm(5, LANES, LANES),
                vm(LANES, LANES),
                vm(LANES, LANES),
                vm(5, HALO, LANES),
                vm(5, HALO, LANES),
                vm(ROWS, LANES),
                vm(ROWS, LANES),
                vm(4, HALO, LANES),
                vm(2, TALL, LANES),
                vm(64, LANES),
                vm(2 * HALO, LANES),
                vm(2 * HALO, LANES),
                vm(2, HALO, LANES),
                vm(2, HALO, LANES),
                vm(4, 2, HALO, LANES),
                vm(2 * HALO, LANES),
                vm(2, 2, HALO, LANES),
                vm(nx // 2, 1, LANES),
                vm(2 * ny, 1, LANES),
                dma((8,)),
                dma((8,)),
                dma((8,)),
                dma((8,)),
                dma((8,)),
                dma((8,)),
                dma((8,)),
                dma((6,)),
                dma((nx // 2,)),
                dma((nx // 2,)),
                dma((2 * ny,)),
                dma((2 * ny,)),
            ],
            compiler_params=pltpu.CompilerParams(
                collective_id=0, has_side_effects=True, vmem_limit_bytes=32 * 1024 * 1024
            ),
        )(start, *args)
        return pl.pallas_call(
            writer,
            out_shape=shapes,
            in_specs=[vmem_spec, vmem_spec],
            out_specs=(any_spec, any_spec),
            scratch_shapes=[dma((2,))],
        )(
            pltpu.with_memory_space_constraint(state, pltpu.VMEM),
            pltpu.with_memory_space_constraint(gusts, pltpu.VMEM),
        )

    tri, two = P(None, "gy", "gx"), P("gy", "gx")
    return jax.shard_map(
        per_device,
        mesh=mesh,
        in_specs=(tri, tri, tri, two, two, two, two, tri, P()),
        out_specs=(tri, tri),
        check_vma=False,
    )
```

```python
import functools

import jax
import jax.numpy as jnp
from jax import lax
from jax.experimental import pallas as pl
from jax.experimental.pallas import tpu as pltpu
from jax.sharding import PartitionSpec as P

STEPS = 8
SUBTOTAL = 120
HALO = 2 * STEPS
LANES = 128
PAD = 8
CHUNK = 16
NORM_EPS = 1e-06
F32 = jnp.float32
MESH = pl.DeviceIdType.MESH

ROWS = 80
NORTH = slice(80, 96)
GAP = slice(96, 112)
SOUTH = slice(112, 128)
FIRST = PAD + HALO
LAST = FIRST + LANES
TALL = LAST + HALO + PAD
SIGNS = (-1.0, -1.0, 1.0, 1.0, 1.0, -1.0, -1.0, 1.0, 1.0)

N, S, E, W, NE, NW, SE, SW = range(8)


def flip_lanes(x, index):
    return jnp.take_along_axis(x, index, axis=1)


def flip_strip(strip, lane_index, sign):
    row_index = 7 - lax.broadcasted_iota(jnp.int32, (8, LANES), 0)
    upper = jnp.take_along_axis(strip[8:16], row_index, axis=0)
    lower = jnp.take_along_axis(strip[0:8], row_index, axis=0)
    upper = flip_lanes(upper, lane_index)
    lower = flip_lanes(lower, lane_index)
    return sign * upper, sign * lower


def kernel(
    nx,
    ny,
    start_ref,
    velocity,
    stress,
    wind,
    strength,
    mass,
    land,
    region,
    observed,
    state_out,
    wind_out,
    raw,
    mass_v,
    land_v,
    region_v,
    target,
    bundle_e,
    bundle_w,
    corner_out,
    got_e,
    got_w,
    got_c,
    rev_n,
    rev_c,
    field,
    static,
    saved,
    back,
    fin,
    fin_e,
    fin_w,
    got_n_f,
    got_s_f,
    got_e_f,
    got_w_f,
    got_c_f,
    gust,
    gust_ns,
    got_n_w,
    got_s_w,
    got_e_w,
    got_w_w,
    got_c_w,
    rev_n_w,
    rev_c_w,
    red_x,
    red_y,
    load_sem,
    send_sem,
    recv_sem,
    wsend_sem,
    wrecv_sem,
    fsend_sem,
    frecv_sem,
    self_sem,
    xs_sem,
    xr_sem,
    ys_sem,
    yr_sem,
):
    gx = lax.axis_index("gx")
    gy = lax.axis_index("gy")
    top = gy == ny - 1
    bottom = gy == 0
    not_top = gy < ny - 1
    not_bottom = gy > 0
    def wrap(index, count):
        return jnp.where(index >= count, index - count, index)

    east = wrap(gx + 1, nx)
    west = wrap(gx + nx - 1, nx)
    fold = nx - 1 - gx
    fold_e = wrap(2 * nx - 2 - gx, nx)
    fold_w = wrap(nx - gx, nx)

    def at(x, y):
        return {"gx": x, "gy": y}

    loads = [
        pltpu.make_async_copy(velocity, raw.at[0:2, 0:ROWS], load_sem.at[0]),
        pltpu.make_async_copy(stress, raw.at[2:5, 0:ROWS], load_sem.at[1]),
        pltpu.make_async_copy(wind, raw.at[5:7, 0:ROWS], load_sem.at[2]),
        pltpu.make_async_copy(strength, raw.at[7, 0:ROWS], load_sem.at[3]),
        pltpu.make_async_copy(mass, mass_v, load_sem.at[4]),
        pltpu.make_async_copy(land, land_v, load_sem.at[5]),
        pltpu.make_async_copy(region, region_v, load_sem.at[6]),
        pltpu.make_async_copy(observed, target.at[1:3, 0:ROWS], load_sem.at[7]),
    ]
    for copy in loads:
        copy.start()

    ring = lax.div(gx, 4)
    core = lax.rem(gx, 2)
    cross = lax.div(gx - 4 * ring - core, 2)
    rings = nx // 4
    near = ring * 2 + core
    far = cross * ny + gy
    nears, fars = 2 * rings, 2 * ny

    def near_at(d, sign=1):
        r = wrap(ring + (d // 2 if sign > 0 else rings - d // 2), rings) if d // 2 else ring
        c = 1 - core if d % 2 else core
        return r * 2 + c, at(r * 4 + cross * 2 + c, gy)

    def far_at(d, sign=1):
        y = wrap(gy + (d // 2 if sign > 0 else ny - d // 2), ny) if d // 2 else gy
        x = 1 - cross if d % 2 else cross
        return x * ny + y, at(gx + 2 * (x - cross), y)

    barrier = pltpu.get_barrier_semaphore()

    def greet(where):
        pl.semaphore_signal(barrier, inc=1, device_id=where, device_id_type=MESH)

    with jax.named_scope("greet"):
        greet(at(east, gy))
        greet(at(west, gy))

        @pl.when(not_top)
        def _():
            for x in (gx, east, west):
                greet(at(x, gy + 1))

        @pl.when(not_bottom)
        def _():
            for x in (gx, east, west):
                greet(at(x, gy - 1))

        @pl.when(top)
        def _():
            greet(at(fold, gy))

        @pl.when(top & (fold_e != gx))
        def _():
            greet(at(fold_e, gy))

        @pl.when(top & (fold_w != gx))
        def _():
            greet(at(fold_w, gy))

        for d in range(1, fars):
            greet(far_at(d)[1])
        for d in range(1, nears):
            greet(near_at(d)[1])

    zero_gap = jnp.zeros((HALO, LANES), F32)
    for f in range(9):
        raw[f, GAP] = zero_gap
    for f in range(3):
        target[f, ROWS:LANES] = jnp.zeros((LANES - ROWS, LANES), F32)
    zero_pad = jnp.zeros((PAD, LANES), F32)
    for f in range(5):
        field[f, 0:PAD] = zero_pad
        field[f, TALL - PAD : TALL] = zero_pad
    for f in range(12):
        back[f, 0:FIRST] = jnp.zeros((FIRST, LANES), F32)
        back[f, LAST:TALL] = jnp.zeros((FIRST, LANES), F32)
    for f in (4, 5, 6, 10, 11):
        back[f, FIRST:LAST] = jnp.zeros((LANES, LANES), F32)

    @pl.when(bottom)
    def _():
        for f in range(9):
            raw[f, SOUTH] = zero_gap
        for f in range(5):
            got_s_f[f] = zero_gap
        for i in (2, 3):
            got_c[i] = jnp.zeros((2 * HALO, LANES), F32)
            got_c_f[i] = zero_gap
            got_c_w[i] = jnp.zeros((2, HALO, LANES), F32)
        got_s_w[...] = jnp.zeros((2 * HALO, LANES), F32)

    for copy in loads:
        copy.wait()

    lane = lax.broadcasted_iota(jnp.int32, (ROWS, LANES), 1)
    lane16 = lax.broadcasted_iota(jnp.int32, (HALO, LANES), 1)
    lane8 = lax.broadcasted_iota(jnp.int32, (8, LANES), 1)
    whole_flip = LANES - 1 - lane8
    group_flip = lane8 + (HALO - 1) - 2 * lax.rem(lane8, HALO)
    group = lane8 // HALO
    group_sign = jnp.where((group < 2) | ((group >= 5) & (group < 7)), -1.0, 1.0)
    spare_rows = jnp.zeros((LANES - ROWS, LANES), F32)

    with jax.named_scope("pack"):
        drag = land_v[...].astype(F32) * (0.5 / (mass_v[...] + 0.5))
        raw[8, 0:ROWS] = drag
        drag_t = jnp.transpose(jnp.concatenate([drag, spare_rows], axis=0))
        target[0, 0:ROWS] = region_v[...].astype(F32)
        packed_e = pltpu.roll(raw[0, 0:ROWS], HALO, 1)
        packed_w = raw[0, 0:ROWS]
        for f in range(1, 8):
            here = (lane >= HALO * f) & (lane < HALO * (f + 1))
            value = raw[f, 0:ROWS]
            packed_e = jnp.where(here, pltpu.roll(value, (HALO * f + HALO) % LANES, 1), packed_e)
            packed_w = jnp.where(here, pltpu.roll(value, HALO * f, 1), packed_w)
        sides = ((bundle_e, packed_e, drag_t[LANES - HALO :]), (bundle_w, packed_w, drag_t[:HALO]))
        for i, (bundle, packed, strip) in enumerate(sides):
            bundle[0:ROWS] = packed
            bundle[ROWS:] = strip
            corner_out[i, 0:HALO] = packed[64:80]
            corner_out[i, HALO:] = pltpu.roll(strip, 48, 1)
            corner_out[2 + i, 0:HALO] = packed[0:16]
            corner_out[2 + i, HALO:] = pltpu.roll(strip, 80, 1)

        @pl.when(top)
        def _():
            for f in range(9):
                rev_n[f, 0:8], rev_n[f, 8:16] = flip_strip(raw[f, 64:80], whole_flip, SIGNS[f])
            for i in range(2):
                rev_c[i, 0:8], rev_c[i, 8:16] = flip_strip(
                    corner_out[i, 0:HALO], group_flip, group_sign
                )
                upper, lower = flip_strip(corner_out[i, HALO:], whole_flip, 1.0)
                rev_c[i, 16:24] = pltpu.roll(upper, 80, 1)
                rev_c[i, 24:32] = pltpu.roll(lower, 80, 1)

    def remote(src, dst, send, recv, slot, x, y):
        return pltpu.make_async_remote_copy(
            src_ref=src,
            dst_ref=dst,
            send_sem=send.at[slot],
            recv_sem=recv.at[slot],
            device_id=at(x, y),
            device_id_type=MESH,
        )

    def exchange(turn, send, recv, ns, e, w, corners, folded, slots):
        to_n, to_s = ns
        corner = {
            SW: (corners[0], east, gy + 1),
            SE: (corners[1], west, gy + 1),
            NW: (corners[2], east, gy - 1),
            NE: (corners[3], west, gy - 1),
        }

        def side_copies():
            return [
                remote(e, slots[W], send, recv, W, east, gy),
                remote(w, slots[E], send, recv, E, west, gy),
            ]

        def corner_copy(k):
            return remote(corner[k][0], slots[k], send, recv, k, *corner[k][1:])

        def corner_copies(kinds):
            return [corner_copy(k) for k in kinds]

        def north_copy():
            return remote(to_n, slots[S], send, recv, S, gx, gy + 1)

        def south_copy():
            return remote(to_s, slots[N], send, recv, N, gx, gy - 1)

        def north_copies():
            return [*corner_copies((SW, SE)), north_copy()]

        def south_copies():
            return [*corner_copies((NW, NE)), south_copy()]

        def fold_copy(k, src, slot, x):
            return pltpu.make_async_remote_copy(
                src_ref=src,
                dst_ref=slots[slot],
                send_sem=send.at[k],
                recv_sem=recv.at[slot],
                device_id=at(x, gy),
                device_id_type=MESH,
            )

        def local_copy(i, src, slot):
            return pltpu.make_async_copy(src, slots[slot], self_sem.at[2 * turn + i])

        fold_n = lambda: fold_copy(S, folded[0], N, fold)
        fold_ne = lambda: fold_copy(SW, folded[1], NE, fold_e)
        fold_nw = lambda: fold_copy(SE, folded[2], NW, fold_w)
        self_ne = lambda: local_copy(0, folded[1], NE)
        self_nw = lambda: local_copy(1, folded[2], NW)

        @pl.when(not_top)
        def _():
            for copy in corner_copies((SW, SE)):
                copy.start()

        @pl.when(not_bottom)
        def _():
            for copy in corner_copies((NW, NE)):
                copy.start()

        @pl.when(top & (fold_e != gx))
        def _():
            fold_ne().start()

        @pl.when(top & (fold_e == gx))
        def _():
            self_ne().start()

        @pl.when(top & (fold_w != gx))
        def _():
            fold_nw().start()

        @pl.when(top & (fold_w == gx))
        def _():
            self_nw().start()

        for copy in side_copies():
            copy.start()

        @pl.when(top)
        def _():
            fold_n().start()

        @pl.when(not_top)
        def _():
            north_copy().start()

        @pl.when(not_bottom)
        def _():
            south_copy().start()

        def finish_recv():
            for copy in side_copies():
                copy.wait_recv()

            @pl.when(not_bottom)
            def _():
                for copy in north_copies():
                    copy.wait_recv()

            @pl.when(not_top)
            def _():
                for copy in south_copies():
                    copy.wait_recv()

            @pl.when(top)
            def _():
                fold_n().wait_recv()

            @pl.when(top & (fold_e != gx))
            def _():
                fold_ne().wait_recv()

            @pl.when(top & (fold_e == gx))
            def _():
                self_ne().wait()

            @pl.when(top & (fold_w != gx))
            def _():
                fold_nw().wait_recv()

            @pl.when(top & (fold_w == gx))
            def _():
                self_nw().wait()

        def finish_send():
            for copy in side_copies():
                copy.wait_send()

            @pl.when(not_top)
            def _():
                for copy in north_copies():
                    copy.wait_send()

            @pl.when(not_bottom)
            def _():
                for copy in south_copies():
                    copy.wait_send()

            @pl.when(top)
            def _():
                fold_n().wait_send()

            @pl.when(top & (fold_e != gx))
            def _():
                fold_ne().wait_send()

            @pl.when(top & (fold_w != gx))
            def _():
                fold_nw().wait_send()

        return finish_recv, finish_send

    peers = (nears - 1) + (fars - 1) + 2
    as_int = lambda flag: flag.astype(jnp.int32)
    peers = peers + 3 * as_int(not_top) + 3 * as_int(not_bottom) + as_int(top)
    peers = peers + as_int(top & (fold_e != gx)) + as_int(top & (fold_w != gx))
    with jax.named_scope("barrier"):
        pl.semaphore_wait(barrier, peers)

    finish_recv, finish_send = exchange(
        0,
        send_sem,
        recv_sem,
        (raw.at[:, 64:80], raw.at[:, 0:16]),
        bundle_e,
        bundle_w,
        tuple(corner_out.at[i] for i in range(4)),
        (rev_n, rev_c.at[0], rev_c.at[1]),
        {
            N: raw.at[:, NORTH],
            S: raw.at[:, SOUTH],
            E: got_e,
            W: got_w,
            NE: got_c.at[0],
            NW: got_c.at[1],
            SE: got_c.at[2],
            SW: got_c.at[3],
        },
    )
    with jax.named_scope("recv_first"):
        finish_recv()

    centre = slice(FIRST, LAST)
    low = slice(PAD, FIRST)
    high = slice(LAST, LAST + HALO)
    whole = [jnp.transpose(raw[f]) for f in range(9)]

    def side(bundle, upper, lower):
        packed = [bundle[0:ROWS], upper[0:HALO], zero_gap, lower[0:HALO]]
        packed = jnp.transpose(jnp.concatenate(packed, axis=0))
        strip = jnp.where(lane16 < 96, upper[HALO:], jnp.where(lane16 >= 112, lower[HALO:], 0.0))
        strip = jnp.where(lane16 < ROWS, bundle[ROWS:], strip)
        return [packed[HALO * f : HALO * (f + 1)] for f in range(8)] + [strip]

    def place(rows, parts):
        u, v, s1, s2, s12, wu, wv, strong, b = parts
        field[0, rows] = u
        field[1, rows] = v
        field[2, rows] = s1 + s2
        field[3, rows] = s1 - s2
        field[4, rows] = 2.0 * s12
        static[0, rows] = jnp.where(b > 0.0, 1.0, 0.0) - b
        static[1, rows] = 0.25 * b
        static[2, rows] = b * wu
        static[3, rows] = b * wv
        static[4, rows] = strong

    place(centre, whole)
    place(low, side(got_w, got_c.at[1], got_c.at[3]))
    place(high, side(got_e, got_c.at[0], got_c.at[2]))

    begin = start_ref[0].astype(F32)

    def coefs(k):
        step = jnp.full((CHUNK, LANES), begin + jnp.asarray(k + 1, jnp.int32).astype(F32), F32)
        coef = 0.2 + 0.8 * step / SUBTOTAL
        keep = 1.0 / (1.0 + coef)
        return coef, keep

    to_n = lambda x: pltpu.roll(x, LANES - 1, 1)
    to_s = lambda x: pltpu.roll(x, 1, 1)
    wide = range(PAD, TALL - PAD, CHUNK)
    narrow = range(PAD + 8, TALL - PAD - 8, CHUNK)

    def forward(chunks, k, carry):
        coef, keep = coefs(k)
        gain = coef * keep
        for r in chunks:
            rows = slice(r, r + CHUNK)
            up = slice(r + 1, r + 1 + CHUNK)
            down = slice(r - 1, r - 1 + CHUNK)
            u = field[0, rows]
            v = field[1, rows]
            x1 = field[0, up] - field[0, down]
            x2 = field[1, up] - field[1, down]
            y1 = to_n(u) - to_s(u)
            y2 = to_n(v) - to_s(v)
            div = x1 + y2
            ten = x1 - y2
            quarter = 0.25 * ten
            half = 0.5 * (y1 + x2)
            inv = lax.rsqrt(div * div + quarter * ten + half * half + 0.16)
            rate = gain * static[4, rows]
            un = (div + quarter) * inv
            vn = (div - quarter) * inv
            sn = half * inv
            saved[k, 0, rows] = un
            saved[k, 1, rows] = vn
            saved[k, 2, rows] = sn
            saved[k, 3, rows] = rate * inv
            field[2, rows] = keep * field[2, rows] + rate * (un - 1.0)
            field[3, rows] = keep * field[3, rows] + rate * (vn - 1.0)
            field[4, rows] = keep * field[4, rows] + rate * sn
        for r in chunks:
            rows = slice(r, r + CHUNK)
            up = slice(r + 1, r + 1 + CHUNK)
            down = slice(r - 1, r - 1 + CHUNK)
            m = field[3, rows]
            q = field[4, rows]
            fx = (field[2, up] - field[2, down]) + (to_n(q) - to_s(q))
            fy = (field[4, up] - field[4, down]) + (to_n(m) - to_s(m))
            field[0, rows] = static[0, rows] * field[0, rows] + (static[2, rows] + static[1, rows] * fx)
            field[1, rows] = static[0, rows] * field[1, rows] + (static[3, rows] + static[1, rows] * fy)
        return carry

    with jax.named_scope("forward"):
        lax.fori_loop(0, STEPS // 2, functools.partial(forward, wide), 0, unroll=4)
        lax.fori_loop(STEPS // 2, STEPS, functools.partial(forward, narrow), 0, unroll=4)

    where_cost = jnp.transpose(target[0])
    for i in range(2):
        miss = where_cost * (field[i, centre] - jnp.transpose(target[1 + i]))
        back[i, centre] = miss
        back[2 + i, centre] = static[1, centre] * miss

    def backward(chunks, last, i, carry):
        k = STEPS - 1 - i
        _, keep = coefs(k)
        for r in chunks:
            rows = slice(r, r + CHUNK)
            up = slice(r + 1, r + 1 + CHUNK)
            down = slice(r - 1, r - 1 + CHUNK)
            mu = back[2, rows]
            mv = back[3, rows]
            tp = back[4, rows] + (back[2, down] - back[2, up])
            tm = back[5, rows] + (to_s(mv) - to_n(mv))
            tq = back[6, rows] + ((to_s(mu) - to_n(mu)) + (back[3, down] - back[3, up]))
            un = saved[k, 0, rows]
            vn = saved[k, 1, rows]
            sn = saved[k, 2, rows]
            g = saved[k, 3, rows]
            along = tp * un + tm * vn + tq * sn
            total = tp + tm
            quarter = 0.25 * (tp - tm)
            back[7, rows] = g * ((total + quarter) - along * un)
            back[8, rows] = g * ((total - quarter) - along * vn)
            back[9, rows] = (0.5 * g) * (tq - along * sn)
            back[4, rows] = keep * tp
            back[5, rows] = keep * tm
            back[6, rows] = keep * tq
        for r in chunks:
            rows = slice(r, r + CHUNK)
            up = slice(r + 1, r + 1 + CHUNK)
            down = slice(r - 1, r - 1 + CHUNK)
            yb = back[8, rows]
            sb = back[9, rows]
            lu = back[0, rows]
            lv = back[1, rows]
            if not last:
                back[10, rows] = back[10, rows] + lu
                back[11, rows] = back[11, rows] + lv
            new_u = static[0, rows] * lu + ((back[7, down] - back[7, up]) + (to_s(sb) - to_n(sb)))
            new_v = static[0, rows] * lv + ((back[9, down] - back[9, up]) + (to_s(yb) - to_n(yb)))
            back[0, rows] = new_u
            back[1, rows] = new_v
            if not last:
                back[2, rows] = static[1, rows] * new_u
                back[3, rows] = static[1, rows] * new_v
        return carry

    with jax.named_scope("backward"):
        lax.fori_loop(0, STEPS // 2, functools.partial(backward, narrow, False), 0, unroll=4)
        lax.fori_loop(STEPS // 2, STEPS - 1, functools.partial(backward, wide, False), 0, unroll=3)

    lane_all = lax.broadcasted_iota(jnp.int32, (LANES, LANES), 1)
    with jax.named_scope("wind_pack"):
        for i in range(2):
            gust[i] = 4.0 * static[1] * (back[10 + i] + back[i])
        here = ((lane_all >= 80) & (lane_all < 96)) | (lane_all >= 112)
        both = jnp.where(here, gust[0, centre], pltpu.roll(gust[1, centre], LANES - HALO, 1))
        gust_ns[...] = jnp.transpose(both)[64:LANES]

        @pl.when(top)
        def _():
            for i in range(2):
                part = slice(HALO * i, HALO * (i + 1))
                upper, lower = flip_strip(gust_ns[part], whole_flip, -1.0)
                rev_n_w[16 * i : 16 * i + 8] = upper
                rev_n_w[16 * i + 8 : 16 * i + 16] = lower
                for j, rows in ((0, high), (1, low)):
                    upper, lower = flip_strip(gust[i, rows], whole_flip, -1.0)
                    rev_c_w[j, i, 0:8] = pltpu.roll(upper, 80, 1)
                    rev_c_w[j, i, 8:16] = pltpu.roll(lower, 80, 1)

    finish_wind, finish_wind_send = exchange(
        1,
        wsend_sem,
        wrecv_sem,
        (gust_ns.at[0:32], gust_ns.at[32:64]),
        gust.at[:, high],
        gust.at[:, low],
        (gust.at[:, high], gust.at[:, low], gust.at[:, high], gust.at[:, low]),
        (rev_n_w, rev_c_w.at[0], rev_c_w.at[1]),
        {
            N: got_n_w,
            S: got_s_w,
            E: got_e_w,
            W: got_w_w,
            NE: got_c_w.at[0],
            NW: got_c_w.at[1],
            SE: got_c_w.at[2],
            SW: got_c_w.at[3],
        },
    )
    with jax.named_scope("backward_last"):
        backward(wide, True, STEPS - 1, 0)
    finish_send()

    def result(rows):
        p = back[4, rows]
        m = back[5, rows]
        return [back[0, rows], back[1, rows], p + m, p - m, 2.0 * back[6, rows]]

    with jax.named_scope("state_pack"):
        for f, value in enumerate(result(centre)):
            fin[f] = jnp.transpose(value)
        for rows, dst in ((high, fin_e), (low, fin_w)):
            dst[...] = jnp.transpose(jnp.concatenate(result(rows) + [spare_rows], axis=0))

        @pl.when(top)
        def _():
            for f in range(5):
                rev_n[f, 0:8], rev_n[f, 8:16] = flip_strip(fin[f, NORTH], whole_flip, SIGNS[f])
            for i, src in ((0, fin_e), (1, fin_w)):
                rev_c[i, 0:8], rev_c[i, 8:16] = flip_strip(src[NORTH], group_flip, group_sign)

    with jax.named_scope("recv_wind"):
        finish_wind()

    def with_sides(i):
        value = gust[i, centre]

        def ends(straight, upper, lower):
            extra = jnp.where(lane16 < ROWS, straight[i], 0.0)
            upper = pltpu.roll(upper[i], 80, 1)
            extra = extra + jnp.where((lane16 >= 64) & (lane16 < ROWS), upper, 0.0)
            return extra + jnp.where(lane16 < HALO, pltpu.roll(lower[i], 48, 1), 0.0)

        at_w = ends(got_w_w, got_c_w.at[1], got_c_w.at[3])
        at_e = ends(got_e_w, got_c_w.at[0], got_c_w.at[2])
        parts = [value[:HALO] + at_w, value[HALO:-HALO], value[-HALO:] + at_e]
        value = jnp.transpose(jnp.concatenate(parts, axis=0))
        rows = slice(HALO * (1 - i), HALO * (2 - i))
        return jnp.concatenate(
            [value[0:16] + got_s_w[rows], value[16:64], value[64:80] + got_n_w[rows]], axis=0
        )

    with jax.named_scope("wind_add"):
        for i in range(2):
            wind_out[i] = with_sides(i)
        squares = wind_out[0] * wind_out[0] + wind_out[1] * wind_out[1]
        part = jnp.sum(squares, axis=0, keepdims=True)

    def all_sum(buf, send, recv, count, me, where):
        def copy_of(d, slot):
            return pltpu.make_async_remote_copy(
                src_ref=buf.at[me],
                dst_ref=buf.at[slot],
                send_sem=send.at[d],
                recv_sem=recv.at[d],
                device_id=where(d)[1],
                device_id_type=MESH,
            )

        def copies():
            return [copy_of(d, me) for d in range(1, count)]

        def arrivals():
            return [copy_of(d, where(d, -1)[0]) for d in range(1, count)]

        def begin_sum(part):
            buf[me] = part
            for copy in copies():
                copy.start()

        def end_sum():
            for copy in arrivals():
                copy.wait_recv()
            for copy in copies():
                copy.wait_send()
            return jnp.sum(buf[...], axis=0)

        return begin_sum, end_sum

    begin_near, end_near = all_sum(red_x, xs_sem, xr_sem, nears, near, near_at)
    begin_far, end_far = all_sum(red_y, ys_sem, yr_sem, fars, far, far_at)
    begin_near(part)
    finish_state, finish_state_send = exchange(
        2,
        fsend_sem,
        frecv_sem,
        (fin.at[:, NORTH], fin.at[:, SOUTH]),
        fin_e.at[0:ROWS],
        fin_w.at[0:ROWS],
        (fin_e.at[NORTH], fin_w.at[NORTH], fin_e.at[SOUTH], fin_w.at[SOUTH]),
        (rev_n.at[0:5], rev_c.at[0, 0:HALO], rev_c.at[1, 0:HALO]),
        {
            N: got_n_f,
            S: got_s_f,
            E: got_e_f,
            W: got_w_f,
            NE: got_c_f.at[0],
            NW: got_c_f.at[1],
            SE: got_c_f.at[2],
            SW: got_c_f.at[3],
        },
    )
    with jax.named_scope("sum_near"):
        part = end_near()
    begin_far(part)
    with jax.named_scope("recv_state"):
        finish_state()
    with jax.named_scope("state_add"):
        got_e_f[64:80] = got_e_f[64:80] + got_c_f[0]
        got_w_f[64:80] = got_w_f[64:80] + got_c_f[1]
        got_e_f[0:16] = got_e_f[0:16] + got_c_f[2]
        got_w_f[0:16] = got_w_f[0:16] + got_c_f[3]
        packed_e = got_e_f[...]
        packed_w = got_w_f[...]
        for f in range(5):
            side_e = pltpu.roll(packed_e, LANES - HALO - HALO * f, 1)
            side_w = packed_w if f == 0 else pltpu.roll(packed_w, LANES - HALO * f, 1)
            value = fin[f, 0:ROWS]
            value = value + jnp.where(lane >= LANES - HALO, side_e, 0.0)
            value = value + jnp.where(lane < HALO, side_w, 0.0)
            state_out[f] = value
            state_out[f, 0:16] = state_out[f, 0:16] + got_s_f[f]
            state_out[f, 64:80] = state_out[f, 64:80] + got_n_f[f]
    finish_wind_send()
    finish_state_send()
    with jax.named_scope("sum_far"):
        part = end_far()
    total = jnp.sum(jnp.broadcast_to(part, (8, LANES)), axis=1, keepdims=True)[0:1]
    entries = 2 * ROWS * LANES * nx * ny
    inv = lax.rsqrt(total / entries + NORM_EPS)
    for i in range(2):
        wind_out[i] = wind_out[i] * inv


def writer(state, wind, state_hbm, wind_hbm, sem):
    pieces = [(state, state_hbm, f) for f in range(5)] + [(wind, wind_hbm, f) for f in range(2)]
    copies = [
        pltpu.make_async_copy(src.at[f], dst.at[f], sem.at[i])
        for i, (src, dst, f) in enumerate(pieces)
    ]
    for copy in copies:
        copy.start()
    for copy in copies:
        copy.wait()


def solution(mesh):
    nx, ny = mesh.shape["gx"], mesh.shape["gy"]

    def per_device(velocity, stress, wind, strength, mass, land, region, observed, start):
        vm = lambda *shape: pltpu.VMEM(shape, F32)
        dma = pltpu.SemaphoreType.DMA
        any_spec = pl.BlockSpec(memory_space=pl.ANY)
        args = (start, velocity, stress, wind, strength, mass, land, region, observed)
        args = [args[0]] + [pltpu.with_memory_space_constraint(z, pltpu.HBM) for z in args[1:]]
        shapes = (
            jax.ShapeDtypeStruct((5, ROWS, LANES), F32),
            jax.ShapeDtypeStruct((2, ROWS, LANES), F32),
        )
        vmem_spec = pl.BlockSpec(memory_space=pltpu.VMEM)
        state, gusts = pl.pallas_call(
            functools.partial(kernel, nx, ny),
            out_shape=shapes,
            in_specs=[pl.BlockSpec(memory_space=pltpu.SMEM)] + [any_spec] * 8,
            out_specs=(vmem_spec, vmem_spec),
            scratch_shapes=[
                vm(9, LANES, LANES),
                vm(ROWS, LANES),
                pltpu.VMEM((ROWS, LANES), jnp.int32),
                pltpu.VMEM((ROWS, LANES), jnp.int32),
                vm(3, LANES, LANES),
                vm(ROWS + HALO, LANES),
                vm(ROWS + HALO, LANES),
                vm(4, 2 * HALO, LANES),
                vm(ROWS + HALO, LANES),
                vm(ROWS + HALO, LANES),
                vm(4, 2 * HALO, LANES),
                vm(9, HALO, LANES),
                vm(2, 2 * HALO, LANES),
                vm(5, TALL, LANES),
                vm(5, TALL, LANES),
                vm(STEPS, 4, TALL, LANES),
                vm(12, TALL, LANES),
                vm(5, LANES, LANES),
                vm(LANES, LANES),
                vm(LANES, LANES),
                vm(5, HALO, LANES),
                vm(5, HALO, LANES),
                vm(ROWS, LANES),
                vm(ROWS, LANES),
                vm(4, HALO, LANES),
                vm(2, TALL, LANES),
                vm(64, LANES),
                vm(2 * HALO, LANES),
                vm(2 * HALO, LANES),
                vm(2, HALO, LANES),
                vm(2, HALO, LANES),
                vm(4, 2, HALO, LANES),
                vm(2 * HALO, LANES),
                vm(2, 2, HALO, LANES),
                vm(nx // 2, 1, LANES),
                vm(2 * ny, 1, LANES),
                dma((9,)),
                dma((8,)),
                dma((8,)),
                dma((8,)),
                dma((8,)),
                dma((8,)),
                dma((8,)),
                dma((6,)),
                dma((nx // 2,)),
                dma((nx // 2,)),
                dma((2 * ny,)),
                dma((2 * ny,)),
            ],
            compiler_params=pltpu.CompilerParams(
                collective_id=0, has_side_effects=True, vmem_limit_bytes=32 * 1024 * 1024
            ),
        )(*args)
        return pl.pallas_call(
            writer,
            out_shape=shapes,
            in_specs=[vmem_spec, vmem_spec],
            out_specs=(any_spec, any_spec),
            scratch_shapes=[dma((7,))],
        )(
            pltpu.with_memory_space_constraint(state, pltpu.VMEM),
            pltpu.with_memory_space_constraint(gusts, pltpu.VMEM),
        )

    tri, two = P(None, "gy", "gx"), P("gy", "gx")
    return jax.shard_map(
        per_device,
        mesh=mesh,
        in_specs=(tri, tri, tri, two, two, two, two, tri, P()),
        out_specs=(tri, tri),
        check_vma=False,
    )
```

```python
import functools

import jax
import jax.numpy as jnp
from jax import lax
from jax.experimental import pallas as pl
from jax.experimental.pallas import tpu as pltpu
from jax.sharding import PartitionSpec as P

STEPS = 8
SUBTOTAL = 120
HALO = 2 * STEPS
LANES = 128
PAD = 8
CHUNK = 8
NORM_EPS = 1e-06
F32 = jnp.float32
MESH = pl.DeviceIdType.MESH

ROWS = 80
NORTH = slice(80, 96)
GAP = slice(96, 112)
SOUTH = slice(112, 128)
FIRST = PAD + HALO
LAST = FIRST + LANES
TALL = LAST + HALO + PAD
SIGNS = (-1.0, -1.0, 1.0, 1.0, 1.0, -1.0, -1.0, 1.0, 1.0)

N, S, E, W, NE, NW, SE, SW = range(8)


def flip_lanes(x, index):
    return jnp.take_along_axis(x, index, axis=1)


def flip_strip(strip, lane_index, sign):
    row_index = 7 - lax.broadcasted_iota(jnp.int32, (8, LANES), 0)
    upper = jnp.take_along_axis(strip[8:16], row_index, axis=0)
    lower = jnp.take_along_axis(strip[0:8], row_index, axis=0)
    upper = flip_lanes(upper, lane_index)
    lower = flip_lanes(lower, lane_index)
    return sign * upper, sign * lower


def kernel(
    nx,
    ny,
    start_ref,
    velocity,
    stress,
    wind,
    strength,
    mass,
    land,
    region,
    observed,
    state_out,
    wind_out,
    raw,
    mass_v,
    land_v,
    region_v,
    target,
    bundle_e,
    bundle_w,
    corner_out,
    got_e,
    got_w,
    got_c,
    rev_n,
    rev_c,
    field,
    static,
    saved,
    back,
    fin,
    fin_e,
    fin_w,
    got_n_f,
    got_s_f,
    got_e_f,
    got_w_f,
    got_c_f,
    gust,
    gust_ns,
    gust_c,
    got_n_w,
    got_s_w,
    got_e_w,
    got_w_w,
    got_c_w,
    rev_n_w,
    rev_c_w,
    red_x,
    red_y,
    load_sem,
    send_sem,
    recv_sem,
    wsend_sem,
    wrecv_sem,
    fsend_sem,
    frecv_sem,
    self_sem,
    xs_sem,
    xr_sem,
    ys_sem,
    yr_sem,
):
    gx = lax.axis_index("gx")
    gy = lax.axis_index("gy")
    top = gy == ny - 1
    bottom = gy == 0
    not_top = gy < ny - 1
    not_bottom = gy > 0
    def wrap(index, count):
        return jnp.where(index >= count, index - count, index)

    east = wrap(gx + 1, nx)
    west = wrap(gx + nx - 1, nx)
    fold = nx - 1 - gx
    fold_e = wrap(2 * nx - 2 - gx, nx)
    fold_w = wrap(nx - gx, nx)

    def at(x, y):
        return {"gx": x, "gy": y}

    loads = [
        pltpu.make_async_copy(velocity, raw.at[0:2, 0:ROWS], load_sem.at[0]),
        pltpu.make_async_copy(stress, raw.at[2:5, 0:ROWS], load_sem.at[1]),
        pltpu.make_async_copy(wind, raw.at[5:7, 0:ROWS], load_sem.at[2]),
        pltpu.make_async_copy(strength, raw.at[7, 0:ROWS], load_sem.at[3]),
        pltpu.make_async_copy(mass, mass_v, load_sem.at[4]),
        pltpu.make_async_copy(land, land_v, load_sem.at[5]),
        pltpu.make_async_copy(region, region_v, load_sem.at[6]),
        pltpu.make_async_copy(observed, target.at[1:3, 0:ROWS], load_sem.at[7]),
    ]
    for copy in loads:
        copy.start()

    ring = lax.div(gx, 4)
    core = lax.rem(gx, 2)
    cross = lax.div(gx - 4 * ring - core, 2)
    rings = nx // 4
    near = ring * 2 + core
    far = cross * ny + gy
    nears, fars = 2 * rings, 2 * ny

    def near_at(d, sign=1):
        r = wrap(ring + (d // 2 if sign > 0 else rings - d // 2), rings) if d // 2 else ring
        c = 1 - core if d % 2 else core
        return r * 2 + c, at(r * 4 + cross * 2 + c, gy)

    def far_at(d, sign=1):
        y = wrap(gy + (d // 2 if sign > 0 else ny - d // 2), ny) if d // 2 else gy
        x = 1 - cross if d % 2 else cross
        return x * ny + y, at(gx + 2 * (x - cross), y)

    barrier = pltpu.get_barrier_semaphore()

    def greet(where):
        pl.semaphore_signal(barrier, inc=1, device_id=where, device_id_type=MESH)

    with jax.named_scope("greet"):
        greet(at(east, gy))
        greet(at(west, gy))

        @pl.when(not_top)
        def _():
            for x in (gx, east, west):
                greet(at(x, gy + 1))

        @pl.when(not_bottom)
        def _():
            for x in (gx, east, west):
                greet(at(x, gy - 1))

        @pl.when(top)
        def _():
            greet(at(fold, gy))

        @pl.when(top & (fold_e != gx))
        def _():
            greet(at(fold_e, gy))

        @pl.when(top & (fold_w != gx))
        def _():
            greet(at(fold_w, gy))

        for d in range(1, fars):
            greet(far_at(d)[1])
        for d in range(1, nears):
            greet(near_at(d)[1])

    zero_gap = jnp.zeros((HALO, LANES), F32)
    for f in range(9):
        raw[f, GAP] = zero_gap
    for f in range(3):
        target[f, ROWS:LANES] = jnp.zeros((LANES - ROWS, LANES), F32)
    zero_pad = jnp.zeros((PAD, LANES), F32)
    for f in range(5):
        field[f, 0:PAD] = zero_pad
        field[f, TALL - PAD : TALL] = zero_pad
    for f in range(12):
        back[f, 0:FIRST] = jnp.zeros((FIRST, LANES), F32)
        back[f, LAST:TALL] = jnp.zeros((FIRST, LANES), F32)
    for f in (4, 5, 6, 10, 11):
        back[f, FIRST:LAST] = jnp.zeros((LANES, LANES), F32)

    @pl.when(bottom)
    def _():
        for f in range(9):
            raw[f, SOUTH] = zero_gap
        for f in range(5):
            got_s_f[f] = zero_gap
        for i in (2, 3):
            got_c[i] = jnp.zeros((HALO + 8, LANES), F32)
            got_c_f[i] = zero_gap
            got_c_w[i] = jnp.zeros((8, LANES), F32)
        got_s_w[...] = jnp.zeros((2 * HALO, LANES), F32)

    for copy in loads:
        copy.wait()

    lane = lax.broadcasted_iota(jnp.int32, (ROWS, LANES), 1)
    lane16 = lax.broadcasted_iota(jnp.int32, (HALO, LANES), 1)
    lane8 = lax.broadcasted_iota(jnp.int32, (8, LANES), 1)
    whole_flip = LANES - 1 - lane8
    group_flip = lane8 + (HALO - 1) - 2 * lax.rem(lane8, HALO)
    group = lane8 // HALO
    group_sign = jnp.where((group < 2) | ((group >= 5) & (group < 7)), -1.0, 1.0)
    odd = lax.rem(group, 2) == 1

    def two_tiles(first, second):
        return jnp.where(odd, first, pltpu.roll(second, LANES - HALO, 1))

    spare_rows = jnp.zeros((LANES - ROWS, LANES), F32)

    with jax.named_scope("pack"):
        drag = land_v[...].astype(F32) * (0.5 / (mass_v[...] + 0.5))
        raw[8, 0:ROWS] = drag
        drag_t = jnp.transpose(jnp.concatenate([drag, spare_rows], axis=0))
        target[0, 0:ROWS] = region_v[...].astype(F32)
        packed_e = pltpu.roll(raw[0, 0:ROWS], HALO, 1)
        packed_w = raw[0, 0:ROWS]
        for f in range(1, 8):
            here = (lane >= HALO * f) & (lane < HALO * (f + 1))
            value = raw[f, 0:ROWS]
            packed_e = jnp.where(here, pltpu.roll(value, (HALO * f + HALO) % LANES, 1), packed_e)
            packed_w = jnp.where(here, pltpu.roll(value, HALO * f, 1), packed_w)
        sides = ((bundle_e, packed_e, drag_t[LANES - HALO :]), (bundle_w, packed_w, drag_t[:HALO]))
        strips = []
        for i, (bundle, packed, strip) in enumerate(sides):
            bundle[0:ROWS] = packed
            bundle[ROWS:] = strip
            upper, lower = pltpu.roll(strip, 48, 1), pltpu.roll(strip, 80, 1)
            strips.append(upper)
            corner_out[i, 0:HALO] = packed[64:80]
            corner_out[i, HALO:] = two_tiles(upper[0:8], upper[8:16])
            corner_out[2 + i, 0:HALO] = packed[0:16]
            corner_out[2 + i, HALO:] = two_tiles(lower[0:8], lower[8:16])

        @pl.when(top)
        def _():
            for f in range(9):
                rev_n[f, 0:8], rev_n[f, 8:16] = flip_strip(raw[f, 64:80], whole_flip, SIGNS[f])
            for i in range(2):
                rev_c[i, 0:8], rev_c[i, 8:16] = flip_strip(
                    corner_out[i, 0:HALO], group_flip, group_sign
                )
                upper, lower = flip_strip(strips[i], whole_flip, 1.0)
                rev_c[i, HALO:] = two_tiles(pltpu.roll(upper, 80, 1), pltpu.roll(lower, 80, 1))

    def remote(src, dst, send, recv, slot, x, y):
        return pltpu.make_async_remote_copy(
            src_ref=src,
            dst_ref=dst,
            send_sem=send.at[slot],
            recv_sem=recv.at[slot],
            device_id=at(x, y),
            device_id_type=MESH,
        )

    def exchange(turn, send, recv, ns, e, w, corners, folded, slots):
        to_n, to_s = ns
        corner = {
            SW: (corners[0], east, gy + 1),
            SE: (corners[1], west, gy + 1),
            NW: (corners[2], east, gy - 1),
            NE: (corners[3], west, gy - 1),
        }

        def side_copies():
            return [
                remote(e, slots[W], send, recv, W, east, gy),
                remote(w, slots[E], send, recv, E, west, gy),
            ]

        def corner_copy(k):
            return remote(corner[k][0], slots[k], send, recv, k, *corner[k][1:])

        def corner_copies(kinds):
            return [corner_copy(k) for k in kinds]

        def north_copy():
            return remote(to_n, slots[S], send, recv, S, gx, gy + 1)

        def south_copy():
            return remote(to_s, slots[N], send, recv, N, gx, gy - 1)

        def north_copies():
            return [*corner_copies((SW, SE)), north_copy()]

        def south_copies():
            return [*corner_copies((NW, NE)), south_copy()]

        def fold_copy(k, src, slot, x):
            return pltpu.make_async_remote_copy(
                src_ref=src,
                dst_ref=slots[slot],
                send_sem=send.at[k],
                recv_sem=recv.at[slot],
                device_id=at(x, gy),
                device_id_type=MESH,
            )

        def local_copy(i, src, slot):
            return pltpu.make_async_copy(src, slots[slot], self_sem.at[2 * turn + i])

        fold_n = lambda: fold_copy(S, folded[0], N, fold)
        fold_ne = lambda: fold_copy(SW, folded[1], NE, fold_e)
        fold_nw = lambda: fold_copy(SE, folded[2], NW, fold_w)
        self_ne = lambda: local_copy(0, folded[1], NE)
        self_nw = lambda: local_copy(1, folded[2], NW)

        @pl.when(not_top)
        def _():
            for copy in corner_copies((SW, SE)):
                copy.start()

        @pl.when(not_bottom)
        def _():
            for copy in corner_copies((NW, NE)):
                copy.start()

        @pl.when(top & (fold_e != gx))
        def _():
            fold_ne().start()

        @pl.when(top & (fold_e == gx))
        def _():
            self_ne().start()

        @pl.when(top & (fold_w != gx))
        def _():
            fold_nw().start()

        @pl.when(top & (fold_w == gx))
        def _():
            self_nw().start()

        for copy in side_copies():
            copy.start()

        @pl.when(top)
        def _():
            fold_n().start()

        @pl.when(not_top)
        def _():
            north_copy().start()

        @pl.when(not_bottom)
        def _():
            south_copy().start()

        def finish_recv():
            for copy in side_copies():
                copy.wait_recv()

            @pl.when(not_bottom)
            def _():
                for copy in north_copies():
                    copy.wait_recv()

            @pl.when(not_top)
            def _():
                for copy in south_copies():
                    copy.wait_recv()

            @pl.when(top)
            def _():
                fold_n().wait_recv()

            @pl.when(top & (fold_e != gx))
            def _():
                fold_ne().wait_recv()

            @pl.when(top & (fold_e == gx))
            def _():
                self_ne().wait()

            @pl.when(top & (fold_w != gx))
            def _():
                fold_nw().wait_recv()

            @pl.when(top & (fold_w == gx))
            def _():
                self_nw().wait()

        def finish_send():
            for copy in side_copies():
                copy.wait_send()

            @pl.when(not_top)
            def _():
                for copy in north_copies():
                    copy.wait_send()

            @pl.when(not_bottom)
            def _():
                for copy in south_copies():
                    copy.wait_send()

            @pl.when(top)
            def _():
                fold_n().wait_send()

            @pl.when(top & (fold_e != gx))
            def _():
                fold_ne().wait_send()

            @pl.when(top & (fold_w != gx))
            def _():
                fold_nw().wait_send()

        return finish_recv, finish_send

    peers = (nears - 1) + (fars - 1) + 2
    as_int = lambda flag: flag.astype(jnp.int32)
    peers = peers + 3 * as_int(not_top) + 3 * as_int(not_bottom) + as_int(top)
    peers = peers + as_int(top & (fold_e != gx)) + as_int(top & (fold_w != gx))
    with jax.named_scope("barrier"):
        pl.semaphore_wait(barrier, peers)

    finish_recv, finish_send = exchange(
        0,
        send_sem,
        recv_sem,
        (raw.at[:, 64:80], raw.at[:, 0:16]),
        bundle_e,
        bundle_w,
        tuple(corner_out.at[i] for i in range(4)),
        (rev_n, rev_c.at[0], rev_c.at[1]),
        {
            N: raw.at[:, NORTH],
            S: raw.at[:, SOUTH],
            E: got_e,
            W: got_w,
            NE: got_c.at[0],
            NW: got_c.at[1],
            SE: got_c.at[2],
            SW: got_c.at[3],
        },
    )
    with jax.named_scope("recv_first"):
        finish_recv()

    centre = slice(FIRST, LAST)
    low = slice(PAD, FIRST)
    high = slice(LAST, LAST + HALO)
    whole = [jnp.transpose(raw[f]) for f in range(9)]

    def side(bundle, upper, lower):
        packed = [bundle[0:ROWS], upper[0:HALO], zero_gap, lower[0:HALO]]
        packed = jnp.transpose(jnp.concatenate(packed, axis=0))
        upper, lower = [
            jnp.concatenate([x[HALO:], pltpu.roll(x[HALO:], HALO, 1)], axis=0)
            for x in (upper, lower)
        ]
        strip = jnp.where(lane16 < 96, upper, jnp.where(lane16 >= 112, lower, 0.0))
        strip = jnp.where(lane16 < ROWS, bundle[ROWS:], strip)
        return [packed[HALO * f : HALO * (f + 1)] for f in range(8)] + [strip]

    def place(rows, parts):
        u, v, s1, s2, s12, wu, wv, strong, b = parts
        field[0, rows] = u
        field[1, rows] = v
        field[2, rows] = s1 + s2
        field[3, rows] = s1 - s2
        field[4, rows] = 2.0 * s12
        static[0, rows] = jnp.where(b > 0.0, 1.0, 0.0) - b
        static[1, rows] = 0.25 * b
        static[2, rows] = b * wu
        static[3, rows] = b * wv
        static[4, rows] = strong

    place(centre, whole)
    place(low, side(got_w, got_c.at[1], got_c.at[3]))
    place(high, side(got_e, got_c.at[0], got_c.at[2]))

    begin = start_ref[0].astype(F32)

    def coefs(k):
        step = jnp.full((CHUNK, LANES), begin + jnp.asarray(k + 1, jnp.int32).astype(F32), F32)
        coef = 0.2 + 0.8 * step / SUBTOTAL
        keep = 1.0 / (1.0 + coef)
        return coef, keep

    to_n = lambda x: pltpu.roll(x, LANES - 1, 1)
    to_s = lambda x: pltpu.roll(x, 1, 1)
    wide = range(PAD, TALL - PAD, CHUNK)
    narrow = range(PAD + 8, TALL - PAD - 8, CHUNK)

    def forward(chunks, k, carry):
        coef, keep = coefs(k)
        gain = coef * keep
        for r in chunks:
            rows = slice(r, r + CHUNK)
            up = slice(r + 1, r + 1 + CHUNK)
            down = slice(r - 1, r - 1 + CHUNK)
            u = field[0, rows]
            v = field[1, rows]
            x1 = field[0, up] - field[0, down]
            x2 = field[1, up] - field[1, down]
            y1 = to_n(u) - to_s(u)
            y2 = to_n(v) - to_s(v)
            div = x1 + y2
            ten = x1 - y2
            quarter = 0.25 * ten
            half = 0.5 * (y1 + x2)
            inv = lax.rsqrt(div * div + quarter * ten + half * half + 0.16)
            rate = gain * static[4, rows]
            un = (div + quarter) * inv
            vn = (div - quarter) * inv
            sn = half * inv
            saved[k, 0, rows] = un
            saved[k, 1, rows] = vn
            saved[k, 2, rows] = sn
            saved[k, 3, rows] = rate * inv
            field[2, rows] = keep * field[2, rows] + rate * (un - 1.0)
            field[3, rows] = keep * field[3, rows] + rate * (vn - 1.0)
            field[4, rows] = keep * field[4, rows] + rate * sn
        for r in chunks:
            rows = slice(r, r + CHUNK)
            up = slice(r + 1, r + 1 + CHUNK)
            down = slice(r - 1, r - 1 + CHUNK)
            m = field[3, rows]
            q = field[4, rows]
            fx = (field[2, up] - field[2, down]) + (to_n(q) - to_s(q))
            fy = (field[4, up] - field[4, down]) + (to_n(m) - to_s(m))
            field[0, rows] = static[0, rows] * field[0, rows] + (static[2, rows] + static[1, rows] * fx)
            field[1, rows] = static[0, rows] * field[1, rows] + (static[3, rows] + static[1, rows] * fy)
        return carry

    with jax.named_scope("forward"):
        lax.fori_loop(0, STEPS // 2, functools.partial(forward, wide), 0, unroll=4)
        lax.fori_loop(STEPS // 2, STEPS, functools.partial(forward, narrow), 0, unroll=4)

    where_cost = jnp.transpose(target[0])
    for i in range(2):
        miss = where_cost * (field[i, centre] - jnp.transpose(target[1 + i]))
        back[i, centre] = miss
        back[2 + i, centre] = static[1, centre] * miss

    def backward(chunks, last, i, carry):
        k = STEPS - 1 - i
        _, keep = coefs(k)
        for r in chunks:
            rows = slice(r, r + CHUNK)
            up = slice(r + 1, r + 1 + CHUNK)
            down = slice(r - 1, r - 1 + CHUNK)
            mu = back[2, rows]
            mv = back[3, rows]
            tp = back[4, rows] + (back[2, down] - back[2, up])
            tm = back[5, rows] + (to_s(mv) - to_n(mv))
            tq = back[6, rows] + ((to_s(mu) - to_n(mu)) + (back[3, down] - back[3, up]))
            un = saved[k, 0, rows]
            vn = saved[k, 1, rows]
            sn = saved[k, 2, rows]
            g = saved[k, 3, rows]
            along = tp * un + tm * vn + tq * sn
            total = tp + tm
            quarter = 0.25 * (tp - tm)
            back[7, rows] = g * ((total + quarter) - along * un)
            back[8, rows] = g * ((total - quarter) - along * vn)
            back[9, rows] = (0.5 * g) * (tq - along * sn)
            back[4, rows] = keep * tp
            back[5, rows] = keep * tm
            back[6, rows] = keep * tq
        for r in chunks:
            rows = slice(r, r + CHUNK)
            up = slice(r + 1, r + 1 + CHUNK)
            down = slice(r - 1, r - 1 + CHUNK)
            yb = back[8, rows]
            sb = back[9, rows]
            lu = back[0, rows]
            lv = back[1, rows]
            if not last:
                back[10, rows] = back[10, rows] + lu
                back[11, rows] = back[11, rows] + lv
            new_u = static[0, rows] * lu + ((back[7, down] - back[7, up]) + (to_s(sb) - to_n(sb)))
            new_v = static[0, rows] * lv + ((back[9, down] - back[9, up]) + (to_s(yb) - to_n(yb)))
            back[0, rows] = new_u
            back[1, rows] = new_v
            if not last:
                back[2, rows] = static[1, rows] * new_u
                back[3, rows] = static[1, rows] * new_v
        return carry

    with jax.named_scope("backward"):
        lax.fori_loop(0, STEPS // 2, functools.partial(backward, narrow, False), 0, unroll=4)
        lax.fori_loop(STEPS // 2, STEPS - 1, functools.partial(backward, wide, False), 0, unroll=3)

    def four_tiles(u0, u1, v0, v1):
        other = two_tiles(pltpu.roll(v0, 64, 1), pltpu.roll(v1, 64, 1))
        return jnp.where(lane8 >= 64, two_tiles(u0, u1), other)

    lane_all = lax.broadcasted_iota(jnp.int32, (LANES, LANES), 1)
    with jax.named_scope("wind_pack"):
        for i in range(2):
            gust[i] = 4.0 * static[1] * (back[10 + i] + back[i])
        here = ((lane_all >= 80) & (lane_all < 96)) | (lane_all >= 112)
        both = jnp.where(here, gust[0, centre], pltpu.roll(gust[1, centre], LANES - HALO, 1))
        gust_ns[...] = jnp.transpose(both)[64:LANES]
        for j, rows in ((0, high), (1, low)):
            u, v = gust[0, rows], gust[1, rows]
            gust_c[j] = four_tiles(u[0:8], u[8:16], v[0:8], v[8:16])

        @pl.when(top)
        def _():
            for i in range(2):
                part = slice(HALO * i, HALO * (i + 1))
                upper, lower = flip_strip(gust_ns[part], whole_flip, -1.0)
                rev_n_w[16 * i : 16 * i + 8] = upper
                rev_n_w[16 * i + 8 : 16 * i + 16] = lower
            for j, rows in ((0, high), (1, low)):
                tiles = []
                for i in range(2):
                    tiles += flip_strip(gust[i, rows], whole_flip, -1.0)
                rev_c_w[j] = four_tiles(*[pltpu.roll(tile, 80, 1) for tile in tiles])

    finish_wind, finish_wind_send = exchange(
        1,
        wsend_sem,
        wrecv_sem,
        (gust_ns.at[0:32], gust_ns.at[32:64]),
        gust.at[:, high],
        gust.at[:, low],
        (gust_c.at[0], gust_c.at[1], gust_c.at[0], gust_c.at[1]),
        (rev_n_w, rev_c_w.at[0], rev_c_w.at[1]),
        {
            N: got_n_w,
            S: got_s_w,
            E: got_e_w,
            W: got_w_w,
            NE: got_c_w.at[0],
            NW: got_c_w.at[1],
            SE: got_c_w.at[2],
            SW: got_c_w.at[3],
        },
    )
    with jax.named_scope("backward_last"):
        backward(wide, True, STEPS - 1, 0)
    finish_send()

    def result(rows):
        p = back[4, rows]
        m = back[5, rows]
        return [back[0, rows], back[1, rows], p + m, p - m, 2.0 * back[6, rows]]

    with jax.named_scope("state_pack"):
        for f, value in enumerate(result(centre)):
            fin[f] = jnp.transpose(value)
        for rows, dst in ((high, fin_e), (low, fin_w)):
            dst[...] = jnp.transpose(jnp.concatenate(result(rows) + [spare_rows], axis=0))

        @pl.when(top)
        def _():
            for f in range(5):
                rev_n[f, 0:8], rev_n[f, 8:16] = flip_strip(fin[f, NORTH], whole_flip, SIGNS[f])
            for i, src in ((0, fin_e), (1, fin_w)):
                rev_c[i, 0:8], rev_c[i, 8:16] = flip_strip(src[NORTH], group_flip, group_sign)

    with jax.named_scope("recv_wind"):
        finish_wind()

    def with_sides(i):
        value = gust[i, centre]

        def ends(straight, upper, lower):
            extra = jnp.where(lane16 < ROWS, straight[i], 0.0)
            place = 64 * i
            upper = [pltpu.roll(upper[...], (80 - place + LANES + 16 * t) % LANES, 1) for t in (0, 1)]
            lower = [pltpu.roll(lower[...], (48 + place + 16 * t) % LANES, 1) for t in (0, 1)]
            upper, lower = jnp.concatenate(upper, axis=0), jnp.concatenate(lower, axis=0)
            extra = extra + jnp.where((lane16 >= 64) & (lane16 < ROWS), upper, 0.0)
            return extra + jnp.where(lane16 < HALO, lower, 0.0)

        at_w = ends(got_w_w, got_c_w.at[1], got_c_w.at[3])
        at_e = ends(got_e_w, got_c_w.at[0], got_c_w.at[2])
        parts = [value[:HALO] + at_w, value[HALO:-HALO], value[-HALO:] + at_e]
        value = jnp.transpose(jnp.concatenate(parts, axis=0))
        rows = slice(HALO * (1 - i), HALO * (2 - i))
        return jnp.concatenate(
            [value[0:16] + got_s_w[rows], value[16:64], value[64:80] + got_n_w[rows]], axis=0
        )

    with jax.named_scope("wind_add"):
        for i in range(2):
            wind_out[i] = with_sides(i)
        squares = wind_out[0] * wind_out[0] + wind_out[1] * wind_out[1]
        part = jnp.sum(squares, axis=0, keepdims=True)

    def all_sum(buf, send, recv, count, me, where):
        def copy_of(d, slot):
            return pltpu.make_async_remote_copy(
                src_ref=buf.at[me],
                dst_ref=buf.at[slot],
                send_sem=send.at[d],
                recv_sem=recv.at[d],
                device_id=where(d)[1],
                device_id_type=MESH,
            )

        def copies():
            return [copy_of(d, me) for d in range(1, count)]

        def arrivals():
            return [copy_of(d, where(d, -1)[0]) for d in range(1, count)]

        def begin_sum(part):
            buf[me] = part
            for copy in copies():
                copy.start()

        def end_sum():
            for copy in arrivals():
                copy.wait_recv()
            for copy in copies():
                copy.wait_send()
            return jnp.sum(buf[...], axis=0)

        return begin_sum, end_sum

    begin_near, end_near = all_sum(red_x, xs_sem, xr_sem, nears, near, near_at)
    begin_far, end_far = all_sum(red_y, ys_sem, yr_sem, fars, far, far_at)
    begin_near(part)
    finish_state, finish_state_send = exchange(
        2,
        fsend_sem,
        frecv_sem,
        (fin.at[:, NORTH], fin.at[:, SOUTH]),
        fin_e.at[0:ROWS],
        fin_w.at[0:ROWS],
        (fin_e.at[NORTH], fin_w.at[NORTH], fin_e.at[SOUTH], fin_w.at[SOUTH]),
        (rev_n.at[0:5], rev_c.at[0, 0:HALO], rev_c.at[1, 0:HALO]),
        {
            N: got_n_f,
            S: got_s_f,
            E: got_e_f,
            W: got_w_f,
            NE: got_c_f.at[0],
            NW: got_c_f.at[1],
            SE: got_c_f.at[2],
            SW: got_c_f.at[3],
        },
    )
    with jax.named_scope("sum_near"):
        part = end_near()
    begin_far(part)
    with jax.named_scope("recv_state"):
        finish_state()
    with jax.named_scope("state_add"):
        got_e_f[64:80] = got_e_f[64:80] + got_c_f[0]
        got_w_f[64:80] = got_w_f[64:80] + got_c_f[1]
        got_e_f[0:16] = got_e_f[0:16] + got_c_f[2]
        got_w_f[0:16] = got_w_f[0:16] + got_c_f[3]
        packed_e = got_e_f[...]
        packed_w = got_w_f[...]
        for f in range(5):
            side_e = pltpu.roll(packed_e, LANES - HALO - HALO * f, 1)
            side_w = packed_w if f == 0 else pltpu.roll(packed_w, LANES - HALO * f, 1)
            value = fin[f, 0:ROWS]
            value = value + jnp.where(lane >= LANES - HALO, side_e, 0.0)
            value = value + jnp.where(lane < HALO, side_w, 0.0)
            state_out[f] = value
            state_out[f, 0:16] = state_out[f, 0:16] + got_s_f[f]
            state_out[f, 64:80] = state_out[f, 64:80] + got_n_f[f]
    finish_wind_send()
    finish_state_send()
    with jax.named_scope("sum_far"):
        part = end_far()
    total = jnp.sum(jnp.broadcast_to(part, (8, LANES)), axis=1, keepdims=True)[0:1]
    entries = 2 * ROWS * LANES * nx * ny
    inv = lax.rsqrt(total / entries + NORM_EPS)
    for i in range(2):
        wind_out[i] = wind_out[i] * inv


def writer(state, wind, state_hbm, wind_hbm, sem):
    pieces = [(state, state_hbm, f) for f in range(5)] + [(wind, wind_hbm, f) for f in range(2)]
    copies = [
        pltpu.make_async_copy(src.at[f], dst.at[f], sem.at[i])
        for i, (src, dst, f) in enumerate(pieces)
    ]
    for copy in copies:
        copy.start()
    for copy in copies:
        copy.wait()


def solution(mesh):
    nx, ny = mesh.shape["gx"], mesh.shape["gy"]

    def per_device(velocity, stress, wind, strength, mass, land, region, observed, start):
        vm = lambda *shape: pltpu.VMEM(shape, F32)
        dma = pltpu.SemaphoreType.DMA
        any_spec = pl.BlockSpec(memory_space=pl.ANY)
        args = (start, velocity, stress, wind, strength, mass, land, region, observed)
        args = [args[0]] + [pltpu.with_memory_space_constraint(z, pltpu.HBM) for z in args[1:]]
        shapes = (
            jax.ShapeDtypeStruct((5, ROWS, LANES), F32),
            jax.ShapeDtypeStruct((2, ROWS, LANES), F32),
        )
        vmem_spec = pl.BlockSpec(memory_space=pltpu.VMEM)
        state, gusts = pl.pallas_call(
            functools.partial(kernel, nx, ny),
            out_shape=shapes,
            in_specs=[pl.BlockSpec(memory_space=pltpu.SMEM)] + [any_spec] * 8,
            out_specs=(vmem_spec, vmem_spec),
            scratch_shapes=[
                vm(9, LANES, LANES),
                vm(ROWS, LANES),
                pltpu.VMEM((ROWS, LANES), jnp.int32),
                pltpu.VMEM((ROWS, LANES), jnp.int32),
                vm(3, LANES, LANES),
                vm(ROWS + HALO, LANES),
                vm(ROWS + HALO, LANES),
                vm(4, HALO + 8, LANES),
                vm(ROWS + HALO, LANES),
                vm(ROWS + HALO, LANES),
                vm(4, HALO + 8, LANES),
                vm(9, HALO, LANES),
                vm(2, HALO + 8, LANES),
                vm(5, TALL, LANES),
                vm(5, TALL, LANES),
                vm(STEPS, 4, TALL, LANES),
                vm(12, TALL, LANES),
                vm(5, LANES, LANES),
                vm(LANES, LANES),
                vm(LANES, LANES),
                vm(5, HALO, LANES),
                vm(5, HALO, LANES),
                vm(ROWS, LANES),
                vm(ROWS, LANES),
                vm(4, HALO, LANES),
                vm(2, TALL, LANES),
                vm(64, LANES),
                vm(2, 8, LANES),
                vm(2 * HALO, LANES),
                vm(2 * HALO, LANES),
                vm(2, HALO, LANES),
                vm(2, HALO, LANES),
                vm(4, 8, LANES),
                vm(2 * HALO, LANES),
                vm(2, 8, LANES),
                vm(nx // 2, 1, LANES),
                vm(2 * ny, 1, LANES),
                dma((9,)),
                dma((8,)),
                dma((8,)),
                dma((8,)),
                dma((8,)),
                dma((8,)),
                dma((8,)),
                dma((6,)),
                dma((nx // 2,)),
                dma((nx // 2,)),
                dma((2 * ny,)),
                dma((2 * ny,)),
            ],
            compiler_params=pltpu.CompilerParams(
                collective_id=0, has_side_effects=True, vmem_limit_bytes=32 * 1024 * 1024
            ),
        )(*args)
        return pl.pallas_call(
            writer,
            out_shape=shapes,
            in_specs=[vmem_spec, vmem_spec],
            out_specs=(any_spec, any_spec),
            scratch_shapes=[dma((7,))],
        )(
            pltpu.with_memory_space_constraint(state, pltpu.VMEM),
            pltpu.with_memory_space_constraint(gusts, pltpu.VMEM),
        )

    tri, two = P(None, "gy", "gx"), P("gy", "gx")
    return jax.shard_map(
        per_device,
        mesh=mesh,
        in_specs=(tri, tri, tri, two, two, two, two, tri, P()),
        out_specs=(tri, tri),
        check_vma=False,
    )
```

```python
import functools

import jax
import jax.numpy as jnp
from jax import lax
from jax.experimental import pallas as pl
from jax.experimental.pallas import tpu as pltpu
from jax.sharding import PartitionSpec as P

STEPS = 8
SUBTOTAL = 120
HALO = 2 * STEPS
LANES = 128
PAD = 8
CHUNK = 8
NORM_EPS = 1e-06
F32 = jnp.float32
MESH = pl.DeviceIdType.MESH

ROWS = 80
NORTH = slice(80, 96)
GAP = slice(96, 112)
SOUTH = slice(112, 128)
FIRST = PAD + HALO
LAST = FIRST + LANES
TALL = LAST + HALO + PAD
SIGNS = (-1.0, -1.0, 1.0, 1.0, 1.0, -1.0, -1.0, 1.0, 1.0)

N, S, E, W, NE, NW, SE, SW = range(8)


def flip_lanes(x, index):
    return jnp.take_along_axis(x, index, axis=1)


def flip_strip(strip, lane_index, sign):
    row_index = 7 - lax.broadcasted_iota(jnp.int32, (8, LANES), 0)
    upper = jnp.take_along_axis(strip[8:16], row_index, axis=0)
    lower = jnp.take_along_axis(strip[0:8], row_index, axis=0)
    upper = flip_lanes(upper, lane_index)
    lower = flip_lanes(lower, lane_index)
    return sign * upper, sign * lower


def kernel(
    nx,
    ny,
    start_ref,
    velocity,
    stress,
    wind,
    strength,
    mass,
    land,
    region,
    observed,
    state_out,
    wind_out,
    raw,
    mass_v,
    land_v,
    region_v,
    target,
    goal,
    bundle_e,
    bundle_w,
    corner_out,
    got_e,
    got_w,
    got_c,
    rev_n,
    rev_c,
    field,
    static,
    saved,
    back,
    fin,
    fin_e,
    fin_w,
    got_n_f,
    got_s_f,
    got_e_f,
    got_w_f,
    got_c_f,
    gust,
    gust_ns,
    gust_c,
    got_n_w,
    got_s_w,
    got_e_w,
    got_w_w,
    got_c_w,
    rev_n_w,
    rev_c_w,
    red_x,
    red_y,
    load_sem,
    send_sem,
    recv_sem,
    wsend_sem,
    wrecv_sem,
    fsend_sem,
    frecv_sem,
    self_sem,
    xs_sem,
    xr_sem,
    ys_sem,
    yr_sem,
):
    gx = lax.axis_index("gx")
    gy = lax.axis_index("gy")
    top = gy == ny - 1
    bottom = gy == 0
    not_top = gy < ny - 1
    not_bottom = gy > 0
    def wrap(index, count):
        return jnp.where(index >= count, index - count, index)

    east = wrap(gx + 1, nx)
    west = wrap(gx + nx - 1, nx)
    fold = nx - 1 - gx
    fold_e = wrap(2 * nx - 2 - gx, nx)
    fold_w = wrap(nx - gx, nx)

    def at(x, y):
        return {"gx": x, "gy": y}

    loads = [
        pltpu.make_async_copy(velocity, raw.at[0:2, 0:ROWS], load_sem.at[0]),
        pltpu.make_async_copy(stress, raw.at[2:5, 0:ROWS], load_sem.at[1]),
        pltpu.make_async_copy(wind, raw.at[5:7, 0:ROWS], load_sem.at[2]),
        pltpu.make_async_copy(strength, raw.at[7, 0:ROWS], load_sem.at[3]),
        pltpu.make_async_copy(mass, mass_v, load_sem.at[4]),
        pltpu.make_async_copy(land, land_v, load_sem.at[5]),
        pltpu.make_async_copy(region, region_v, load_sem.at[6]),
        pltpu.make_async_copy(observed, target.at[1:3, 0:ROWS], load_sem.at[7]),
    ]
    for copy in loads:
        copy.start()

    ring = lax.div(gx, 4)
    core = lax.rem(gx, 2)
    cross = lax.div(gx - 4 * ring - core, 2)
    rings = nx // 4
    near = ring * 2 + core
    far = cross * ny + gy
    nears, fars = 2 * rings, 2 * ny

    def near_at(d, sign=1):
        r = wrap(ring + (d // 2 if sign > 0 else rings - d // 2), rings) if d // 2 else ring
        c = 1 - core if d % 2 else core
        return r * 2 + c, at(r * 4 + cross * 2 + c, gy)

    def far_at(d, sign=1):
        y = wrap(gy + (d // 2 if sign > 0 else ny - d // 2), ny) if d // 2 else gy
        x = 1 - cross if d % 2 else cross
        return x * ny + y, at(gx + 2 * (x - cross), y)

    barrier = pltpu.get_barrier_semaphore()

    def greet(where):
        pl.semaphore_signal(barrier, inc=1, device_id=where, device_id_type=MESH)

    with jax.named_scope("greet"):
        greet(at(east, gy))
        greet(at(west, gy))

        @pl.when(not_top)
        def _():
            for x in (gx, east, west):
                greet(at(x, gy + 1))

        @pl.when(not_bottom)
        def _():
            for x in (gx, east, west):
                greet(at(x, gy - 1))

        @pl.when(top)
        def _():
            greet(at(fold, gy))

        @pl.when(top & (fold_e != gx))
        def _():
            greet(at(fold_e, gy))

        @pl.when(top & (fold_w != gx))
        def _():
            greet(at(fold_w, gy))

        for d in range(1, fars):
            greet(far_at(d)[1])
        for d in range(1, nears):
            greet(near_at(d)[1])

    zero_gap = jnp.zeros((HALO, LANES), F32)
    for f in range(9):
        raw[f, GAP] = zero_gap
    for f in range(3):
        target[f, ROWS:LANES] = jnp.zeros((LANES - ROWS, LANES), F32)
    zero_pad = jnp.zeros((PAD, LANES), F32)
    for f in range(5):
        field[f, 0:PAD] = zero_pad
        field[f, TALL - PAD : TALL] = zero_pad
    for f in range(12):
        back[f, 0:FIRST] = jnp.zeros((FIRST, LANES), F32)
        back[f, LAST:TALL] = jnp.zeros((FIRST, LANES), F32)
    for f in (4, 5, 6, 10, 11):
        back[f, FIRST:LAST] = jnp.zeros((LANES, LANES), F32)

    @pl.when(bottom)
    def _():
        for f in range(9):
            raw[f, SOUTH] = zero_gap
        for f in range(5):
            got_s_f[f] = zero_gap
        for i in (2, 3):
            got_c[i] = jnp.zeros((HALO + 8, LANES), F32)
            got_c_f[i] = zero_gap
            got_c_w[i] = jnp.zeros((8, LANES), F32)
        got_s_w[...] = jnp.zeros((2 * HALO, LANES), F32)

    for copy in loads:
        copy.wait()

    lane = lax.broadcasted_iota(jnp.int32, (ROWS, LANES), 1)
    lane16 = lax.broadcasted_iota(jnp.int32, (HALO, LANES), 1)
    lane8 = lax.broadcasted_iota(jnp.int32, (8, LANES), 1)
    whole_flip = LANES - 1 - lane8
    group_flip = lane8 + (HALO - 1) - 2 * lax.rem(lane8, HALO)
    group = lane8 // HALO
    group_sign = jnp.where((group < 2) | ((group >= 5) & (group < 7)), -1.0, 1.0)
    odd = lax.rem(group, 2) == 1

    def two_tiles(first, second):
        return jnp.where(odd, first, pltpu.roll(second, LANES - HALO, 1))

    spare_rows = jnp.zeros((LANES - ROWS, LANES), F32)

    with jax.named_scope("pack"):
        drag = land_v[...].astype(F32) * (0.5 / (mass_v[...] + 0.5))
        raw[8, 0:ROWS] = drag
        drag_t = jnp.transpose(jnp.concatenate([drag, spare_rows], axis=0))
        target[0, 0:ROWS] = region_v[...].astype(F32)
        packed_e = pltpu.roll(raw[0, 0:ROWS], HALO, 1)
        packed_w = raw[0, 0:ROWS]
        for f in range(1, 8):
            here = (lane >= HALO * f) & (lane < HALO * (f + 1))
            value = raw[f, 0:ROWS]
            packed_e = jnp.where(here, pltpu.roll(value, (HALO * f + HALO) % LANES, 1), packed_e)
            packed_w = jnp.where(here, pltpu.roll(value, HALO * f, 1), packed_w)
        sides = ((bundle_e, packed_e, drag_t[LANES - HALO :]), (bundle_w, packed_w, drag_t[:HALO]))
        strips = []
        for i, (bundle, packed, strip) in enumerate(sides):
            bundle[0:ROWS] = packed
            bundle[ROWS:] = strip
            upper, lower = pltpu.roll(strip, 48, 1), pltpu.roll(strip, 80, 1)
            strips.append(upper)
            corner_out[i, 0:HALO] = packed[64:80]
            corner_out[i, HALO:] = two_tiles(upper[0:8], upper[8:16])
            corner_out[2 + i, 0:HALO] = packed[0:16]
            corner_out[2 + i, HALO:] = two_tiles(lower[0:8], lower[8:16])

        @pl.when(top)
        def _():
            for f in range(9):
                rev_n[f, 0:8], rev_n[f, 8:16] = flip_strip(raw[f, 64:80], whole_flip, SIGNS[f])
            for i in range(2):
                rev_c[i, 0:8], rev_c[i, 8:16] = flip_strip(
                    corner_out[i, 0:HALO], group_flip, group_sign
                )
                upper, lower = flip_strip(strips[i], whole_flip, 1.0)
                rev_c[i, HALO:] = two_tiles(pltpu.roll(upper, 80, 1), pltpu.roll(lower, 80, 1))

    def remote(src, dst, send, recv, slot, x, y):
        return pltpu.make_async_remote_copy(
            src_ref=src,
            dst_ref=dst,
            send_sem=send.at[slot],
            recv_sem=recv.at[slot],
            device_id=at(x, y),
            device_id_type=MESH,
        )

    def exchange(turn, middle, late, send, recv, ns, e, w, corners, folded, slots):
        to_n, to_s = ns
        corner = {
            SW: (corners[0], east, gy + 1),
            SE: (corners[1], west, gy + 1),
            NW: (corners[2], east, gy - 1),
            NE: (corners[3], west, gy - 1),
        }

        def side_copies():
            return [
                remote(e, slots[W], send, recv, W, east, gy),
                remote(w, slots[E], send, recv, E, west, gy),
            ]

        def corner_copy(k):
            return remote(corner[k][0], slots[k], send, recv, k, *corner[k][1:])

        def corner_copies(kinds):
            return [corner_copy(k) for k in kinds]

        def north_copy():
            return remote(to_n, slots[S], send, recv, S, gx, gy + 1)

        def south_copy():
            return remote(to_s, slots[N], send, recv, N, gx, gy - 1)

        def north_copies():
            return [*corner_copies((SW, SE)), north_copy()]

        def south_copies():
            return [*corner_copies((NW, NE)), south_copy()]

        def fold_copy(k, src, slot, x):
            return pltpu.make_async_remote_copy(
                src_ref=src,
                dst_ref=slots[slot],
                send_sem=send.at[k],
                recv_sem=recv.at[slot],
                device_id=at(x, gy),
                device_id_type=MESH,
            )

        def local_copy(i, src, slot):
            return pltpu.make_async_copy(src, slots[slot], self_sem.at[2 * turn + i])

        fold_n = lambda: fold_copy(S, folded[0], N, fold)
        fold_ne = lambda: fold_copy(SW, folded[1], NE, fold_e)
        fold_nw = lambda: fold_copy(SE, folded[2], NW, fold_w)
        self_ne = lambda: local_copy(0, folded[1], NE)
        self_nw = lambda: local_copy(1, folded[2], NW)

        @pl.when(not_top)
        def _():
            for copy in corner_copies((SW, SE)):
                copy.start()

        @pl.when(not_bottom)
        def _():
            for copy in corner_copies((NW, NE)):
                copy.start()

        def fold_corners():
            @pl.when(top & (fold_e != gx))
            def _():
                fold_ne().start()

            @pl.when(top & (fold_e == gx))
            def _():
                self_ne().start()

            @pl.when(top & (fold_w != gx))
            def _():
                fold_nw().start()

            @pl.when(top & (fold_w == gx))
            def _():
                self_nw().start()

        def fold_rows():
            @pl.when(top)
            def _():
                fold_n().start()

        if late is None:
            fold_corners()
        for copy in side_copies():
            copy.start()
        if middle is not None:
            middle()
        if late is None:
            fold_rows()

        @pl.when(not_top)
        def _():
            north_copy().start()

        @pl.when(not_bottom)
        def _():
            south_copy().start()

        if late is not None:
            pl.when(top)(late)
            fold_corners()
            fold_rows()

        def finish_sides():
            for copy in side_copies():
                copy.wait_recv()

            @pl.when(not_bottom)
            def _():
                for copy in corner_copies((SW, SE)):
                    copy.wait_recv()

            @pl.when(not_top)
            def _():
                for copy in corner_copies((NW, NE)):
                    copy.wait_recv()

            @pl.when(top & (fold_e != gx))
            def _():
                fold_ne().wait_recv()

            @pl.when(top & (fold_e == gx))
            def _():
                self_ne().wait()

            @pl.when(top & (fold_w != gx))
            def _():
                fold_nw().wait_recv()

            @pl.when(top & (fold_w == gx))
            def _():
                self_nw().wait()

        def finish_rows():
            @pl.when(not_bottom)
            def _():
                north_copy().wait_recv()

            @pl.when(not_top)
            def _():
                south_copy().wait_recv()

            @pl.when(top)
            def _():
                fold_n().wait_recv()

        def finish_send():
            for copy in side_copies():
                copy.wait_send()

            @pl.when(not_top)
            def _():
                for copy in north_copies():
                    copy.wait_send()

            @pl.when(not_bottom)
            def _():
                for copy in south_copies():
                    copy.wait_send()

            @pl.when(top)
            def _():
                fold_n().wait_send()

            @pl.when(top & (fold_e != gx))
            def _():
                fold_ne().wait_send()

            @pl.when(top & (fold_w != gx))
            def _():
                fold_nw().wait_send()

        return finish_sides, finish_rows, finish_send

    peers = (nears - 1) + (fars - 1) + 2
    as_int = lambda flag: flag.astype(jnp.int32)
    peers = peers + 3 * as_int(not_top) + 3 * as_int(not_bottom) + as_int(top)
    peers = peers + as_int(top & (fold_e != gx)) + as_int(top & (fold_w != gx))
    with jax.named_scope("barrier"):
        pl.semaphore_wait(barrier, peers)

    finish_sides, finish_rows, finish_send = exchange(
        0,
        None,
        None,
        send_sem,
        recv_sem,
        (raw.at[:, 64:80], raw.at[:, 0:16]),
        bundle_e,
        bundle_w,
        tuple(corner_out.at[i] for i in range(4)),
        (rev_n, rev_c.at[0], rev_c.at[1]),
        {
            N: raw.at[:, NORTH],
            S: raw.at[:, SOUTH],
            E: got_e,
            W: got_w,
            NE: got_c.at[0],
            NW: got_c.at[1],
            SE: got_c.at[2],
            SW: got_c.at[3],
        },
    )
    for i in range(3):
        goal[i] = jnp.transpose(target[i])
    with jax.named_scope("recv_first"):
        finish_sides()

    centre = slice(FIRST, LAST)
    low = slice(PAD, FIRST)
    high = slice(LAST, LAST + HALO)

    def side(bundle, upper, lower):
        packed = [bundle[0:ROWS], upper[0:HALO], zero_gap, lower[0:HALO]]
        packed = jnp.transpose(jnp.concatenate(packed, axis=0))
        upper, lower = [
            jnp.concatenate([x[HALO:], pltpu.roll(x[HALO:], HALO, 1)], axis=0)
            for x in (upper, lower)
        ]
        strip = jnp.where(lane16 < 96, upper, jnp.where(lane16 >= 112, lower, 0.0))
        strip = jnp.where(lane16 < ROWS, bundle[ROWS:], strip)
        return [packed[HALO * f : HALO * (f + 1)] for f in range(8)] + [strip]

    def place(rows, parts):
        u, v, s1, s2, s12, wu, wv, strong, b = parts
        field[0, rows] = u
        field[1, rows] = v
        field[2, rows] = s1 + s2
        field[3, rows] = s1 - s2
        field[4, rows] = 2.0 * s12
        static[0, rows] = jnp.where(b > 0.0, 1.0, 0.0) - b
        static[1, rows] = 0.25 * b
        static[2, rows] = b * wu
        static[3, rows] = b * wv
        static[4, rows] = strong

    place(low, side(got_w, got_c.at[1], got_c.at[3]))
    place(high, side(got_e, got_c.at[0], got_c.at[2]))
    with jax.named_scope("recv_rows"):
        finish_rows()
    place(centre, [jnp.transpose(raw[f]) for f in range(9)])

    begin = start_ref[0].astype(F32)

    def coefs(k):
        step = jnp.full((CHUNK, LANES), begin + jnp.asarray(k + 1, jnp.int32).astype(F32), F32)
        coef = 0.2 + 0.8 * step / SUBTOTAL
        keep = 1.0 / (1.0 + coef)
        return coef, keep

    to_n = lambda x: pltpu.roll(x, LANES - 1, 1)
    to_s = lambda x: pltpu.roll(x, 1, 1)
    wide = range(PAD, TALL - PAD, CHUNK)
    narrow = range(PAD + 8, TALL - PAD - 8, CHUNK)

    def forward(chunks, k, carry):
        coef, keep = coefs(k)
        gain = coef * keep
        for r in chunks:
            rows = slice(r, r + CHUNK)
            up = slice(r + 1, r + 1 + CHUNK)
            down = slice(r - 1, r - 1 + CHUNK)
            u = field[0, rows]
            v = field[1, rows]
            x1 = field[0, up] - field[0, down]
            x2 = field[1, up] - field[1, down]
            y1 = to_n(u) - to_s(u)
            y2 = to_n(v) - to_s(v)
            div = x1 + y2
            ten = x1 - y2
            quarter = 0.25 * ten
            half = 0.5 * (y1 + x2)
            inv = lax.rsqrt(div * div + quarter * ten + half * half + 0.16)
            rate = gain * static[4, rows]
            un = (div + quarter) * inv
            vn = (div - quarter) * inv
            sn = half * inv
            saved[k, 0, rows] = un
            saved[k, 1, rows] = vn
            saved[k, 2, rows] = sn
            saved[k, 3, rows] = rate * inv
            field[2, rows] = keep * field[2, rows] + rate * (un - 1.0)
            field[3, rows] = keep * field[3, rows] + rate * (vn - 1.0)
            field[4, rows] = keep * field[4, rows] + rate * sn
        for r in chunks:
            rows = slice(r, r + CHUNK)
            up = slice(r + 1, r + 1 + CHUNK)
            down = slice(r - 1, r - 1 + CHUNK)
            m = field[3, rows]
            q = field[4, rows]
            fx = (field[2, up] - field[2, down]) + (to_n(q) - to_s(q))
            fy = (field[4, up] - field[4, down]) + (to_n(m) - to_s(m))
            field[0, rows] = static[0, rows] * field[0, rows] + (static[2, rows] + static[1, rows] * fx)
            field[1, rows] = static[0, rows] * field[1, rows] + (static[3, rows] + static[1, rows] * fy)
        return carry

    with jax.named_scope("forward"):
        lax.fori_loop(0, STEPS // 2, functools.partial(forward, wide), 0, unroll=4)
        lax.fori_loop(STEPS // 2, STEPS, functools.partial(forward, narrow), 0, unroll=4)

    for i in range(2):
        miss = goal[0] * (field[i, centre] - goal[1 + i])
        back[i, centre] = miss
        back[2 + i, centre] = static[1, centre] * miss

    def backward(chunks, last, i, carry):
        k = STEPS - 1 - i
        _, keep = coefs(k)
        for r in chunks:
            rows = slice(r, r + CHUNK)
            up = slice(r + 1, r + 1 + CHUNK)
            down = slice(r - 1, r - 1 + CHUNK)
            mu = back[2, rows]
            mv = back[3, rows]
            tp = back[4, rows] + (back[2, down] - back[2, up])
            tm = back[5, rows] + (to_s(mv) - to_n(mv))
            tq = back[6, rows] + ((to_s(mu) - to_n(mu)) + (back[3, down] - back[3, up]))
            un = saved[k, 0, rows]
            vn = saved[k, 1, rows]
            sn = saved[k, 2, rows]
            g = saved[k, 3, rows]
            along = tp * un + tm * vn + tq * sn
            total = tp + tm
            quarter = 0.25 * (tp - tm)
            back[7, rows] = g * ((total + quarter) - along * un)
            back[8, rows] = g * ((total - quarter) - along * vn)
            back[9, rows] = (0.5 * g) * (tq - along * sn)
            back[4, rows] = keep * tp
            back[5, rows] = keep * tm
            back[6, rows] = keep * tq
        for r in chunks:
            rows = slice(r, r + CHUNK)
            up = slice(r + 1, r + 1 + CHUNK)
            down = slice(r - 1, r - 1 + CHUNK)
            yb = back[8, rows]
            sb = back[9, rows]
            lu = back[0, rows]
            lv = back[1, rows]
            if not last:
                back[10, rows] = back[10, rows] + lu
                back[11, rows] = back[11, rows] + lv
            new_u = static[0, rows] * lu + ((back[7, down] - back[7, up]) + (to_s(sb) - to_n(sb)))
            new_v = static[0, rows] * lv + ((back[9, down] - back[9, up]) + (to_s(yb) - to_n(yb)))
            back[0, rows] = new_u
            back[1, rows] = new_v
            if not last:
                back[2, rows] = static[1, rows] * new_u
                back[3, rows] = static[1, rows] * new_v
        return carry

    with jax.named_scope("backward"):
        lax.fori_loop(0, STEPS // 2, functools.partial(backward, narrow, False), 0, unroll=4)
        lax.fori_loop(STEPS // 2, STEPS - 1, functools.partial(backward, wide, False), 0, unroll=3)

    def four_tiles(u0, u1, v0, v1):
        other = two_tiles(pltpu.roll(v0, 64, 1), pltpu.roll(v1, 64, 1))
        return jnp.where(lane8 >= 64, two_tiles(u0, u1), other)

    lane_all = lax.broadcasted_iota(jnp.int32, (LANES, LANES), 1)
    def gusts(rows):
        for i in range(2):
            gust[i, rows] = 4.0 * static[1, rows] * (back[10 + i, rows] + back[i, rows])

    with jax.named_scope("wind_pack"):
        gusts(high)
        gusts(low)
        for j, rows in ((0, high), (1, low)):
            u, v = gust[0, rows], gust[1, rows]
            gust_c[j] = four_tiles(u[0:8], u[8:16], v[0:8], v[8:16])

    def wind_rows():
        gusts(centre)
        here = ((lane_all >= 80) & (lane_all < 96)) | (lane_all >= 112)
        both = jnp.where(here, gust[0, centre], pltpu.roll(gust[1, centre], LANES - HALO, 1))
        gust_ns[...] = jnp.transpose(both)[64:LANES]

    def flip_index(shift):
        return lax.rem(2 * LANES - 1 + shift - lane8, LANES)

    def flip_wind():
        for i in range(2):
            part = slice(HALO * i, HALO * (i + 1))
            upper, lower = flip_strip(gust_ns[part], whole_flip, -1.0)
            rev_n_w[16 * i : 16 * i + 8] = upper
            rev_n_w[16 * i + 8 : 16 * i + 16] = lower
        row_flip = 7 - lax.broadcasted_iota(jnp.int32, (8, LANES), 0)
        for j, rows in ((0, high), (1, low)):
            tiles = []
            for i, shifts in ((0, (80, 64)), (1, (16, 0))):
                strip = gust[i, rows]
                for part, shift in zip((strip[8:16], strip[0:8]), shifts):
                    part = jnp.take_along_axis(part, row_flip, axis=0)
                    tiles.append(-flip_lanes(part, flip_index(shift)))
            pairs = [jnp.where(odd, tiles[2 * i], tiles[2 * i + 1]) for i in range(2)]
            rev_c_w[j] = jnp.where(lane8 >= 64, pairs[0], pairs[1])

    finish_wind_sides, finish_wind_rows, finish_wind_send = exchange(
        1,
        wind_rows,
        flip_wind,
        wsend_sem,
        wrecv_sem,
        (gust_ns.at[0:32], gust_ns.at[32:64]),
        gust.at[:, high],
        gust.at[:, low],
        (gust_c.at[0], gust_c.at[1], gust_c.at[0], gust_c.at[1]),
        (rev_n_w, rev_c_w.at[0], rev_c_w.at[1]),
        {
            N: got_n_w,
            S: got_s_w,
            E: got_e_w,
            W: got_w_w,
            NE: got_c_w.at[0],
            NW: got_c_w.at[1],
            SE: got_c_w.at[2],
            SW: got_c_w.at[3],
        },
    )
    with jax.named_scope("backward_last"):
        backward(wide, True, STEPS - 1, 0)
    finish_send()

    def result(rows):
        p = back[4, rows]
        m = back[5, rows]
        return [back[0, rows], back[1, rows], p + m, p - m, 2.0 * back[6, rows]]

    with jax.named_scope("state_pack"):
        for f, value in enumerate(result(centre)):
            fin[f] = jnp.transpose(value)
        for rows, dst in ((high, fin_e), (low, fin_w)):
            dst[...] = jnp.transpose(jnp.concatenate(result(rows) + [spare_rows], axis=0))

        @pl.when(top)
        def _():
            for f in range(5):
                rev_n[f, 0:8], rev_n[f, 8:16] = flip_strip(fin[f, NORTH], whole_flip, SIGNS[f])
            for i, src in ((0, fin_e), (1, fin_w)):
                rev_c[i, 0:8], rev_c[i, 8:16] = flip_strip(src[NORTH], group_flip, group_sign)

    with jax.named_scope("recv_wind"):
        finish_wind_sides()

    def with_sides(i):
        value = gust[i, centre]

        def ends(straight, upper, lower):
            extra = jnp.where(lane16 < ROWS, straight[i], 0.0)
            place = 64 * i
            upper = [pltpu.roll(upper[...], (80 - place + LANES + 16 * t) % LANES, 1) for t in (0, 1)]
            lower = [pltpu.roll(lower[...], (48 + place + 16 * t) % LANES, 1) for t in (0, 1)]
            upper, lower = jnp.concatenate(upper, axis=0), jnp.concatenate(lower, axis=0)
            extra = extra + jnp.where((lane16 >= 64) & (lane16 < ROWS), upper, 0.0)
            return extra + jnp.where(lane16 < HALO, lower, 0.0)

        at_w = ends(got_w_w, got_c_w.at[1], got_c_w.at[3])
        at_e = ends(got_e_w, got_c_w.at[0], got_c_w.at[2])
        parts = [value[:HALO] + at_w, value[HALO:-HALO], value[-HALO:] + at_e]
        return jnp.transpose(jnp.concatenate(parts, axis=0))[0:ROWS]

    with jax.named_scope("wind_add"):
        for i in range(2):
            wind_out[i] = with_sides(i)
    with jax.named_scope("recv_wind_rows"):
        finish_wind_rows()
    with jax.named_scope("squares"):
        for i in range(2):
            rows = slice(HALO * (1 - i), HALO * (2 - i))
            wind_out[i, 0:16] = wind_out[i, 0:16] + got_s_w[rows]
            wind_out[i, 64:80] = wind_out[i, 64:80] + got_n_w[rows]
        squares = wind_out[0] * wind_out[0] + wind_out[1] * wind_out[1]
        part = jnp.sum(squares, axis=0, keepdims=True)

    def all_sum(buf, send, recv, count, me, where):
        def copy_of(d, slot):
            return pltpu.make_async_remote_copy(
                src_ref=buf.at[me],
                dst_ref=buf.at[slot],
                send_sem=send.at[d],
                recv_sem=recv.at[d],
                device_id=where(d)[1],
                device_id_type=MESH,
            )

        def copies():
            return [copy_of(d, me) for d in range(1, count)]

        def arrivals():
            return [copy_of(d, where(d, -1)[0]) for d in range(1, count)]

        def begin_sum(part):
            buf[me] = part
            for copy in copies():
                copy.start()

        def end_sum():
            for copy in arrivals():
                copy.wait_recv()
            for copy in copies():
                copy.wait_send()
            return jnp.sum(buf[...], axis=0)

        return begin_sum, end_sum

    begin_near, end_near = all_sum(red_x, xs_sem, xr_sem, nears, near, near_at)
    begin_far, end_far = all_sum(red_y, ys_sem, yr_sem, fars, far, far_at)
    begin_near(part)
    finish_state_sides, finish_state_rows, finish_state_send = exchange(
        2,
        None,
        None,
        fsend_sem,
        frecv_sem,
        (fin.at[:, NORTH], fin.at[:, SOUTH]),
        fin_e.at[0:ROWS],
        fin_w.at[0:ROWS],
        (fin_e.at[NORTH], fin_w.at[NORTH], fin_e.at[SOUTH], fin_w.at[SOUTH]),
        (rev_n.at[0:5], rev_c.at[0, 0:HALO], rev_c.at[1, 0:HALO]),
        {
            N: got_n_f,
            S: got_s_f,
            E: got_e_f,
            W: got_w_f,
            NE: got_c_f.at[0],
            NW: got_c_f.at[1],
            SE: got_c_f.at[2],
            SW: got_c_f.at[3],
        },
    )
    with jax.named_scope("sum_near"):
        part = end_near()
    begin_far(part)
    with jax.named_scope("recv_state"):
        finish_state_sides()
        finish_state_rows()
    with jax.named_scope("state_add"):
        got_e_f[64:80] = got_e_f[64:80] + got_c_f[0]
        got_w_f[64:80] = got_w_f[64:80] + got_c_f[1]
        got_e_f[0:16] = got_e_f[0:16] + got_c_f[2]
        got_w_f[0:16] = got_w_f[0:16] + got_c_f[3]
        packed_e = got_e_f[...]
        packed_w = got_w_f[...]
        for f in range(5):
            side_e = pltpu.roll(packed_e, LANES - HALO - HALO * f, 1)
            side_w = packed_w if f == 0 else pltpu.roll(packed_w, LANES - HALO * f, 1)
            value = fin[f, 0:ROWS]
            value = value + jnp.where(lane >= LANES - HALO, side_e, 0.0)
            value = value + jnp.where(lane < HALO, side_w, 0.0)
            state_out[f] = value
            state_out[f, 0:16] = state_out[f, 0:16] + got_s_f[f]
            state_out[f, 64:80] = state_out[f, 64:80] + got_n_f[f]
    finish_wind_send()
    finish_state_send()
    with jax.named_scope("sum_far"):
        part = end_far()
    total = jnp.sum(jnp.broadcast_to(part, (8, LANES)), axis=1, keepdims=True)[0:1]
    entries = 2 * ROWS * LANES * nx * ny
    inv = lax.rsqrt(total / entries + NORM_EPS)
    for i in range(2):
        wind_out[i] = wind_out[i] * inv


def writer(state, wind, state_hbm, wind_hbm, sem):
    pieces = [(state, state_hbm, f) for f in range(5)] + [(wind, wind_hbm, f) for f in range(2)]
    copies = [
        pltpu.make_async_copy(src.at[f], dst.at[f], sem.at[i])
        for i, (src, dst, f) in enumerate(pieces)
    ]
    for copy in copies:
        copy.start()
    for copy in copies:
        copy.wait()


def solution(mesh):
    nx, ny = mesh.shape["gx"], mesh.shape["gy"]

    def per_device(velocity, stress, wind, strength, mass, land, region, observed, start):
        vm = lambda *shape: pltpu.VMEM(shape, F32)
        dma = pltpu.SemaphoreType.DMA
        any_spec = pl.BlockSpec(memory_space=pl.ANY)
        args = (start, velocity, stress, wind, strength, mass, land, region, observed)
        args = [args[0]] + [pltpu.with_memory_space_constraint(z, pltpu.HBM) for z in args[1:]]
        shapes = (
            jax.ShapeDtypeStruct((5, ROWS, LANES), F32),
            jax.ShapeDtypeStruct((2, ROWS, LANES), F32),
        )
        vmem_spec = pl.BlockSpec(memory_space=pltpu.VMEM)
        state, gusts = pl.pallas_call(
            functools.partial(kernel, nx, ny),
            out_shape=shapes,
            in_specs=[pl.BlockSpec(memory_space=pltpu.SMEM)] + [any_spec] * 8,
            out_specs=(vmem_spec, vmem_spec),
            scratch_shapes=[
                vm(9, LANES, LANES),
                vm(ROWS, LANES),
                pltpu.VMEM((ROWS, LANES), jnp.int32),
                pltpu.VMEM((ROWS, LANES), jnp.int32),
                vm(3, LANES, LANES),
                vm(3, LANES, LANES),
                vm(ROWS + HALO, LANES),
                vm(ROWS + HALO, LANES),
                vm(4, HALO + 8, LANES),
                vm(ROWS + HALO, LANES),
                vm(ROWS + HALO, LANES),
                vm(4, HALO + 8, LANES),
                vm(9, HALO, LANES),
                vm(2, HALO + 8, LANES),
                vm(5, TALL, LANES),
                vm(5, TALL, LANES),
                vm(STEPS, 4, TALL, LANES),
                vm(12, TALL, LANES),
                vm(5, LANES, LANES),
                vm(LANES, LANES),
                vm(LANES, LANES),
                vm(5, HALO, LANES),
                vm(5, HALO, LANES),
                vm(ROWS, LANES),
                vm(ROWS, LANES),
                vm(4, HALO, LANES),
                vm(2, TALL, LANES),
                vm(64, LANES),
                vm(2, 8, LANES),
                vm(2 * HALO, LANES),
                vm(2 * HALO, LANES),
                vm(2, HALO, LANES),
                vm(2, HALO, LANES),
                vm(4, 8, LANES),
                vm(2 * HALO, LANES),
                vm(2, 8, LANES),
                vm(nx // 2, 1, LANES),
                vm(2 * ny, 1, LANES),
                dma((9,)),
                dma((8,)),
                dma((8,)),
                dma((8,)),
                dma((8,)),
                dma((8,)),
                dma((8,)),
                dma((6,)),
                dma((nx // 2,)),
                dma((nx // 2,)),
                dma((2 * ny,)),
                dma((2 * ny,)),
            ],
            compiler_params=pltpu.CompilerParams(
                collective_id=0, has_side_effects=True, vmem_limit_bytes=32 * 1024 * 1024
            ),
        )(*args)
        return pl.pallas_call(
            writer,
            out_shape=shapes,
            in_specs=[vmem_spec, vmem_spec],
            out_specs=(any_spec, any_spec),
            scratch_shapes=[dma((7,))],
        )(
            pltpu.with_memory_space_constraint(state, pltpu.VMEM),
            pltpu.with_memory_space_constraint(gusts, pltpu.VMEM),
        )

    tri, two = P(None, "gy", "gx"), P("gy", "gx")
    return jax.shard_map(
        per_device,
        mesh=mesh,
        in_specs=(tri, tri, tri, two, two, two, two, tri, P()),
        out_specs=(tri, tri),
        check_vma=False,
    )
```

```python
import functools

import jax
import jax.numpy as jnp
from jax import lax
from jax.experimental import pallas as pl
from jax.experimental.pallas import tpu as pltpu
from jax.sharding import PartitionSpec as P

STEPS = 8
SUBTOTAL = 120
HALO = 2 * STEPS
LANES = 128
PAD = 8
CHUNK = 8
NORM_EPS = 1e-06
F32 = jnp.float32
MESH = pl.DeviceIdType.MESH

ROWS = 80
NORTH = slice(80, 96)
GAP = slice(96, 112)
SOUTH = slice(112, 128)
FIRST = PAD + HALO
LAST = FIRST + LANES
TALL = LAST + HALO + PAD
SIGNS = (-1.0, -1.0, 1.0, 1.0, 1.0, -1.0, -1.0, 1.0, 1.0)

N, S, E, W, NE, NW, SE, SW = range(8)


def flip_lanes(x, index):
    return jnp.take_along_axis(x, index, axis=1)


def flip_strip(strip, lane_index, sign):
    row_index = 7 - lax.broadcasted_iota(jnp.int32, (8, LANES), 0)
    upper = jnp.take_along_axis(strip[8:16], row_index, axis=0)
    lower = jnp.take_along_axis(strip[0:8], row_index, axis=0)
    upper = flip_lanes(upper, lane_index)
    lower = flip_lanes(lower, lane_index)
    return sign * upper, sign * lower


def kernel(
    nx,
    ny,
    start_ref,
    velocity,
    stress,
    wind,
    strength,
    mass,
    land,
    region,
    observed,
    state_out,
    wind_out,
    raw,
    mass_v,
    land_v,
    region_v,
    target,
    goal,
    bundle_e,
    bundle_w,
    corner_out,
    got_e,
    got_w,
    got_c,
    rev_n,
    rev_c,
    field,
    static,
    saved,
    back,
    fin,
    fin_e,
    fin_w,
    got_n_f,
    got_s_f,
    got_e_f,
    got_w_f,
    got_c_f,
    gust,
    gust_ns,
    gust_c,
    got_n_w,
    got_s_w,
    got_e_w,
    got_w_w,
    got_c_w,
    rev_n_w,
    rev_c_w,
    red,
    load_sem,
    send_sem,
    recv_sem,
    wsend_sem,
    wrecv_sem,
    fsend_sem,
    frecv_sem,
    self_sem,
    sum_sem,
    ready,
):
    gx = lax.axis_index("gx")
    gy = lax.axis_index("gy")
    top = gy == ny - 1
    bottom = gy == 0
    not_top = gy < ny - 1
    not_bottom = gy > 0
    def wrap(index, count):
        return jnp.where(index >= count, index - count, index)

    east = wrap(gx + 1, nx)
    west = wrap(gx + nx - 1, nx)
    fold = nx - 1 - gx
    fold_e = wrap(2 * nx - 2 - gx, nx)
    fold_w = wrap(nx - gx, nx)

    def at(x, y):
        return {"gx": x, "gy": y}

    loads = [
        pltpu.make_async_copy(velocity, raw.at[0:2, 0:ROWS], load_sem.at[0]),
        pltpu.make_async_copy(stress, raw.at[2:5, 0:ROWS], load_sem.at[1]),
        pltpu.make_async_copy(wind, raw.at[5:7, 0:ROWS], load_sem.at[2]),
        pltpu.make_async_copy(strength, raw.at[7, 0:ROWS], load_sem.at[3]),
        pltpu.make_async_copy(mass, mass_v, load_sem.at[4]),
        pltpu.make_async_copy(land, land_v, load_sem.at[5]),
        pltpu.make_async_copy(region, region_v, load_sem.at[6]),
        pltpu.make_async_copy(observed, target.at[1:3, 0:ROWS], load_sem.at[7]),
    ]
    for copy in loads:
        copy.start()

    ring = lax.div(gx, 4)
    core = lax.rem(gx, 2)
    cross = lax.div(gx - 4 * ring - core, 2)
    rings = nx // 4
    near = ring * 2 + core
    far = cross * ny + gy
    nears, fars = 2 * rings, 2 * ny
    everyone = nx * ny
    me = gx * ny + gy

    def near_at(d, sign=1):
        r = wrap(ring + (d // 2 if sign > 0 else rings - d // 2), rings) if d // 2 else ring
        c = 1 - core if d % 2 else core
        return r * 2 + c, at(r * 4 + cross * 2 + c, gy)

    def far_at(d, sign=1):
        y = wrap(gy + (d // 2 if sign > 0 else ny - d // 2), ny) if d // 2 else gy
        x = 1 - cross if d % 2 else cross
        return x * ny + y, at(gx + 2 * (x - cross), y)

    barrier = pltpu.get_barrier_semaphore()

    def greet(where):
        pl.semaphore_signal(barrier, inc=1, device_id=where, device_id_type=MESH)

    with jax.named_scope("greet"):
        greet(at(east, gy))
        greet(at(west, gy))

        @pl.when(not_top)
        def _():
            for x in (gx, east, west):
                greet(at(x, gy + 1))

        @pl.when(not_bottom)
        def _():
            for x in (gx, east, west):
                greet(at(x, gy - 1))

        @pl.when(top)
        def _():
            greet(at(fold, gy))

        @pl.when(top & (fold_e != gx))
        def _():
            greet(at(fold_e, gy))

        @pl.when(top & (fold_w != gx))
        def _():
            greet(at(fold_w, gy))

        for d in range(1, fars):
            greet(far_at(d)[1])
        for d in range(1, nears):
            greet(near_at(d)[1])

    zero_gap = jnp.zeros((HALO, LANES), F32)
    for f in range(9):
        raw[f, GAP] = zero_gap
    for f in range(3):
        target[f, ROWS:LANES] = jnp.zeros((LANES - ROWS, LANES), F32)
    zero_pad = jnp.zeros((PAD, LANES), F32)
    for f in range(5):
        field[f, 0:PAD] = zero_pad
        field[f, TALL - PAD : TALL] = zero_pad
    for f in range(12):
        back[f, 0:FIRST] = jnp.zeros((FIRST, LANES), F32)
        back[f, LAST:TALL] = jnp.zeros((FIRST, LANES), F32)
    for f in (4, 5, 6, 10, 11):
        back[f, FIRST:LAST] = jnp.zeros((LANES, LANES), F32)

    @pl.when(bottom)
    def _():
        for f in range(9):
            raw[f, SOUTH] = zero_gap
        for f in range(5):
            got_s_f[f] = zero_gap
        for i in (2, 3):
            got_c[i] = jnp.zeros((HALO + 8, LANES), F32)
            got_c_f[i] = zero_gap
            got_c_w[i] = jnp.zeros((8, LANES), F32)
        got_s_w[...] = jnp.zeros((2 * HALO, LANES), F32)

    for copy in loads:
        copy.wait()

    lane = lax.broadcasted_iota(jnp.int32, (ROWS, LANES), 1)
    lane16 = lax.broadcasted_iota(jnp.int32, (HALO, LANES), 1)
    lane8 = lax.broadcasted_iota(jnp.int32, (8, LANES), 1)
    whole_flip = LANES - 1 - lane8
    group_flip = lane8 + (HALO - 1) - 2 * lax.rem(lane8, HALO)
    group = lane8 // HALO
    group_sign = jnp.where((group < 2) | ((group >= 5) & (group < 7)), -1.0, 1.0)
    odd = lax.rem(group, 2) == 1

    def two_tiles(first, second):
        return jnp.where(odd, first, pltpu.roll(second, LANES - HALO, 1))

    spare_rows = jnp.zeros((LANES - ROWS, LANES), F32)

    with jax.named_scope("pack"):
        drag = land_v[...].astype(F32) * (0.5 / (mass_v[...] + 0.5))
        raw[8, 0:ROWS] = drag
        drag_t = jnp.transpose(jnp.concatenate([drag, spare_rows], axis=0))
        target[0, 0:ROWS] = region_v[...].astype(F32)
        packed_e = pltpu.roll(raw[0, 0:ROWS], HALO, 1)
        packed_w = raw[0, 0:ROWS]
        for f in range(1, 8):
            here = (lane >= HALO * f) & (lane < HALO * (f + 1))
            value = raw[f, 0:ROWS]
            packed_e = jnp.where(here, pltpu.roll(value, (HALO * f + HALO) % LANES, 1), packed_e)
            packed_w = jnp.where(here, pltpu.roll(value, HALO * f, 1), packed_w)
        sides = ((bundle_e, packed_e, drag_t[LANES - HALO :]), (bundle_w, packed_w, drag_t[:HALO]))
        strips = []
        for i, (bundle, packed, strip) in enumerate(sides):
            bundle[0:ROWS] = packed
            bundle[ROWS:] = strip
            upper, lower = pltpu.roll(strip, 48, 1), pltpu.roll(strip, 80, 1)
            strips.append(upper)
            corner_out[i, 0:HALO] = packed[64:80]
            corner_out[i, HALO:] = two_tiles(upper[0:8], upper[8:16])
            corner_out[2 + i, 0:HALO] = packed[0:16]
            corner_out[2 + i, HALO:] = two_tiles(lower[0:8], lower[8:16])

        @pl.when(top)
        def _():
            for f in range(9):
                rev_n[f, 0:8], rev_n[f, 8:16] = flip_strip(raw[f, 64:80], whole_flip, SIGNS[f])
            for i in range(2):
                rev_c[i, 0:8], rev_c[i, 8:16] = flip_strip(
                    corner_out[i, 0:HALO], group_flip, group_sign
                )
                upper, lower = flip_strip(strips[i], whole_flip, 1.0)
                rev_c[i, HALO:] = two_tiles(pltpu.roll(upper, 80, 1), pltpu.roll(lower, 80, 1))

    def remote(src, dst, send, recv, slot, x, y):
        return pltpu.make_async_remote_copy(
            src_ref=src,
            dst_ref=dst,
            send_sem=send.at[slot],
            recv_sem=recv.at[slot],
            device_id=at(x, y),
            device_id_type=MESH,
        )

    def exchange(turn, middle, late, send, recv, ns, e, w, corners, folded, slots):
        to_n, to_s = ns
        corner = {
            SW: (corners[0], east, gy + 1),
            SE: (corners[1], west, gy + 1),
            NW: (corners[2], east, gy - 1),
            NE: (corners[3], west, gy - 1),
        }

        def side_copies():
            return [
                remote(e, slots[W], send, recv, W, east, gy),
                remote(w, slots[E], send, recv, E, west, gy),
            ]

        def corner_copy(k):
            return remote(corner[k][0], slots[k], send, recv, k, *corner[k][1:])

        def corner_copies(kinds):
            return [corner_copy(k) for k in kinds]

        def north_copy():
            return remote(to_n, slots[S], send, recv, S, gx, gy + 1)

        def south_copy():
            return remote(to_s, slots[N], send, recv, N, gx, gy - 1)

        def north_copies():
            return [*corner_copies((SW, SE)), north_copy()]

        def south_copies():
            return [*corner_copies((NW, NE)), south_copy()]

        def fold_copy(k, src, slot, x):
            return pltpu.make_async_remote_copy(
                src_ref=src,
                dst_ref=slots[slot],
                send_sem=send.at[k],
                recv_sem=recv.at[slot],
                device_id=at(x, gy),
                device_id_type=MESH,
            )

        def local_copy(i, src, slot):
            return pltpu.make_async_copy(src, slots[slot], self_sem.at[2 * turn + i])

        fold_n = lambda: fold_copy(S, folded[0], N, fold)
        fold_ne = lambda: fold_copy(SW, folded[1], NE, fold_e)
        fold_nw = lambda: fold_copy(SE, folded[2], NW, fold_w)
        self_ne = lambda: local_copy(0, folded[1], NE)
        self_nw = lambda: local_copy(1, folded[2], NW)

        @pl.when(not_top)
        def _():
            for copy in corner_copies((SW, SE)):
                copy.start()

        @pl.when(not_bottom)
        def _():
            for copy in corner_copies((NW, NE)):
                copy.start()

        def fold_corners():
            @pl.when(top & (fold_e != gx))
            def _():
                fold_ne().start()

            @pl.when(top & (fold_e == gx))
            def _():
                self_ne().start()

            @pl.when(top & (fold_w != gx))
            def _():
                fold_nw().start()

            @pl.when(top & (fold_w == gx))
            def _():
                self_nw().start()

        def fold_rows():
            @pl.when(top)
            def _():
                fold_n().start()

        if late is None:
            fold_corners()
        for copy in side_copies():
            copy.start()
        if middle is not None:
            middle()
        if late is None:
            fold_rows()

        @pl.when(not_top)
        def _():
            north_copy().start()

        @pl.when(not_bottom)
        def _():
            south_copy().start()

        if late is not None:
            pl.when(top)(late)
            fold_corners()
            fold_rows()

        def finish_sides():
            for copy in side_copies():
                copy.wait_recv()

            @pl.when(not_bottom)
            def _():
                for copy in corner_copies((SW, SE)):
                    copy.wait_recv()

            @pl.when(not_top)
            def _():
                for copy in corner_copies((NW, NE)):
                    copy.wait_recv()

            @pl.when(top & (fold_e != gx))
            def _():
                fold_ne().wait_recv()

            @pl.when(top & (fold_e == gx))
            def _():
                self_ne().wait()

            @pl.when(top & (fold_w != gx))
            def _():
                fold_nw().wait_recv()

            @pl.when(top & (fold_w == gx))
            def _():
                self_nw().wait()

        def finish_rows():
            @pl.when(not_bottom)
            def _():
                north_copy().wait_recv()

            @pl.when(not_top)
            def _():
                south_copy().wait_recv()

            @pl.when(top)
            def _():
                fold_n().wait_recv()

        def finish_send():
            for copy in side_copies():
                copy.wait_send()

            @pl.when(not_top)
            def _():
                for copy in north_copies():
                    copy.wait_send()

            @pl.when(not_bottom)
            def _():
                for copy in south_copies():
                    copy.wait_send()

            @pl.when(top)
            def _():
                fold_n().wait_send()

            @pl.when(top & (fold_e != gx))
            def _():
                fold_ne().wait_send()

            @pl.when(top & (fold_w != gx))
            def _():
                fold_nw().wait_send()

        return finish_sides, finish_rows, finish_send

    peers = (nears - 1) + (fars - 1) + 2
    as_int = lambda flag: flag.astype(jnp.int32)
    peers = peers + 3 * as_int(not_top) + 3 * as_int(not_bottom) + as_int(top)
    peers = peers + as_int(top & (fold_e != gx)) + as_int(top & (fold_w != gx))
    with jax.named_scope("barrier"):
        pl.semaphore_wait(barrier, peers)

    finish_sides, finish_rows, finish_send = exchange(
        0,
        None,
        None,
        send_sem,
        recv_sem,
        (raw.at[:, 64:80], raw.at[:, 0:16]),
        bundle_e,
        bundle_w,
        tuple(corner_out.at[i] for i in range(4)),
        (rev_n, rev_c.at[0], rev_c.at[1]),
        {
            N: raw.at[:, NORTH],
            S: raw.at[:, SOUTH],
            E: got_e,
            W: got_w,
            NE: got_c.at[0],
            NW: got_c.at[1],
            SE: got_c.at[2],
            SW: got_c.at[3],
        },
    )
    for d in range(1, nears):
        pl.semaphore_signal(ready, inc=1, device_id=near_at(d)[1], device_id_type=MESH)
    for i in range(3):
        goal[i] = jnp.transpose(target[i])
    with jax.named_scope("recv_first"):
        finish_sides()

    centre = slice(FIRST, LAST)
    low = slice(PAD, FIRST)
    high = slice(LAST, LAST + HALO)

    def side(bundle, upper, lower):
        packed = [bundle[0:ROWS], upper[0:HALO], zero_gap, lower[0:HALO]]
        packed = jnp.transpose(jnp.concatenate(packed, axis=0))
        upper, lower = [
            jnp.concatenate([x[HALO:], pltpu.roll(x[HALO:], HALO, 1)], axis=0)
            for x in (upper, lower)
        ]
        strip = jnp.where(lane16 < 96, upper, jnp.where(lane16 >= 112, lower, 0.0))
        strip = jnp.where(lane16 < ROWS, bundle[ROWS:], strip)
        return [packed[HALO * f : HALO * (f + 1)] for f in range(8)] + [strip]

    def place(rows, parts):
        u, v, s1, s2, s12, wu, wv, strong, b = parts
        field[0, rows] = u
        field[1, rows] = v
        field[2, rows] = s1 + s2
        field[3, rows] = s1 - s2
        field[4, rows] = 2.0 * s12
        static[0, rows] = jnp.where(b > 0.0, 1.0, 0.0) - b
        static[1, rows] = 0.25 * b
        static[2, rows] = b * wu
        static[3, rows] = b * wv
        static[4, rows] = strong

    place(low, side(got_w, got_c.at[1], got_c.at[3]))
    place(high, side(got_e, got_c.at[0], got_c.at[2]))
    with jax.named_scope("recv_rows"):
        finish_rows()
    place(centre, [jnp.transpose(raw[f]) for f in range(9)])

    begin = start_ref[0].astype(F32)

    def coefs(k):
        step = jnp.full((CHUNK, LANES), begin + jnp.asarray(k + 1, jnp.int32).astype(F32), F32)
        coef = 0.2 + 0.8 * step / SUBTOTAL
        keep = 1.0 / (1.0 + coef)
        return coef, keep

    to_n = lambda x: pltpu.roll(x, LANES - 1, 1)
    to_s = lambda x: pltpu.roll(x, 1, 1)
    wide = range(PAD, TALL - PAD, CHUNK)
    narrow = range(PAD + 8, TALL - PAD - 8, CHUNK)

    def forward(chunks, k, carry):
        coef, keep = coefs(k)
        gain = coef * keep
        for r in chunks:
            rows = slice(r, r + CHUNK)
            up = slice(r + 1, r + 1 + CHUNK)
            down = slice(r - 1, r - 1 + CHUNK)
            u = field[0, rows]
            v = field[1, rows]
            x1 = field[0, up] - field[0, down]
            x2 = field[1, up] - field[1, down]
            y1 = to_n(u) - to_s(u)
            y2 = to_n(v) - to_s(v)
            div = x1 + y2
            ten = x1 - y2
            quarter = 0.25 * ten
            half = 0.5 * (y1 + x2)
            inv = lax.rsqrt(div * div + quarter * ten + half * half + 0.16)
            rate = gain * static[4, rows]
            un = (div + quarter) * inv
            vn = (div - quarter) * inv
            sn = half * inv
            saved[k, 0, rows] = un
            saved[k, 1, rows] = vn
            saved[k, 2, rows] = sn
            saved[k, 3, rows] = rate * inv
            field[2, rows] = keep * field[2, rows] + rate * (un - 1.0)
            field[3, rows] = keep * field[3, rows] + rate * (vn - 1.0)
            field[4, rows] = keep * field[4, rows] + rate * sn
        for r in chunks:
            rows = slice(r, r + CHUNK)
            up = slice(r + 1, r + 1 + CHUNK)
            down = slice(r - 1, r - 1 + CHUNK)
            m = field[3, rows]
            q = field[4, rows]
            fx = (field[2, up] - field[2, down]) + (to_n(q) - to_s(q))
            fy = (field[4, up] - field[4, down]) + (to_n(m) - to_s(m))
            field[0, rows] = static[0, rows] * field[0, rows] + (static[2, rows] + static[1, rows] * fx)
            field[1, rows] = static[0, rows] * field[1, rows] + (static[3, rows] + static[1, rows] * fy)
        return carry

    with jax.named_scope("forward"):
        lax.fori_loop(0, STEPS // 2, functools.partial(forward, wide), 0, unroll=4)
        lax.fori_loop(STEPS // 2, STEPS, functools.partial(forward, narrow), 0, unroll=4)

    for i in range(2):
        miss = goal[0] * (field[i, centre] - goal[1 + i])
        back[i, centre] = miss
        back[2 + i, centre] = static[1, centre] * miss

    def backward(chunks, last, i, carry):
        k = STEPS - 1 - i
        _, keep = coefs(k)
        for r in chunks:
            rows = slice(r, r + CHUNK)
            up = slice(r + 1, r + 1 + CHUNK)
            down = slice(r - 1, r - 1 + CHUNK)
            mu = back[2, rows]
            mv = back[3, rows]
            tp = back[4, rows] + (back[2, down] - back[2, up])
            tm = back[5, rows] + (to_s(mv) - to_n(mv))
            tq = back[6, rows] + ((to_s(mu) - to_n(mu)) + (back[3, down] - back[3, up]))
            un = saved[k, 0, rows]
            vn = saved[k, 1, rows]
            sn = saved[k, 2, rows]
            g = saved[k, 3, rows]
            along = tp * un + tm * vn + tq * sn
            total = tp + tm
            quarter = 0.25 * (tp - tm)
            back[7, rows] = g * ((total + quarter) - along * un)
            back[8, rows] = g * ((total - quarter) - along * vn)
            back[9, rows] = (0.5 * g) * (tq - along * sn)
            back[4, rows] = keep * tp
            back[5, rows] = keep * tm
            back[6, rows] = keep * tq
        for r in chunks:
            rows = slice(r, r + CHUNK)
            up = slice(r + 1, r + 1 + CHUNK)
            down = slice(r - 1, r - 1 + CHUNK)
            yb = back[8, rows]
            sb = back[9, rows]
            lu = back[0, rows]
            lv = back[1, rows]
            if not last:
                back[10, rows] = back[10, rows] + lu
                back[11, rows] = back[11, rows] + lv
            new_u = static[0, rows] * lu + ((back[7, down] - back[7, up]) + (to_s(sb) - to_n(sb)))
            new_v = static[0, rows] * lv + ((back[9, down] - back[9, up]) + (to_s(yb) - to_n(yb)))
            back[0, rows] = new_u
            back[1, rows] = new_v
            if not last:
                back[2, rows] = static[1, rows] * new_u
                back[3, rows] = static[1, rows] * new_v
        return carry

    with jax.named_scope("backward"):
        lax.fori_loop(0, STEPS // 2, functools.partial(backward, narrow, False), 0, unroll=4)
        lax.fori_loop(STEPS // 2, STEPS - 1, functools.partial(backward, wide, False), 0, unroll=3)

    def four_tiles(u0, u1, v0, v1):
        other = two_tiles(pltpu.roll(v0, 64, 1), pltpu.roll(v1, 64, 1))
        return jnp.where(lane8 >= 64, two_tiles(u0, u1), other)

    lane_all = lax.broadcasted_iota(jnp.int32, (LANES, LANES), 1)
    def gusts(rows):
        for i in range(2):
            gust[i, rows] = 4.0 * static[1, rows] * (back[10 + i, rows] + back[i, rows])

    with jax.named_scope("wind_pack"):
        gusts(high)
        gusts(low)
        for j, rows in ((0, high), (1, low)):
            u, v = gust[0, rows], gust[1, rows]
            gust_c[j] = four_tiles(u[0:8], u[8:16], v[0:8], v[8:16])

    def wind_rows():
        gusts(centre)
        here = ((lane_all >= 80) & (lane_all < 96)) | (lane_all >= 112)
        both = jnp.where(here, gust[0, centre], pltpu.roll(gust[1, centre], LANES - HALO, 1))
        gust_ns[...] = jnp.transpose(both)[64:LANES]

    def flip_index(shift):
        return lax.rem(2 * LANES - 1 + shift - lane8, LANES)

    def flip_wind():
        for i in range(2):
            part = slice(HALO * i, HALO * (i + 1))
            upper, lower = flip_strip(gust_ns[part], whole_flip, -1.0)
            rev_n_w[16 * i : 16 * i + 8] = upper
            rev_n_w[16 * i + 8 : 16 * i + 16] = lower
        row_flip = 7 - lax.broadcasted_iota(jnp.int32, (8, LANES), 0)
        for j, rows in ((0, high), (1, low)):
            tiles = []
            for i, shifts in ((0, (80, 64)), (1, (16, 0))):
                strip = gust[i, rows]
                for part, shift in zip((strip[8:16], strip[0:8]), shifts):
                    part = jnp.take_along_axis(part, row_flip, axis=0)
                    tiles.append(-flip_lanes(part, flip_index(shift)))
            pairs = [jnp.where(odd, tiles[2 * i], tiles[2 * i + 1]) for i in range(2)]
            rev_c_w[j] = jnp.where(lane8 >= 64, pairs[0], pairs[1])

    finish_wind_sides, finish_wind_rows, finish_wind_send = exchange(
        1,
        wind_rows,
        flip_wind,
        wsend_sem,
        wrecv_sem,
        (gust_ns.at[0:32], gust_ns.at[32:64]),
        gust.at[:, high],
        gust.at[:, low],
        (gust_c.at[0], gust_c.at[1], gust_c.at[0], gust_c.at[1]),
        (rev_n_w, rev_c_w.at[0], rev_c_w.at[1]),
        {
            N: got_n_w,
            S: got_s_w,
            E: got_e_w,
            W: got_w_w,
            NE: got_c_w.at[0],
            NW: got_c_w.at[1],
            SE: got_c_w.at[2],
            SW: got_c_w.at[3],
        },
    )
    with jax.named_scope("backward_last"):
        backward(wide, True, STEPS - 1, 0)
    finish_send()

    def result(rows):
        p = back[4, rows]
        m = back[5, rows]
        return [back[0, rows], back[1, rows], p + m, p - m, 2.0 * back[6, rows]]

    with jax.named_scope("state_pack"):
        for f, value in enumerate(result(centre)):
            fin[f] = jnp.transpose(value)
        for rows, dst in ((high, fin_e), (low, fin_w)):
            dst[...] = jnp.transpose(jnp.concatenate(result(rows) + [spare_rows], axis=0))

        @pl.when(top)
        def _():
            for f in range(5):
                rev_n[f, 0:8], rev_n[f, 8:16] = flip_strip(fin[f, NORTH], whole_flip, SIGNS[f])
            for i, src in ((0, fin_e), (1, fin_w)):
                rev_c[i, 0:8], rev_c[i, 8:16] = flip_strip(src[NORTH], group_flip, group_sign)

    with jax.named_scope("recv_wind"):
        finish_wind_sides()

    def with_sides(i):
        value = gust[i, centre]

        def ends(straight, upper, lower):
            extra = jnp.where(lane16 < ROWS, straight[i], 0.0)
            place = 64 * i
            upper = [pltpu.roll(upper[...], (80 - place + LANES + 16 * t) % LANES, 1) for t in (0, 1)]
            lower = [pltpu.roll(lower[...], (48 + place + 16 * t) % LANES, 1) for t in (0, 1)]
            upper, lower = jnp.concatenate(upper, axis=0), jnp.concatenate(lower, axis=0)
            extra = extra + jnp.where((lane16 >= 64) & (lane16 < ROWS), upper, 0.0)
            return extra + jnp.where(lane16 < HALO, lower, 0.0)

        at_w = ends(got_w_w, got_c_w.at[1], got_c_w.at[3])
        at_e = ends(got_e_w, got_c_w.at[0], got_c_w.at[2])
        parts = [value[:HALO] + at_w, value[HALO:-HALO], value[-HALO:] + at_e]
        return jnp.transpose(jnp.concatenate(parts, axis=0))[0:ROWS]

    with jax.named_scope("wind_add"):
        for i in range(2):
            wind_out[i] = with_sides(i)
    with jax.named_scope("recv_wind_rows"):
        finish_wind_rows()
    with jax.named_scope("squares"):
        for i in range(2):
            rows = slice(HALO * (1 - i), HALO * (2 - i))
            wind_out[i, 0:16] = wind_out[i, 0:16] + got_s_w[rows]
            wind_out[i, 64:80] = wind_out[i, 64:80] + got_n_w[rows]
        squares = wind_out[0] * wind_out[0] + wind_out[1] * wind_out[1]
        part = jnp.sum(squares, axis=0, keepdims=True)

    layer, odd_x = lax.div(gy, 2), lax.rem(gy, 2)
    layers = ny // 2
    by_ring = [wrap(ring + r, rings) * (4 * ny) for r in range(rings)]
    by_cross = [cross * (2 * ny), (1 - cross) * (2 * ny)]
    by_core = [core * ny, (1 - core) * ny]
    by_layer = [wrap(layer + z, layers) * 2 for z in range(layers)]
    by_odd = [odd_x, 1 - odd_x]
    slow = {(r, c): by_ring[r] + by_cross[c] for r in range(rings) for c in range(2)}
    fast = {
        (k, z, o): by_core[k] + (by_layer[z] + by_odd[o])
        for k in range(2)
        for z in range(layers)
        for o in range(2)
    }
    steps = sorted(
        (-(min(r, rings - r) + min(z, layers - z) + (1 if o else 2 * c)), r, c, k, z, o)
        for r, c in slow
        for k, z, o in fast
    )
    others = [step[1:] for step in steps if any(step[1:])]

    def sum_copies():
        return [
            pltpu.make_async_remote_copy(
                src_ref=red.at[me],
                dst_ref=red.at[me],
                send_sem=sum_sem.at[0],
                recv_sem=sum_sem.at[1],
                device_id=slow[r, c] + fast[k, z, o],
                device_id_type=pl.DeviceIdType.LOGICAL,
            )
            for r, c, k, z, o in others
        ]

    def end_sum():
        most = red.at[0 : everyone - 1]
        pltpu.make_async_copy(most, most, sum_sem.at[1]).wait()
        pltpu.make_async_copy(most, most, sum_sem.at[0]).wait()
        return jnp.sum(red[...], axis=0)

    pl.semaphore_wait(ready, nears - 1)
    red[me] = part
    with jax.named_scope("sum_start"):
        for copy in sum_copies():
            copy.start()
    finish_state_sides, finish_state_rows, finish_state_send = exchange(
        2,
        None,
        None,
        fsend_sem,
        frecv_sem,
        (fin.at[:, NORTH], fin.at[:, SOUTH]),
        fin_e.at[0:ROWS],
        fin_w.at[0:ROWS],
        (fin_e.at[NORTH], fin_w.at[NORTH], fin_e.at[SOUTH], fin_w.at[SOUTH]),
        (rev_n.at[0:5], rev_c.at[0, 0:HALO], rev_c.at[1, 0:HALO]),
        {
            N: got_n_f,
            S: got_s_f,
            E: got_e_f,
            W: got_w_f,
            NE: got_c_f.at[0],
            NW: got_c_f.at[1],
            SE: got_c_f.at[2],
            SW: got_c_f.at[3],
        },
    )
    with jax.named_scope("recv_state"):
        finish_state_sides()
        finish_state_rows()
    with jax.named_scope("state_add"):
        got_e_f[64:80] = got_e_f[64:80] + got_c_f[0]
        got_w_f[64:80] = got_w_f[64:80] + got_c_f[1]
        got_e_f[0:16] = got_e_f[0:16] + got_c_f[2]
        got_w_f[0:16] = got_w_f[0:16] + got_c_f[3]
        packed_e = got_e_f[...]
        packed_w = got_w_f[...]
        for f in range(5):
            side_e = pltpu.roll(packed_e, LANES - HALO - HALO * f, 1)
            side_w = packed_w if f == 0 else pltpu.roll(packed_w, LANES - HALO * f, 1)
            value = fin[f, 0:ROWS]
            value = value + jnp.where(lane >= LANES - HALO, side_e, 0.0)
            value = value + jnp.where(lane < HALO, side_w, 0.0)
            state_out[f] = value
            state_out[f, 0:16] = state_out[f, 0:16] + got_s_f[f]
            state_out[f, 64:80] = state_out[f, 64:80] + got_n_f[f]
    finish_wind_send()
    finish_state_send()
    with jax.named_scope("sum_all"):
        part = end_sum()
    total = jnp.sum(jnp.broadcast_to(part, (8, LANES)), axis=1, keepdims=True)[0:1]
    entries = 2 * ROWS * LANES * nx * ny
    inv = lax.rsqrt(total / entries + NORM_EPS)
    for i in range(2):
        wind_out[i] = wind_out[i] * inv


def writer(state, wind, state_hbm, wind_hbm, sem):
    pieces = [(state, state_hbm, f) for f in range(5)] + [(wind, wind_hbm, f) for f in range(2)]
    copies = [
        pltpu.make_async_copy(src.at[f], dst.at[f], sem.at[i])
        for i, (src, dst, f) in enumerate(pieces)
    ]
    for copy in copies:
        copy.start()
    for copy in copies:
        copy.wait()


def solution(mesh):
    nx, ny = mesh.shape["gx"], mesh.shape["gy"]

    def per_device(velocity, stress, wind, strength, mass, land, region, observed, start):
        vm = lambda *shape: pltpu.VMEM(shape, F32)
        dma = pltpu.SemaphoreType.DMA
        any_spec = pl.BlockSpec(memory_space=pl.ANY)
        args = (start, velocity, stress, wind, strength, mass, land, region, observed)
        args = [args[0]] + [pltpu.with_memory_space_constraint(z, pltpu.HBM) for z in args[1:]]
        shapes = (
            jax.ShapeDtypeStruct((5, ROWS, LANES), F32),
            jax.ShapeDtypeStruct((2, ROWS, LANES), F32),
        )
        vmem_spec = pl.BlockSpec(memory_space=pltpu.VMEM)
        state, gusts = pl.pallas_call(
            functools.partial(kernel, nx, ny),
            out_shape=shapes,
            in_specs=[pl.BlockSpec(memory_space=pltpu.SMEM)] + [any_spec] * 8,
            out_specs=(vmem_spec, vmem_spec),
            scratch_shapes=[
                vm(9, LANES, LANES),
                vm(ROWS, LANES),
                pltpu.VMEM((ROWS, LANES), jnp.int32),
                pltpu.VMEM((ROWS, LANES), jnp.int32),
                vm(3, LANES, LANES),
                vm(3, LANES, LANES),
                vm(ROWS + HALO, LANES),
                vm(ROWS + HALO, LANES),
                vm(4, HALO + 8, LANES),
                vm(ROWS + HALO, LANES),
                vm(ROWS + HALO, LANES),
                vm(4, HALO + 8, LANES),
                vm(9, HALO, LANES),
                vm(2, HALO + 8, LANES),
                vm(5, TALL, LANES),
                vm(5, TALL, LANES),
                vm(STEPS, 4, TALL, LANES),
                vm(12, TALL, LANES),
                vm(5, LANES, LANES),
                vm(LANES, LANES),
                vm(LANES, LANES),
                vm(5, HALO, LANES),
                vm(5, HALO, LANES),
                vm(ROWS, LANES),
                vm(ROWS, LANES),
                vm(4, HALO, LANES),
                vm(2, TALL, LANES),
                vm(64, LANES),
                vm(2, 8, LANES),
                vm(2 * HALO, LANES),
                vm(2 * HALO, LANES),
                vm(2, HALO, LANES),
                vm(2, HALO, LANES),
                vm(4, 8, LANES),
                vm(2 * HALO, LANES),
                vm(2, 8, LANES),
                vm(nx * ny, 1, LANES),
                dma((9,)),
                dma((8,)),
                dma((8,)),
                dma((8,)),
                dma((8,)),
                dma((8,)),
                dma((8,)),
                dma((6,)),
                dma((2,)),
                pltpu.SemaphoreType.REGULAR,
            ],
            compiler_params=pltpu.CompilerParams(
                collective_id=0, has_side_effects=True, vmem_limit_bytes=32 * 1024 * 1024
            ),
        )(*args)
        return pl.pallas_call(
            writer,
            out_shape=shapes,
            in_specs=[vmem_spec, vmem_spec],
            out_specs=(any_spec, any_spec),
            scratch_shapes=[dma((7,))],
        )(
            pltpu.with_memory_space_constraint(state, pltpu.VMEM),
            pltpu.with_memory_space_constraint(gusts, pltpu.VMEM),
        )

    tri, two = P(None, "gy", "gx"), P("gy", "gx")
    return jax.shard_map(
        per_device,
        mesh=mesh,
        in_specs=(tri, tri, tri, two, two, two, two, tri, P()),
        out_specs=(tri, tri),
        check_vma=False,
    )
```

```python
import functools

import jax
import jax.numpy as jnp
from jax import lax
from jax.experimental import pallas as pl
from jax.experimental.pallas import tpu as pltpu
from jax.sharding import PartitionSpec as P

STEPS = 8
SUBTOTAL = 120
HALO = 2 * STEPS
LANES = 128
PAD = 8
CHUNK = 8
NORM_EPS = 1e-06
F32 = jnp.float32
MESH = pl.DeviceIdType.MESH

ROWS = 80
NORTH = slice(80, 96)
GAP = slice(96, 112)
SOUTH = slice(112, 128)
FIRST = PAD + HALO
LAST = FIRST + LANES
TALL = LAST + HALO + PAD
SIGNS = (-1.0, -1.0, 1.0, 1.0, 1.0, -1.0, -1.0, 1.0, 1.0)

N, S, E, W, NE, NW, SE, SW = range(8)


def flip_lanes(x, index):
    return jnp.take_along_axis(x, index, axis=1)


def flip_strip(strip, lane_index, sign):
    row_index = 7 - lax.broadcasted_iota(jnp.int32, (8, LANES), 0)
    upper = jnp.take_along_axis(strip[8:16], row_index, axis=0)
    lower = jnp.take_along_axis(strip[0:8], row_index, axis=0)
    upper = flip_lanes(upper, lane_index)
    lower = flip_lanes(lower, lane_index)
    return sign * upper, sign * lower


def kernel(
    nx,
    ny,
    start_ref,
    velocity,
    stress,
    wind,
    strength,
    mass,
    land,
    region,
    observed,
    state_out,
    wind_out,
    raw,
    mass_v,
    land_v,
    region_v,
    target,
    goal,
    bundle_e,
    bundle_w,
    corner_out,
    got_e,
    got_w,
    got_c,
    rev_n,
    rev_c,
    field,
    static,
    saved,
    back,
    fin,
    fin_e,
    fin_w,
    got_n_f,
    got_s_f,
    got_e_f,
    got_w_f,
    got_c_f,
    gust,
    gust_ns,
    gust_c,
    got_n_w,
    got_s_w,
    got_e_w,
    got_w_w,
    got_c_w,
    rev_n_w,
    rev_c_w,
    red,
    load_sem,
    send_sem,
    recv_sem,
    wsend_sem,
    wrecv_sem,
    fsend_sem,
    frecv_sem,
    self_sem,
    sum_sem,
    ready,
):
    gx = lax.axis_index("gx")
    gy = lax.axis_index("gy")
    top = gy == ny - 1
    bottom = gy == 0
    not_top = gy < ny - 1
    not_bottom = gy > 0
    def wrap(index, count):
        return jnp.where(index >= count, index - count, index)

    east = wrap(gx + 1, nx)
    west = wrap(gx + nx - 1, nx)
    fold = nx - 1 - gx
    fold_e = wrap(2 * nx - 2 - gx, nx)
    fold_w = wrap(nx - gx, nx)

    def at(x, y):
        return {"gx": x, "gy": y}

    loads = [
        pltpu.make_async_copy(velocity, raw.at[0:2, 0:ROWS], load_sem.at[0]),
        pltpu.make_async_copy(stress, raw.at[2:5, 0:ROWS], load_sem.at[1]),
        pltpu.make_async_copy(wind, raw.at[5:7, 0:ROWS], load_sem.at[2]),
        pltpu.make_async_copy(strength, raw.at[7, 0:ROWS], load_sem.at[3]),
        pltpu.make_async_copy(mass, mass_v, load_sem.at[4]),
        pltpu.make_async_copy(land, land_v, load_sem.at[5]),
        pltpu.make_async_copy(region, region_v, load_sem.at[6]),
        pltpu.make_async_copy(observed, target.at[1:3, 0:ROWS], load_sem.at[7]),
    ]
    for copy in loads:
        copy.start()

    ring = lax.div(gx, 4)
    core = lax.rem(gx, 2)
    cross = lax.div(gx - 4 * ring - core, 2)
    rings = nx // 4
    near = ring * 2 + core
    far = cross * ny + gy
    nears, fars = 2 * rings, 2 * ny
    everyone = nx * ny
    me = gx * ny + gy

    def near_at(d, sign=1):
        r = wrap(ring + (d // 2 if sign > 0 else rings - d // 2), rings) if d // 2 else ring
        c = 1 - core if d % 2 else core
        return r * 2 + c, at(r * 4 + cross * 2 + c, gy)

    def far_at(d, sign=1):
        y = wrap(gy + (d // 2 if sign > 0 else ny - d // 2), ny) if d // 2 else gy
        x = 1 - cross if d % 2 else cross
        return x * ny + y, at(gx + 2 * (x - cross), y)

    barrier = pltpu.get_barrier_semaphore()

    def greet(where):
        pl.semaphore_signal(barrier, inc=1, device_id=where, device_id_type=MESH)

    with jax.named_scope("greet"):
        greet(at(east, gy))
        greet(at(west, gy))

        @pl.when(not_top)
        def _():
            for x in (gx, east, west):
                greet(at(x, gy + 1))

        @pl.when(not_bottom)
        def _():
            for x in (gx, east, west):
                greet(at(x, gy - 1))

        @pl.when(top)
        def _():
            greet(at(fold, gy))

        @pl.when(top & (fold_e != gx))
        def _():
            greet(at(fold_e, gy))

        @pl.when(top & (fold_w != gx))
        def _():
            greet(at(fold_w, gy))

        for d in range(1, fars):
            greet(far_at(d)[1])
        for d in range(1, nears):
            greet(near_at(d)[1])

    zero_gap = jnp.zeros((HALO, LANES), F32)
    for f in range(9):
        raw[f, GAP] = zero_gap
    for f in range(3):
        target[f, ROWS:LANES] = jnp.zeros((LANES - ROWS, LANES), F32)
    zero_pad = jnp.zeros((PAD, LANES), F32)
    for f in range(5):
        field[f, 0:PAD] = zero_pad
        field[f, TALL - PAD : TALL] = zero_pad
    for f in range(12):
        back[f, 0:FIRST] = jnp.zeros((FIRST, LANES), F32)
        back[f, LAST:TALL] = jnp.zeros((FIRST, LANES), F32)
    for f in (4, 5, 6, 10, 11):
        back[f, FIRST:LAST] = jnp.zeros((LANES, LANES), F32)

    @pl.when(bottom)
    def _():
        for f in range(9):
            raw[f, SOUTH] = zero_gap
        for f in range(5):
            got_s_f[f] = zero_gap
        for i in (2, 3):
            got_c[i] = jnp.zeros((HALO + 8, LANES), F32)
            got_c_f[i] = zero_gap
            got_c_w[i] = jnp.zeros((8, LANES), F32)
        got_s_w[...] = jnp.zeros((2 * HALO, LANES), F32)

    for copy in loads:
        copy.wait()

    lane = lax.broadcasted_iota(jnp.int32, (ROWS, LANES), 1)
    lane16 = lax.broadcasted_iota(jnp.int32, (HALO, LANES), 1)
    lane8 = lax.broadcasted_iota(jnp.int32, (8, LANES), 1)
    whole_flip = LANES - 1 - lane8
    group_flip = lane8 + (HALO - 1) - 2 * lax.rem(lane8, HALO)
    group = lane8 // HALO
    group_sign = jnp.where((group < 2) | ((group >= 5) & (group < 7)), -1.0, 1.0)
    odd = lax.rem(group, 2) == 1

    def two_tiles(first, second):
        return jnp.where(odd, first, pltpu.roll(second, LANES - HALO, 1))

    spare_rows = jnp.zeros((LANES - ROWS, LANES), F32)

    with jax.named_scope("pack"):
        drag = land_v[...].astype(F32) * (0.5 / (mass_v[...] + 0.5))
        raw[8, 0:ROWS] = drag
        drag_t = jnp.transpose(jnp.concatenate([drag, spare_rows], axis=0))
        target[0, 0:ROWS] = region_v[...].astype(F32)
        packed_e = pltpu.roll(raw[0, 0:ROWS], HALO, 1)
        packed_w = raw[0, 0:ROWS]
        for f in range(1, 8):
            here = (lane >= HALO * f) & (lane < HALO * (f + 1))
            value = raw[f, 0:ROWS]
            packed_e = jnp.where(here, pltpu.roll(value, (HALO * f + HALO) % LANES, 1), packed_e)
            packed_w = jnp.where(here, pltpu.roll(value, HALO * f, 1), packed_w)
        sides = ((bundle_e, packed_e, drag_t[LANES - HALO :]), (bundle_w, packed_w, drag_t[:HALO]))
        strips = []
        for i, (bundle, packed, strip) in enumerate(sides):
            bundle[0:ROWS] = packed
            bundle[ROWS:] = strip
            upper, lower = pltpu.roll(strip, 48, 1), pltpu.roll(strip, 80, 1)
            strips.append(upper)
            corner_out[i, 0:HALO] = packed[64:80]
            corner_out[i, HALO:] = two_tiles(upper[0:8], upper[8:16])
            corner_out[2 + i, 0:HALO] = packed[0:16]
            corner_out[2 + i, HALO:] = two_tiles(lower[0:8], lower[8:16])

        @pl.when(top)
        def _():
            for f in range(9):
                rev_n[f, 0:8], rev_n[f, 8:16] = flip_strip(raw[f, 64:80], whole_flip, SIGNS[f])
            for i in range(2):
                rev_c[i, 0:8], rev_c[i, 8:16] = flip_strip(
                    corner_out[i, 0:HALO], group_flip, group_sign
                )
                upper, lower = flip_strip(strips[i], whole_flip, 1.0)
                rev_c[i, HALO:] = two_tiles(pltpu.roll(upper, 80, 1), pltpu.roll(lower, 80, 1))

    def remote(src, dst, send, recv, slot, x, y):
        return pltpu.make_async_remote_copy(
            src_ref=src,
            dst_ref=dst,
            send_sem=send.at[slot],
            recv_sem=recv.at[slot],
            device_id=at(x, y),
            device_id_type=MESH,
        )

    def exchange(turn, middle, late, send, recv, ns, e, w, corners, folded, slots):
        to_n, to_s = ns
        corner = {
            SW: (corners[0], east, gy + 1),
            SE: (corners[1], west, gy + 1),
            NW: (corners[2], east, gy - 1),
            NE: (corners[3], west, gy - 1),
        }

        def side_copies():
            return [
                remote(e, slots[W], send, recv, W, east, gy),
                remote(w, slots[E], send, recv, E, west, gy),
            ]

        def corner_copy(k):
            return remote(corner[k][0], slots[k], send, recv, k, *corner[k][1:])

        def corner_copies(kinds):
            return [corner_copy(k) for k in kinds]

        def north_copy():
            return remote(to_n, slots[S], send, recv, S, gx, gy + 1)

        def south_copy():
            return remote(to_s, slots[N], send, recv, N, gx, gy - 1)

        def north_copies():
            return [*corner_copies((SW, SE)), north_copy()]

        def south_copies():
            return [*corner_copies((NW, NE)), south_copy()]

        def fold_copy(k, src, slot, x):
            return pltpu.make_async_remote_copy(
                src_ref=src,
                dst_ref=slots[slot],
                send_sem=send.at[k],
                recv_sem=recv.at[slot],
                device_id=at(x, gy),
                device_id_type=MESH,
            )

        def local_copy(i, src, slot):
            return pltpu.make_async_copy(src, slots[slot], self_sem.at[2 * turn + i])

        fold_n = lambda: fold_copy(S, folded[0], N, fold)
        fold_ne = lambda: fold_copy(SW, folded[1], NE, fold_e)
        fold_nw = lambda: fold_copy(SE, folded[2], NW, fold_w)
        self_ne = lambda: local_copy(0, folded[1], NE)
        self_nw = lambda: local_copy(1, folded[2], NW)

        @pl.when(not_top)
        def _():
            for copy in corner_copies((SW, SE)):
                copy.start()

        @pl.when(not_bottom)
        def _():
            for copy in corner_copies((NW, NE)):
                copy.start()

        def fold_corners():
            @pl.when(top & (fold_e != gx))
            def _():
                fold_ne().start()

            @pl.when(top & (fold_e == gx))
            def _():
                self_ne().start()

            @pl.when(top & (fold_w != gx))
            def _():
                fold_nw().start()

            @pl.when(top & (fold_w == gx))
            def _():
                self_nw().start()

        def fold_rows():
            @pl.when(top)
            def _():
                fold_n().start()

        if late is None:
            fold_corners()
        for copy in side_copies():
            copy.start()
        if middle is not None:
            middle()
        if late is None:
            fold_rows()

        @pl.when(not_top)
        def _():
            north_copy().start()

        @pl.when(not_bottom)
        def _():
            south_copy().start()

        if late is not None:
            pl.when(top)(late)
            fold_corners()
            fold_rows()

        def finish_sides():
            for copy in side_copies():
                copy.wait_recv()

            @pl.when(not_bottom)
            def _():
                for copy in corner_copies((SW, SE)):
                    copy.wait_recv()

            @pl.when(not_top)
            def _():
                for copy in corner_copies((NW, NE)):
                    copy.wait_recv()

            @pl.when(top & (fold_e != gx))
            def _():
                fold_ne().wait_recv()

            @pl.when(top & (fold_e == gx))
            def _():
                self_ne().wait()

            @pl.when(top & (fold_w != gx))
            def _():
                fold_nw().wait_recv()

            @pl.when(top & (fold_w == gx))
            def _():
                self_nw().wait()

        def finish_rows():
            @pl.when(not_bottom)
            def _():
                north_copy().wait_recv()

            @pl.when(not_top)
            def _():
                south_copy().wait_recv()

            @pl.when(top)
            def _():
                fold_n().wait_recv()

        def finish_send():
            for copy in side_copies():
                copy.wait_send()

            @pl.when(not_top)
            def _():
                for copy in north_copies():
                    copy.wait_send()

            @pl.when(not_bottom)
            def _():
                for copy in south_copies():
                    copy.wait_send()

            @pl.when(top)
            def _():
                fold_n().wait_send()

            @pl.when(top & (fold_e != gx))
            def _():
                fold_ne().wait_send()

            @pl.when(top & (fold_w != gx))
            def _():
                fold_nw().wait_send()

        return finish_sides, finish_rows, finish_send

    peers = (nears - 1) + (fars - 1) + 2
    as_int = lambda flag: flag.astype(jnp.int32)
    peers = peers + 3 * as_int(not_top) + 3 * as_int(not_bottom) + as_int(top)
    peers = peers + as_int(top & (fold_e != gx)) + as_int(top & (fold_w != gx))
    with jax.named_scope("barrier"):
        pl.semaphore_wait(barrier, peers)

    finish_sides, finish_rows, finish_send = exchange(
        0,
        None,
        None,
        send_sem,
        recv_sem,
        (raw.at[:, 64:80], raw.at[:, 0:16]),
        bundle_e,
        bundle_w,
        tuple(corner_out.at[i] for i in range(4)),
        (rev_n, rev_c.at[0], rev_c.at[1]),
        {
            N: raw.at[:, NORTH],
            S: raw.at[:, SOUTH],
            E: got_e,
            W: got_w,
            NE: got_c.at[0],
            NW: got_c.at[1],
            SE: got_c.at[2],
            SW: got_c.at[3],
        },
    )
    for d in range(1, nears):
        pl.semaphore_signal(ready, inc=1, device_id=near_at(d)[1], device_id_type=MESH)
    for i in range(3):
        goal[i] = jnp.transpose(target[i])
    with jax.named_scope("recv_first"):
        finish_sides()

    centre = slice(FIRST, LAST)
    low = slice(PAD, FIRST)
    high = slice(LAST, LAST + HALO)

    def side(bundle, upper, lower):
        packed = [bundle[0:ROWS], upper[0:HALO], zero_gap, lower[0:HALO]]
        packed = jnp.transpose(jnp.concatenate(packed, axis=0))
        upper, lower = [
            jnp.concatenate([x[HALO:], pltpu.roll(x[HALO:], HALO, 1)], axis=0)
            for x in (upper, lower)
        ]
        strip = jnp.where(lane16 < 96, upper, jnp.where(lane16 >= 112, lower, 0.0))
        strip = jnp.where(lane16 < ROWS, bundle[ROWS:], strip)
        return [packed[HALO * f : HALO * (f + 1)] for f in range(8)] + [strip]

    def place(rows, parts):
        u, v, s1, s2, s12, wu, wv, strong, b = parts
        field[0, rows] = u
        field[1, rows] = v
        field[2, rows] = s1 + s2
        field[3, rows] = s1 - s2
        field[4, rows] = 2.0 * s12
        static[0, rows] = jnp.where(b > 0.0, 1.0, 0.0) - b
        static[1, rows] = 0.25 * b
        static[2, rows] = b * wu
        static[3, rows] = b * wv
        static[4, rows] = strong

    place(low, side(got_w, got_c.at[1], got_c.at[3]))
    place(high, side(got_e, got_c.at[0], got_c.at[2]))
    with jax.named_scope("recv_rows"):
        finish_rows()
    place(centre, [jnp.transpose(raw[f]) for f in range(9)])

    begin = start_ref[0].astype(F32)

    def coefs(k):
        step = jnp.full((CHUNK, LANES), begin + jnp.asarray(k + 1, jnp.int32).astype(F32), F32)
        coef = 0.2 + 0.8 * step / SUBTOTAL
        keep = 1.0 / (1.0 + coef)
        return coef, keep

    to_n = lambda x: pltpu.roll(x, LANES - 1, 1)
    to_s = lambda x: pltpu.roll(x, 1, 1)
    wide = range(PAD, TALL - PAD, CHUNK)
    narrow = range(PAD + 8, TALL - PAD - 8, CHUNK)

    def forward(chunks, k, carry):
        coef, keep = coefs(k)
        gain = coef * keep
        for r in chunks:
            rows = slice(r, r + CHUNK)
            up = slice(r + 1, r + 1 + CHUNK)
            down = slice(r - 1, r - 1 + CHUNK)
            u = field[0, rows]
            v = field[1, rows]
            x1 = field[0, up] - field[0, down]
            x2 = field[1, up] - field[1, down]
            y1 = to_n(u) - to_s(u)
            y2 = to_n(v) - to_s(v)
            div = x1 + y2
            ten = x1 - y2
            quarter = 0.25 * ten
            half = 0.5 * (y1 + x2)
            inv = lax.rsqrt(div * div + quarter * ten + half * half + 0.16)
            rate = gain * static[4, rows]
            un = (div + quarter) * inv
            vn = (div - quarter) * inv
            sn = half * inv
            saved[k, 0, rows] = un
            saved[k, 1, rows] = vn
            saved[k, 2, rows] = sn
            saved[k, 3, rows] = rate * inv
            field[2, rows] = keep * field[2, rows] + rate * (un - 1.0)
            field[3, rows] = keep * field[3, rows] + rate * (vn - 1.0)
            field[4, rows] = keep * field[4, rows] + rate * sn
        for r in chunks:
            rows = slice(r, r + CHUNK)
            up = slice(r + 1, r + 1 + CHUNK)
            down = slice(r - 1, r - 1 + CHUNK)
            m = field[3, rows]
            q = field[4, rows]
            fx = (field[2, up] - field[2, down]) + (to_n(q) - to_s(q))
            fy = (field[4, up] - field[4, down]) + (to_n(m) - to_s(m))
            field[0, rows] = static[0, rows] * field[0, rows] + (static[2, rows] + static[1, rows] * fx)
            field[1, rows] = static[0, rows] * field[1, rows] + (static[3, rows] + static[1, rows] * fy)
        return carry

    with jax.named_scope("forward"):
        lax.fori_loop(0, STEPS // 2, functools.partial(forward, wide), 0, unroll=4)
        lax.fori_loop(STEPS // 2, STEPS, functools.partial(forward, narrow), 0, unroll=4)

    for i in range(2):
        miss = goal[0] * (field[i, centre] - goal[1 + i])
        back[i, centre] = miss
        back[2 + i, centre] = static[1, centre] * miss

    def backward(chunks, last, i, carry):
        k = STEPS - 1 - i
        _, keep = coefs(k)
        for r in chunks:
            rows = slice(r, r + CHUNK)
            up = slice(r + 1, r + 1 + CHUNK)
            down = slice(r - 1, r - 1 + CHUNK)
            mu = back[2, rows]
            mv = back[3, rows]
            tp = back[4, rows] + (back[2, down] - back[2, up])
            tm = back[5, rows] + (to_s(mv) - to_n(mv))
            tq = back[6, rows] + ((to_s(mu) - to_n(mu)) + (back[3, down] - back[3, up]))
            un = saved[k, 0, rows]
            vn = saved[k, 1, rows]
            sn = saved[k, 2, rows]
            g = saved[k, 3, rows]
            along = tp * un + tm * vn + tq * sn
            total = tp + tm
            quarter = 0.25 * (tp - tm)
            back[7, rows] = g * ((total + quarter) - along * un)
            back[8, rows] = g * ((total - quarter) - along * vn)
            back[9, rows] = (0.5 * g) * (tq - along * sn)
            back[4, rows] = keep * tp
            back[5, rows] = keep * tm
            back[6, rows] = keep * tq
        for r in chunks:
            rows = slice(r, r + CHUNK)
            up = slice(r + 1, r + 1 + CHUNK)
            down = slice(r - 1, r - 1 + CHUNK)
            yb = back[8, rows]
            sb = back[9, rows]
            lu = back[0, rows]
            lv = back[1, rows]
            if not last:
                back[10, rows] = back[10, rows] + lu
                back[11, rows] = back[11, rows] + lv
            new_u = static[0, rows] * lu + ((back[7, down] - back[7, up]) + (to_s(sb) - to_n(sb)))
            new_v = static[0, rows] * lv + ((back[9, down] - back[9, up]) + (to_s(yb) - to_n(yb)))
            back[0, rows] = new_u
            back[1, rows] = new_v
            if not last:
                back[2, rows] = static[1, rows] * new_u
                back[3, rows] = static[1, rows] * new_v
        return carry

    with jax.named_scope("backward"):
        lax.fori_loop(0, STEPS // 2, functools.partial(backward, narrow, False), 0, unroll=4)
        lax.fori_loop(STEPS // 2, STEPS - 1, functools.partial(backward, wide, False), 0, unroll=3)

    def four_tiles(u0, u1, v0, v1):
        other = two_tiles(pltpu.roll(v0, 64, 1), pltpu.roll(v1, 64, 1))
        return jnp.where(lane8 >= 64, two_tiles(u0, u1), other)

    lane_all = lax.broadcasted_iota(jnp.int32, (LANES, LANES), 1)
    def gusts(rows):
        for i in range(2):
            gust[i, rows] = 4.0 * static[1, rows] * (back[10 + i, rows] + back[i, rows])

    with jax.named_scope("wind_pack"):
        gusts(high)
        gusts(low)
        for j, rows in ((0, high), (1, low)):
            u, v = gust[0, rows], gust[1, rows]
            gust_c[j] = four_tiles(u[0:8], u[8:16], v[0:8], v[8:16])

    def wind_rows():
        gusts(centre)
        here = ((lane_all >= 80) & (lane_all < 96)) | (lane_all >= 112)
        both = jnp.where(here, gust[0, centre], pltpu.roll(gust[1, centre], LANES - HALO, 1))
        gust_ns[...] = jnp.transpose(both)[64:LANES]

    def flip_index(shift):
        return lax.rem(2 * LANES - 1 + shift - lane8, LANES)

    def flip_wind():
        for i in range(2):
            part = slice(HALO * i, HALO * (i + 1))
            upper, lower = flip_strip(gust_ns[part], whole_flip, -1.0)
            rev_n_w[16 * i : 16 * i + 8] = upper
            rev_n_w[16 * i + 8 : 16 * i + 16] = lower
        row_flip = 7 - lax.broadcasted_iota(jnp.int32, (8, LANES), 0)
        for j, rows in ((0, high), (1, low)):
            tiles = []
            for i, shifts in ((0, (80, 64)), (1, (16, 0))):
                strip = gust[i, rows]
                for part, shift in zip((strip[8:16], strip[0:8]), shifts):
                    part = jnp.take_along_axis(part, row_flip, axis=0)
                    tiles.append(-flip_lanes(part, flip_index(shift)))
            pairs = [jnp.where(odd, tiles[2 * i], tiles[2 * i + 1]) for i in range(2)]
            rev_c_w[j] = jnp.where(lane8 >= 64, pairs[0], pairs[1])

    finish_wind_sides, finish_wind_rows, finish_wind_send = exchange(
        1,
        wind_rows,
        flip_wind,
        wsend_sem,
        wrecv_sem,
        (gust_ns.at[0:32], gust_ns.at[32:64]),
        gust.at[:, high],
        gust.at[:, low],
        (gust_c.at[0], gust_c.at[1], gust_c.at[0], gust_c.at[1]),
        (rev_n_w, rev_c_w.at[0], rev_c_w.at[1]),
        {
            N: got_n_w,
            S: got_s_w,
            E: got_e_w,
            W: got_w_w,
            NE: got_c_w.at[0],
            NW: got_c_w.at[1],
            SE: got_c_w.at[2],
            SW: got_c_w.at[3],
        },
    )
    with jax.named_scope("backward_last"):
        backward(wide, True, STEPS - 1, 0)
    finish_send()

    def result(rows):
        p = back[4, rows]
        m = back[5, rows]
        return [back[0, rows], back[1, rows], p + m, p - m, 2.0 * back[6, rows]]

    with jax.named_scope("state_pack"):
        for f, value in enumerate(result(centre)):
            fin[f] = jnp.transpose(value)
        for rows, dst in ((high, fin_e), (low, fin_w)):
            dst[...] = jnp.transpose(jnp.concatenate(result(rows) + [spare_rows], axis=0))

        @pl.when(top)
        def _():
            for f in range(5):
                rev_n[f, 0:8], rev_n[f, 8:16] = flip_strip(fin[f, NORTH], whole_flip, SIGNS[f])
            for i, src in ((0, fin_e), (1, fin_w)):
                rev_c[i, 0:8], rev_c[i, 8:16] = flip_strip(src[NORTH], group_flip, group_sign)

    with jax.named_scope("recv_wind"):
        finish_wind_sides()

    def with_sides(i):
        value = gust[i, centre]

        def ends(straight, upper, lower):
            extra = jnp.where(lane16 < ROWS, straight[i], 0.0)
            place = 64 * i
            upper = [pltpu.roll(upper[...], (80 - place + LANES + 16 * t) % LANES, 1) for t in (0, 1)]
            lower = [pltpu.roll(lower[...], (48 + place + 16 * t) % LANES, 1) for t in (0, 1)]
            upper, lower = jnp.concatenate(upper, axis=0), jnp.concatenate(lower, axis=0)
            extra = extra + jnp.where((lane16 >= 64) & (lane16 < ROWS), upper, 0.0)
            return extra + jnp.where(lane16 < HALO, lower, 0.0)

        at_w = ends(got_w_w, got_c_w.at[1], got_c_w.at[3])
        at_e = ends(got_e_w, got_c_w.at[0], got_c_w.at[2])
        parts = [value[:HALO] + at_w, value[HALO:-HALO], value[-HALO:] + at_e]
        return jnp.transpose(jnp.concatenate(parts, axis=0))[0:ROWS]

    with jax.named_scope("wind_add"):
        for i in range(2):
            wind_out[i] = with_sides(i)
    with jax.named_scope("recv_wind_rows"):
        finish_wind_rows()
    with jax.named_scope("squares"):
        for i in range(2):
            rows = slice(HALO * (1 - i), HALO * (2 - i))
            wind_out[i, 0:16] = wind_out[i, 0:16] + got_s_w[rows]
            wind_out[i, 64:80] = wind_out[i, 64:80] + got_n_w[rows]
        squares = wind_out[0] * wind_out[0] + wind_out[1] * wind_out[1]
        part = jnp.sum(squares, axis=0, keepdims=True)

    layer, odd_x = lax.div(gy, 2), lax.rem(gy, 2)
    layers = ny // 2
    by_ring = [wrap(ring + r, rings) * (4 * ny) for r in range(rings)]
    by_cross = [cross * (2 * ny), (1 - cross) * (2 * ny)]
    by_core = [core * ny, (1 - core) * ny]
    by_layer = [wrap(layer + z, layers) * 2 for z in range(layers)]
    by_odd = [odd_x, 1 - odd_x]
    slow = {(r, c): by_ring[r] + by_cross[c] for r in range(rings) for c in range(2)}
    fast = {
        (k, z, o): by_core[k] + (by_layer[z] + by_odd[o])
        for k in range(2)
        for z in range(layers)
        for o in range(2)
    }
    steps = sorted(
        (-(min(r, rings - r) + min(z, layers - z) + (1 if o else 2 * c)), r, c, k, z, o)
        for r, c in slow
        for k, z, o in fast
    )
    others = [step[1:] for step in steps if any(step[1:])]

    def sum_copies():
        return [
            pltpu.make_async_remote_copy(
                src_ref=red.at[pl.ds(me, 1)],
                dst_ref=red.at[pl.ds(me, 1)],
                send_sem=sum_sem.at[0],
                recv_sem=sum_sem.at[1],
                device_id=slow[r, c] + fast[k, z, o],
                device_id_type=pl.DeviceIdType.LOGICAL,
            )
            for r, c, k, z, o in others
        ]

    def end_sum():
        most = red.at[0 : everyone - 1]
        pltpu.make_async_copy(most, most, sum_sem.at[1]).wait()
        pltpu.make_async_copy(most, most, sum_sem.at[0]).wait()
        return jnp.sum(red[...], axis=0, keepdims=True)

    pl.semaphore_wait(ready, nears - 1)
    red[pl.ds(me, 1)] = part
    with jax.named_scope("sum_start"):
        for copy in sum_copies():
            copy.start()
    finish_state_sides, finish_state_rows, finish_state_send = exchange(
        2,
        None,
        None,
        fsend_sem,
        frecv_sem,
        (fin.at[:, NORTH], fin.at[:, SOUTH]),
        fin_e.at[0:ROWS],
        fin_w.at[0:ROWS],
        (fin_e.at[NORTH], fin_w.at[NORTH], fin_e.at[SOUTH], fin_w.at[SOUTH]),
        (rev_n.at[0:5], rev_c.at[0, 0:HALO], rev_c.at[1, 0:HALO]),
        {
            N: got_n_f,
            S: got_s_f,
            E: got_e_f,
            W: got_w_f,
            NE: got_c_f.at[0],
            NW: got_c_f.at[1],
            SE: got_c_f.at[2],
            SW: got_c_f.at[3],
        },
    )
    with jax.named_scope("recv_state"):
        finish_state_sides()
        finish_state_rows()
    with jax.named_scope("state_add"):
        got_e_f[64:80] = got_e_f[64:80] + got_c_f[0]
        got_w_f[64:80] = got_w_f[64:80] + got_c_f[1]
        got_e_f[0:16] = got_e_f[0:16] + got_c_f[2]
        got_w_f[0:16] = got_w_f[0:16] + got_c_f[3]
        packed_e = got_e_f[...]
        packed_w = got_w_f[...]
        for f in range(5):
            side_e = pltpu.roll(packed_e, LANES - HALO - HALO * f, 1)
            side_w = packed_w if f == 0 else pltpu.roll(packed_w, LANES - HALO * f, 1)
            value = fin[f, 0:ROWS]
            value = value + jnp.where(lane >= LANES - HALO, side_e, 0.0)
            value = value + jnp.where(lane < HALO, side_w, 0.0)
            state_out[f] = value
            state_out[f, 0:16] = state_out[f, 0:16] + got_s_f[f]
            state_out[f, 64:80] = state_out[f, 64:80] + got_n_f[f]
    finish_wind_send()
    finish_state_send()
    with jax.named_scope("sum_all"):
        part = end_sum()
    total = jnp.sum(jnp.broadcast_to(part, (8, LANES)), axis=1, keepdims=True)[0:1]
    entries = 2 * ROWS * LANES * nx * ny
    inv = lax.rsqrt(total / entries + NORM_EPS)
    for i in range(2):
        wind_out[i] = wind_out[i] * inv


def writer(state, wind, state_hbm, wind_hbm, sem):
    pieces = [(state, state_hbm, f) for f in range(5)] + [(wind, wind_hbm, f) for f in range(2)]
    copies = [
        pltpu.make_async_copy(src.at[f], dst.at[f], sem.at[i])
        for i, (src, dst, f) in enumerate(pieces)
    ]
    for copy in copies:
        copy.start()
    for copy in copies:
        copy.wait()


def solution(mesh):
    nx, ny = mesh.shape["gx"], mesh.shape["gy"]

    def per_device(velocity, stress, wind, strength, mass, land, region, observed, start):
        vm = lambda *shape: pltpu.VMEM(shape, F32)
        dma = pltpu.SemaphoreType.DMA
        any_spec = pl.BlockSpec(memory_space=pl.ANY)
        args = (start, velocity, stress, wind, strength, mass, land, region, observed)
        args = [args[0]] + [pltpu.with_memory_space_constraint(z, pltpu.HBM) for z in args[1:]]
        shapes = (
            jax.ShapeDtypeStruct((5, ROWS, LANES), F32),
            jax.ShapeDtypeStruct((2, ROWS, LANES), F32),
        )
        vmem_spec = pl.BlockSpec(memory_space=pltpu.VMEM)
        state, gusts = pl.pallas_call(
            functools.partial(kernel, nx, ny),
            out_shape=shapes,
            in_specs=[pl.BlockSpec(memory_space=pltpu.SMEM)] + [any_spec] * 8,
            out_specs=(vmem_spec, vmem_spec),
            scratch_shapes=[
                vm(9, LANES, LANES),
                vm(ROWS, LANES),
                pltpu.VMEM((ROWS, LANES), jnp.int32),
                pltpu.VMEM((ROWS, LANES), jnp.int32),
                vm(3, LANES, LANES),
                vm(3, LANES, LANES),
                vm(ROWS + HALO, LANES),
                vm(ROWS + HALO, LANES),
                vm(4, HALO + 8, LANES),
                vm(ROWS + HALO, LANES),
                vm(ROWS + HALO, LANES),
                vm(4, HALO + 8, LANES),
                vm(9, HALO, LANES),
                vm(2, HALO + 8, LANES),
                vm(5, TALL, LANES),
                vm(5, TALL, LANES),
                vm(STEPS, 4, TALL, LANES),
                vm(12, TALL, LANES),
                vm(5, LANES, LANES),
                vm(LANES, LANES),
                vm(LANES, LANES),
                vm(5, HALO, LANES),
                vm(5, HALO, LANES),
                vm(ROWS, LANES),
                vm(ROWS, LANES),
                vm(4, HALO, LANES),
                vm(2, TALL, LANES),
                vm(64, LANES),
                vm(2, 8, LANES),
                vm(2 * HALO, LANES),
                vm(2 * HALO, LANES),
                vm(2, HALO, LANES),
                vm(2, HALO, LANES),
                vm(4, 8, LANES),
                vm(2 * HALO, LANES),
                vm(2, 8, LANES),
                vm(nx * ny, LANES),
                dma((9,)),
                dma((8,)),
                dma((8,)),
                dma((8,)),
                dma((8,)),
                dma((8,)),
                dma((8,)),
                dma((6,)),
                dma((2,)),
                pltpu.SemaphoreType.REGULAR,
            ],
            compiler_params=pltpu.CompilerParams(
                collective_id=0, has_side_effects=True, vmem_limit_bytes=32 * 1024 * 1024
            ),
        )(*args)
        return pl.pallas_call(
            writer,
            out_shape=shapes,
            in_specs=[vmem_spec, vmem_spec],
            out_specs=(any_spec, any_spec),
            scratch_shapes=[dma((7,))],
        )(
            pltpu.with_memory_space_constraint(state, pltpu.VMEM),
            pltpu.with_memory_space_constraint(gusts, pltpu.VMEM),
        )

    tri, two = P(None, "gy", "gx"), P("gy", "gx")
    return jax.shard_map(
        per_device,
        mesh=mesh,
        in_specs=(tri, tri, tri, two, two, two, two, tri, P()),
        out_specs=(tri, tri),
        check_vma=False,
    )
```

```python
import functools

import jax
import jax.numpy as jnp
from jax import lax
from jax.experimental import pallas as pl
from jax.experimental.pallas import tpu as pltpu
from jax.sharding import PartitionSpec as P

STEPS = 8
SUBTOTAL = 120
HALO = 2 * STEPS
LANES = 128
PAD = 8
CHUNK = 8
NORM_EPS = 1e-06
F32 = jnp.float32
MESH = pl.DeviceIdType.MESH

ROWS = 80
NORTH = slice(80, 96)
GAP = slice(96, 112)
SOUTH = slice(112, 128)
FIRST = PAD + HALO
LAST = FIRST + LANES
TALL = LAST + HALO + PAD
SIGNS = (-1.0, -1.0, 1.0, 1.0, 1.0, -1.0, -1.0, 1.0, 1.0)

N, S, E, W, NE, NW, SE, SW = range(8)


def flip_lanes(x, index):
    return jnp.take_along_axis(x, index, axis=1)


def flip_strip(strip, lane_index, sign):
    row_index = 7 - lax.broadcasted_iota(jnp.int32, (8, LANES), 0)
    upper = jnp.take_along_axis(strip[8:16], row_index, axis=0)
    lower = jnp.take_along_axis(strip[0:8], row_index, axis=0)
    upper = flip_lanes(upper, lane_index)
    lower = flip_lanes(lower, lane_index)
    return sign * upper, sign * lower


def kernel(
    nx,
    ny,
    start_ref,
    velocity,
    stress,
    wind,
    strength,
    mass,
    land,
    region,
    observed,
    state_out,
    wind_out,
    raw,
    mass_v,
    land_v,
    region_v,
    target,
    goal,
    bundle_e,
    bundle_w,
    corner_out,
    got_e,
    got_w,
    got_c,
    rev_n,
    rev_c,
    field,
    static,
    saved,
    back,
    fin,
    fin_e,
    fin_w,
    got_n_f,
    got_s_f,
    got_e_f,
    got_w_f,
    got_c_f,
    gust,
    gust_ns,
    gust_c,
    got_n_w,
    got_s_w,
    got_e_w,
    got_w_w,
    got_c_w,
    rev_n_w,
    rev_c_w,
    red,
    load_sem,
    send_sem,
    recv_sem,
    wsend_sem,
    wrecv_sem,
    fsend_sem,
    frecv_sem,
    self_sem,
    sum_sem,
    ready,
):
    gx = lax.axis_index("gx")
    gy = lax.axis_index("gy")
    top = gy == ny - 1
    bottom = gy == 0
    not_top = gy < ny - 1
    not_bottom = gy > 0
    def wrap(index, count):
        return jnp.where(index >= count, index - count, index)

    east = wrap(gx + 1, nx)
    west = wrap(gx + nx - 1, nx)
    fold = nx - 1 - gx
    fold_e = wrap(2 * nx - 2 - gx, nx)
    fold_w = wrap(nx - gx, nx)

    def at(x, y):
        return {"gx": x, "gy": y}

    loads = [
        pltpu.make_async_copy(velocity, raw.at[0:2, 0:ROWS], load_sem.at[0]),
        pltpu.make_async_copy(stress, raw.at[2:5, 0:ROWS], load_sem.at[1]),
        pltpu.make_async_copy(wind, raw.at[5:7, 0:ROWS], load_sem.at[2]),
        pltpu.make_async_copy(strength, raw.at[7, 0:ROWS], load_sem.at[3]),
        pltpu.make_async_copy(mass, mass_v, load_sem.at[4]),
        pltpu.make_async_copy(land, land_v, load_sem.at[5]),
        pltpu.make_async_copy(region, region_v, load_sem.at[6]),
        pltpu.make_async_copy(observed, target.at[1:3, 0:ROWS], load_sem.at[7]),
    ]
    for copy in loads:
        copy.start()

    ring = lax.div(gx, 4)
    core = lax.rem(gx, 2)
    cross = lax.div(gx - 4 * ring - core, 2)
    rings = nx // 4
    everyone = nx * ny
    me = gx * ny + gy

    def tell(turn, stride):
        def signal(x, y):
            pl.semaphore_signal(
                ready.at[turn], inc=1, device_id=at(x, y), device_id_type=MESH
            )

        columns = (gx, wrap(gx + stride, nx), wrap(gx + nx - stride, nx))
        for x in columns[1:]:
            signal(x, gy)

        @pl.when(gy + stride < ny)
        def _():
            for x in columns:
                signal(x, gy + stride)

        @pl.when(gy >= stride)
        def _():
            for x in columns:
                signal(x, gy - stride)

    def hear(turn, stride):
        up = (gy + stride < ny).astype(jnp.int32)
        down = (gy >= stride).astype(jnp.int32)
        pl.semaphore_wait(ready.at[turn], 2 + 3 * up + 3 * down)

    barrier = pltpu.get_barrier_semaphore()

    def greet(where):
        pl.semaphore_signal(barrier, inc=1, device_id=where, device_id_type=MESH)

    with jax.named_scope("greet"):
        greet(at(east, gy))
        greet(at(west, gy))

        @pl.when(not_top)
        def _():
            for x in (gx, east, west):
                greet(at(x, gy + 1))

        @pl.when(not_bottom)
        def _():
            for x in (gx, east, west):
                greet(at(x, gy - 1))

        @pl.when(top)
        def _():
            greet(at(fold, gy))

        @pl.when(top & (fold_e != gx))
        def _():
            greet(at(fold_e, gy))

        @pl.when(top & (fold_w != gx))
        def _():
            greet(at(fold_w, gy))


    zero_gap = jnp.zeros((HALO, LANES), F32)
    for f in range(9):
        raw[f, GAP] = zero_gap
    for f in range(3):
        target[f, ROWS:LANES] = jnp.zeros((LANES - ROWS, LANES), F32)
    zero_pad = jnp.zeros((PAD, LANES), F32)
    for f in range(5):
        field[f, 0:PAD] = zero_pad
        field[f, TALL - PAD : TALL] = zero_pad
    for f in range(12):
        back[f, 0:FIRST] = jnp.zeros((FIRST, LANES), F32)
        back[f, LAST:TALL] = jnp.zeros((FIRST, LANES), F32)
    for f in (4, 5, 6, 10, 11):
        back[f, FIRST:LAST] = jnp.zeros((LANES, LANES), F32)

    @pl.when(bottom)
    def _():
        for f in range(9):
            raw[f, SOUTH] = zero_gap
        for f in range(5):
            got_s_f[f] = zero_gap
        for i in (2, 3):
            got_c[i] = jnp.zeros((HALO + 8, LANES), F32)
            got_c_f[i] = zero_gap
            got_c_w[i] = jnp.zeros((8, LANES), F32)
        got_s_w[...] = jnp.zeros((2 * HALO, LANES), F32)

    for copy in loads:
        copy.wait()

    lane = lax.broadcasted_iota(jnp.int32, (ROWS, LANES), 1)
    lane16 = lax.broadcasted_iota(jnp.int32, (HALO, LANES), 1)
    lane8 = lax.broadcasted_iota(jnp.int32, (8, LANES), 1)
    whole_flip = LANES - 1 - lane8
    group_flip = lane8 + (HALO - 1) - 2 * lax.rem(lane8, HALO)
    group = lane8 // HALO
    group_sign = jnp.where((group < 2) | ((group >= 5) & (group < 7)), -1.0, 1.0)
    odd = lax.rem(group, 2) == 1

    def two_tiles(first, second):
        return jnp.where(odd, first, pltpu.roll(second, LANES - HALO, 1))

    spare_rows = jnp.zeros((LANES - ROWS, LANES), F32)

    with jax.named_scope("pack"):
        drag = land_v[...].astype(F32) * (0.5 / (mass_v[...] + 0.5))
        raw[8, 0:ROWS] = drag
        drag_t = jnp.transpose(jnp.concatenate([drag, spare_rows], axis=0))
        target[0, 0:ROWS] = region_v[...].astype(F32)
        packed_e = pltpu.roll(raw[0, 0:ROWS], HALO, 1)
        packed_w = raw[0, 0:ROWS]
        for f in range(1, 8):
            here = (lane >= HALO * f) & (lane < HALO * (f + 1))
            value = raw[f, 0:ROWS]
            packed_e = jnp.where(here, pltpu.roll(value, (HALO * f + HALO) % LANES, 1), packed_e)
            packed_w = jnp.where(here, pltpu.roll(value, HALO * f, 1), packed_w)
        sides = ((bundle_e, packed_e, drag_t[LANES - HALO :]), (bundle_w, packed_w, drag_t[:HALO]))
        strips = []
        for i, (bundle, packed, strip) in enumerate(sides):
            bundle[0:ROWS] = packed
            bundle[ROWS:] = strip
            upper, lower = pltpu.roll(strip, 48, 1), pltpu.roll(strip, 80, 1)
            strips.append(upper)
            corner_out[i, 0:HALO] = packed[64:80]
            corner_out[i, HALO:] = two_tiles(upper[0:8], upper[8:16])
            corner_out[2 + i, 0:HALO] = packed[0:16]
            corner_out[2 + i, HALO:] = two_tiles(lower[0:8], lower[8:16])

        @pl.when(top)
        def _():
            for f in range(9):
                rev_n[f, 0:8], rev_n[f, 8:16] = flip_strip(raw[f, 64:80], whole_flip, SIGNS[f])
            for i in range(2):
                rev_c[i, 0:8], rev_c[i, 8:16] = flip_strip(
                    corner_out[i, 0:HALO], group_flip, group_sign
                )
                upper, lower = flip_strip(strips[i], whole_flip, 1.0)
                rev_c[i, HALO:] = two_tiles(pltpu.roll(upper, 80, 1), pltpu.roll(lower, 80, 1))

    def remote(src, dst, send, recv, slot, x, y):
        return pltpu.make_async_remote_copy(
            src_ref=src,
            dst_ref=dst,
            send_sem=send.at[slot],
            recv_sem=recv.at[slot],
            device_id=at(x, y),
            device_id_type=MESH,
        )

    def exchange(turn, middle, late, send, recv, ns, e, w, corners, folded, slots):
        to_n, to_s = ns
        corner = {
            SW: (corners[0], east, gy + 1),
            SE: (corners[1], west, gy + 1),
            NW: (corners[2], east, gy - 1),
            NE: (corners[3], west, gy - 1),
        }

        def side_copies():
            return [
                remote(e, slots[W], send, recv, W, east, gy),
                remote(w, slots[E], send, recv, E, west, gy),
            ]

        def corner_copy(k):
            return remote(corner[k][0], slots[k], send, recv, k, *corner[k][1:])

        def corner_copies(kinds):
            return [corner_copy(k) for k in kinds]

        def north_copy():
            return remote(to_n, slots[S], send, recv, S, gx, gy + 1)

        def south_copy():
            return remote(to_s, slots[N], send, recv, N, gx, gy - 1)

        def north_copies():
            return [*corner_copies((SW, SE)), north_copy()]

        def south_copies():
            return [*corner_copies((NW, NE)), south_copy()]

        def fold_copy(k, src, slot, x):
            return pltpu.make_async_remote_copy(
                src_ref=src,
                dst_ref=slots[slot],
                send_sem=send.at[k],
                recv_sem=recv.at[slot],
                device_id=at(x, gy),
                device_id_type=MESH,
            )

        def local_copy(i, src, slot):
            return pltpu.make_async_copy(src, slots[slot], self_sem.at[2 * turn + i])

        fold_n = lambda: fold_copy(S, folded[0], N, fold)
        fold_ne = lambda: fold_copy(SW, folded[1], NE, fold_e)
        fold_nw = lambda: fold_copy(SE, folded[2], NW, fold_w)
        self_ne = lambda: local_copy(0, folded[1], NE)
        self_nw = lambda: local_copy(1, folded[2], NW)

        if turn == 1:
            for copy in side_copies():
                copy.start()

        @pl.when(not_top)
        def _():
            for copy in corner_copies((SW, SE)):
                copy.start()

        @pl.when(not_bottom)
        def _():
            for copy in corner_copies((NW, NE)):
                copy.start()

        def fold_corners():
            @pl.when(top & (fold_e != gx))
            def _():
                fold_ne().start()

            @pl.when(top & (fold_e == gx))
            def _():
                self_ne().start()

            @pl.when(top & (fold_w != gx))
            def _():
                fold_nw().start()

            @pl.when(top & (fold_w == gx))
            def _():
                self_nw().start()

        def fold_rows():
            @pl.when(top)
            def _():
                fold_n().start()

        if late is None:
            fold_corners()
        if turn != 1:
            for copy in side_copies():
                copy.start()
        if middle is not None:
            middle()
        if late is None:
            fold_rows()

        @pl.when(not_top)
        def _():
            north_copy().start()

        @pl.when(not_bottom)
        def _():
            south_copy().start()

        if late is not None:
            pl.when(top)(late)
            fold_corners()
            fold_rows()

        def finish_sides():
            for copy in side_copies():
                copy.wait_recv()

            @pl.when(not_bottom)
            def _():
                for copy in corner_copies((SW, SE)):
                    copy.wait_recv()

            @pl.when(not_top)
            def _():
                for copy in corner_copies((NW, NE)):
                    copy.wait_recv()

            @pl.when(top & (fold_e != gx))
            def _():
                fold_ne().wait_recv()

            @pl.when(top & (fold_e == gx))
            def _():
                self_ne().wait()

            @pl.when(top & (fold_w != gx))
            def _():
                fold_nw().wait_recv()

            @pl.when(top & (fold_w == gx))
            def _():
                self_nw().wait()

        def finish_rows():
            @pl.when(not_bottom)
            def _():
                north_copy().wait_recv()

            @pl.when(not_top)
            def _():
                south_copy().wait_recv()

            @pl.when(top)
            def _():
                fold_n().wait_recv()

        def finish_send():
            for copy in side_copies():
                copy.wait_send()

            @pl.when(not_top)
            def _():
                for copy in north_copies():
                    copy.wait_send()

            @pl.when(not_bottom)
            def _():
                for copy in south_copies():
                    copy.wait_send()

            @pl.when(top)
            def _():
                fold_n().wait_send()

            @pl.when(top & (fold_e != gx))
            def _():
                fold_ne().wait_send()

            @pl.when(top & (fold_w != gx))
            def _():
                fold_nw().wait_send()

        return finish_sides, finish_rows, finish_send

    as_int = lambda flag: flag.astype(jnp.int32)
    peers = 2 + 3 * as_int(not_top) + 3 * as_int(not_bottom) + as_int(top)
    peers = peers + as_int(top & (fold_e != gx)) + as_int(top & (fold_w != gx))
    with jax.named_scope("barrier"):
        pl.semaphore_wait(barrier, peers)

    finish_sides, finish_rows, finish_send = exchange(
        0,
        None,
        None,
        send_sem,
        recv_sem,
        (raw.at[:, 64:80], raw.at[:, 0:16]),
        bundle_e,
        bundle_w,
        tuple(corner_out.at[i] for i in range(4)),
        (rev_n, rev_c.at[0], rev_c.at[1]),
        {
            N: raw.at[:, NORTH],
            S: raw.at[:, SOUTH],
            E: got_e,
            W: got_w,
            NE: got_c.at[0],
            NW: got_c.at[1],
            SE: got_c.at[2],
            SW: got_c.at[3],
        },
    )
    tell(0, 1)
    for i in range(3):
        goal[i] = jnp.transpose(target[i])
    with jax.named_scope("recv_first"):
        finish_sides()
    hear(0, 1)
    tell(1, 2)

    centre = slice(FIRST, LAST)
    low = slice(PAD, FIRST)
    high = slice(LAST, LAST + HALO)

    def side(bundle, upper, lower):
        packed = [bundle[0:ROWS], upper[0:HALO], zero_gap, lower[0:HALO]]
        packed = jnp.transpose(jnp.concatenate(packed, axis=0))
        upper, lower = [
            jnp.concatenate([x[HALO:], pltpu.roll(x[HALO:], HALO, 1)], axis=0)
            for x in (upper, lower)
        ]
        strip = jnp.where(lane16 < 96, upper, jnp.where(lane16 >= 112, lower, 0.0))
        strip = jnp.where(lane16 < ROWS, bundle[ROWS:], strip)
        return [packed[HALO * f : HALO * (f + 1)] for f in range(8)] + [strip]

    def place(rows, parts):
        u, v, s1, s2, s12, wu, wv, strong, b = parts
        field[0, rows] = u
        field[1, rows] = v
        field[2, rows] = s1 + s2
        field[3, rows] = s1 - s2
        field[4, rows] = 2.0 * s12
        static[0, rows] = jnp.where(b > 0.0, 1.0, 0.0) - b
        static[1, rows] = 0.25 * b
        static[2, rows] = b * wu
        static[3, rows] = b * wv
        static[4, rows] = strong

    place(low, side(got_w, got_c.at[1], got_c.at[3]))
    place(high, side(got_e, got_c.at[0], got_c.at[2]))
    with jax.named_scope("recv_rows"):
        finish_rows()
    place(centre, [jnp.transpose(raw[f]) for f in range(9)])

    begin = start_ref[0].astype(F32)

    def coefs(k):
        step = jnp.full((CHUNK, LANES), begin + jnp.asarray(k + 1, jnp.int32).astype(F32), F32)
        coef = 0.2 + 0.8 * step / SUBTOTAL
        keep = 1.0 / (1.0 + coef)
        return coef, keep

    to_n = lambda x: pltpu.roll(x, LANES - 1, 1)
    to_s = lambda x: pltpu.roll(x, 1, 1)
    wide = range(PAD, TALL - PAD, CHUNK)
    narrow = range(PAD + 8, TALL - PAD - 8, CHUNK)

    def forward(chunks, k, carry):
        coef, keep = coefs(k)
        gain = coef * keep
        for r in chunks:
            rows = slice(r, r + CHUNK)
            up = slice(r + 1, r + 1 + CHUNK)
            down = slice(r - 1, r - 1 + CHUNK)
            u = field[0, rows]
            v = field[1, rows]
            x1 = field[0, up] - field[0, down]
            x2 = field[1, up] - field[1, down]
            y1 = to_n(u) - to_s(u)
            y2 = to_n(v) - to_s(v)
            div = x1 + y2
            ten = x1 - y2
            quarter = 0.25 * ten
            half = 0.5 * (y1 + x2)
            inv = lax.rsqrt(div * div + quarter * ten + half * half + 0.16)
            rate = gain * static[4, rows]
            un = (div + quarter) * inv
            vn = (div - quarter) * inv
            sn = half * inv
            saved[k, 0, rows] = un
            saved[k, 1, rows] = vn
            saved[k, 2, rows] = sn
            saved[k, 3, rows] = rate * inv
            field[2, rows] = keep * field[2, rows] + rate * (un - 1.0)
            field[3, rows] = keep * field[3, rows] + rate * (vn - 1.0)
            field[4, rows] = keep * field[4, rows] + rate * sn
        for r in chunks:
            rows = slice(r, r + CHUNK)
            up = slice(r + 1, r + 1 + CHUNK)
            down = slice(r - 1, r - 1 + CHUNK)
            m = field[3, rows]
            q = field[4, rows]
            fx = (field[2, up] - field[2, down]) + (to_n(q) - to_s(q))
            fy = (field[4, up] - field[4, down]) + (to_n(m) - to_s(m))
            field[0, rows] = static[0, rows] * field[0, rows] + (static[2, rows] + static[1, rows] * fx)
            field[1, rows] = static[0, rows] * field[1, rows] + (static[3, rows] + static[1, rows] * fy)
        return carry

    with jax.named_scope("forward"):
        lax.fori_loop(0, STEPS // 2, functools.partial(forward, wide), 0, unroll=4)
        lax.fori_loop(STEPS // 2, STEPS, functools.partial(forward, narrow), 0, unroll=4)

    for i in range(2):
        miss = goal[0] * (field[i, centre] - goal[1 + i])
        back[i, centre] = miss
        back[2 + i, centre] = static[1, centre] * miss

    def backward(chunks, last, i, carry):
        k = STEPS - 1 - i
        _, keep = coefs(k)
        for r in chunks:
            rows = slice(r, r + CHUNK)
            up = slice(r + 1, r + 1 + CHUNK)
            down = slice(r - 1, r - 1 + CHUNK)
            mu = back[2, rows]
            mv = back[3, rows]
            tp = back[4, rows] + (back[2, down] - back[2, up])
            tm = back[5, rows] + (to_s(mv) - to_n(mv))
            tq = back[6, rows] + ((to_s(mu) - to_n(mu)) + (back[3, down] - back[3, up]))
            un = saved[k, 0, rows]
            vn = saved[k, 1, rows]
            sn = saved[k, 2, rows]
            g = saved[k, 3, rows]
            along = tp * un + tm * vn + tq * sn
            total = tp + tm
            quarter = 0.25 * (tp - tm)
            back[7, rows] = g * ((total + quarter) - along * un)
            back[8, rows] = g * ((total - quarter) - along * vn)
            back[9, rows] = (0.5 * g) * (tq - along * sn)
            back[4, rows] = keep * tp
            back[5, rows] = keep * tm
            back[6, rows] = keep * tq
        for r in chunks:
            rows = slice(r, r + CHUNK)
            up = slice(r + 1, r + 1 + CHUNK)
            down = slice(r - 1, r - 1 + CHUNK)
            yb = back[8, rows]
            sb = back[9, rows]
            lu = back[0, rows]
            lv = back[1, rows]
            if not last:
                back[10, rows] = back[10, rows] + lu
                back[11, rows] = back[11, rows] + lv
            new_u = static[0, rows] * lu + ((back[7, down] - back[7, up]) + (to_s(sb) - to_n(sb)))
            new_v = static[0, rows] * lv + ((back[9, down] - back[9, up]) + (to_s(yb) - to_n(yb)))
            back[0, rows] = new_u
            back[1, rows] = new_v
            if not last:
                back[2, rows] = static[1, rows] * new_u
                back[3, rows] = static[1, rows] * new_v
        return carry

    with jax.named_scope("backward"):
        lax.fori_loop(0, STEPS // 2, functools.partial(backward, narrow, False), 0, unroll=4)
        lax.fori_loop(STEPS // 2, STEPS - 1, functools.partial(backward, wide, False), 0, unroll=3)

    def four_tiles(u0, u1, v0, v1):
        other = two_tiles(pltpu.roll(v0, 64, 1), pltpu.roll(v1, 64, 1))
        return jnp.where(lane8 >= 64, two_tiles(u0, u1), other)

    lane_all = lax.broadcasted_iota(jnp.int32, (LANES, LANES), 1)
    def gusts(rows):
        for i in range(2):
            gust[i, rows] = 4.0 * static[1, rows] * (back[10 + i, rows] + back[i, rows])

    with jax.named_scope("wind_pack"):
        gusts(high)
        gusts(low)
        for j, rows in ((0, high), (1, low)):
            u, v = gust[0, rows], gust[1, rows]
            gust_c[j] = four_tiles(u[0:8], u[8:16], v[0:8], v[8:16])

    def wind_rows():
        gusts(centre)
        here = ((lane_all >= 80) & (lane_all < 96)) | (lane_all >= 112)
        both = jnp.where(here, gust[0, centre], pltpu.roll(gust[1, centre], LANES - HALO, 1))
        gust_ns[...] = jnp.transpose(both)[64:LANES]

    def flip_index(shift):
        return lax.rem(2 * LANES - 1 + shift - lane8, LANES)

    def flip_wind():
        for i in range(2):
            part = slice(HALO * i, HALO * (i + 1))
            upper, lower = flip_strip(gust_ns[part], whole_flip, -1.0)
            rev_n_w[16 * i : 16 * i + 8] = upper
            rev_n_w[16 * i + 8 : 16 * i + 16] = lower
        row_flip = 7 - lax.broadcasted_iota(jnp.int32, (8, LANES), 0)
        for j, rows in ((0, high), (1, low)):
            tiles = []
            for i, shifts in ((0, (80, 64)), (1, (16, 0))):
                strip = gust[i, rows]
                for part, shift in zip((strip[8:16], strip[0:8]), shifts):
                    part = jnp.take_along_axis(part, row_flip, axis=0)
                    tiles.append(-flip_lanes(part, flip_index(shift)))
            pairs = [jnp.where(odd, tiles[2 * i], tiles[2 * i + 1]) for i in range(2)]
            rev_c_w[j] = jnp.where(lane8 >= 64, pairs[0], pairs[1])

    finish_wind_sides, finish_wind_rows, finish_wind_send = exchange(
        1,
        wind_rows,
        flip_wind,
        wsend_sem,
        wrecv_sem,
        (gust_ns.at[0:32], gust_ns.at[32:64]),
        gust.at[:, high],
        gust.at[:, low],
        (gust_c.at[0], gust_c.at[1], gust_c.at[0], gust_c.at[1]),
        (rev_n_w, rev_c_w.at[0], rev_c_w.at[1]),
        {
            N: got_n_w,
            S: got_s_w,
            E: got_e_w,
            W: got_w_w,
            NE: got_c_w.at[0],
            NW: got_c_w.at[1],
            SE: got_c_w.at[2],
            SW: got_c_w.at[3],
        },
    )
    with jax.named_scope("backward_last"):
        backward(wide, True, STEPS - 1, 0)
    hear(1, 2)
    tell(2, 4)
    finish_send()

    def result(rows):
        p = back[4, rows]
        m = back[5, rows]
        return [back[0, rows], back[1, rows], p + m, p - m, 2.0 * back[6, rows]]

    with jax.named_scope("state_pack"):
        for f, value in enumerate(result(centre)):
            fin[f] = jnp.transpose(value)
        for rows, dst in ((high, fin_e), (low, fin_w)):
            dst[...] = jnp.transpose(jnp.concatenate(result(rows) + [spare_rows], axis=0))

        @pl.when(top)
        def _():
            for f in range(5):
                rev_n[f, 0:8], rev_n[f, 8:16] = flip_strip(fin[f, NORTH], whole_flip, SIGNS[f])
            for i, src in ((0, fin_e), (1, fin_w)):
                rev_c[i, 0:8], rev_c[i, 8:16] = flip_strip(src[NORTH], group_flip, group_sign)

    with jax.named_scope("recv_wind"):
        finish_wind_sides()

    def with_sides(i):
        value = gust[i, centre]

        def ends(straight, upper, lower):
            extra = jnp.where(lane16 < ROWS, straight[i], 0.0)
            place = 64 * i
            upper = [pltpu.roll(upper[...], (80 - place + LANES + 16 * t) % LANES, 1) for t in (0, 1)]
            lower = [pltpu.roll(lower[...], (48 + place + 16 * t) % LANES, 1) for t in (0, 1)]
            upper, lower = jnp.concatenate(upper, axis=0), jnp.concatenate(lower, axis=0)
            extra = extra + jnp.where((lane16 >= 64) & (lane16 < ROWS), upper, 0.0)
            return extra + jnp.where(lane16 < HALO, lower, 0.0)

        at_w = ends(got_w_w, got_c_w.at[1], got_c_w.at[3])
        at_e = ends(got_e_w, got_c_w.at[0], got_c_w.at[2])
        parts = [value[:HALO] + at_w, value[HALO:-HALO], value[-HALO:] + at_e]
        return jnp.transpose(jnp.concatenate(parts, axis=0))[0:ROWS]

    with jax.named_scope("wind_add"):
        for i in range(2):
            wind_out[i] = with_sides(i)
    with jax.named_scope("recv_wind_rows"):
        finish_wind_rows()
    with jax.named_scope("squares"):
        for i in range(2):
            rows = slice(HALO * (1 - i), HALO * (2 - i))
            wind_out[i, 0:16] = wind_out[i, 0:16] + got_s_w[rows]
            wind_out[i, 64:80] = wind_out[i, 64:80] + got_n_w[rows]
        squares = wind_out[0] * wind_out[0] + wind_out[1] * wind_out[1]
        part = jnp.sum(squares, axis=0, keepdims=True)

    layer, odd_x = lax.div(gy, 2), lax.rem(gy, 2)
    layers = ny // 2
    by_ring = [wrap(ring + r, rings) * (4 * ny) for r in range(rings)]
    by_cross = [cross * (2 * ny), (1 - cross) * (2 * ny)]
    by_core = [core * ny, (1 - core) * ny]
    by_layer = [wrap(layer + z, layers) * 2 for z in range(layers)]
    by_odd = [odd_x, 1 - odd_x]
    slow = {(r, c): by_ring[r] + by_cross[c] for r in range(rings) for c in range(2)}
    fast = {
        (k, z, o): by_core[k] + (by_layer[z] + by_odd[o])
        for k in range(2)
        for z in range(layers)
        for o in range(2)
    }
    steps = sorted(
        (-(min(r, rings - r) + min(z, layers - z) + (1 if o else 2 * c)), r, c, k, z, o)
        for r, c in slow
        for k, z, o in fast
    )
    others = [step[1:] for step in steps if any(step[1:])]

    def sum_copies():
        return [
            pltpu.make_async_remote_copy(
                src_ref=red.at[pl.ds(me, 1)],
                dst_ref=red.at[pl.ds(me, 1)],
                send_sem=sum_sem.at[0],
                recv_sem=sum_sem.at[1],
                device_id=slow[r, c] + fast[k, z, o],
                device_id_type=pl.DeviceIdType.LOGICAL,
            )
            for r, c, k, z, o in others
        ]

    def end_sum():
        most = red.at[0 : everyone - 1]
        pltpu.make_async_copy(most, most, sum_sem.at[1]).wait()
        pltpu.make_async_copy(most, most, sum_sem.at[0]).wait()
        return jnp.sum(red[...], axis=0, keepdims=True)

    hear(2, 4)
    red[pl.ds(me, 1)] = part
    with jax.named_scope("sum_start"):
        for copy in sum_copies():
            copy.start()
    finish_state_sides, finish_state_rows, finish_state_send = exchange(
        2,
        None,
        None,
        fsend_sem,
        frecv_sem,
        (fin.at[:, NORTH], fin.at[:, SOUTH]),
        fin_e.at[0:ROWS],
        fin_w.at[0:ROWS],
        (fin_e.at[NORTH], fin_w.at[NORTH], fin_e.at[SOUTH], fin_w.at[SOUTH]),
        (rev_n.at[0:5], rev_c.at[0, 0:HALO], rev_c.at[1, 0:HALO]),
        {
            N: got_n_f,
            S: got_s_f,
            E: got_e_f,
            W: got_w_f,
            NE: got_c_f.at[0],
            NW: got_c_f.at[1],
            SE: got_c_f.at[2],
            SW: got_c_f.at[3],
        },
    )
    with jax.named_scope("recv_state"):
        finish_state_sides()
        finish_state_rows()
    with jax.named_scope("state_add"):
        got_e_f[64:80] = got_e_f[64:80] + got_c_f[0]
        got_w_f[64:80] = got_w_f[64:80] + got_c_f[1]
        got_e_f[0:16] = got_e_f[0:16] + got_c_f[2]
        got_w_f[0:16] = got_w_f[0:16] + got_c_f[3]
        packed_e = got_e_f[...]
        packed_w = got_w_f[...]
        for f in range(5):
            side_e = pltpu.roll(packed_e, LANES - HALO - HALO * f, 1)
            side_w = packed_w if f == 0 else pltpu.roll(packed_w, LANES - HALO * f, 1)
            value = fin[f, 0:ROWS]
            value = value + jnp.where(lane >= LANES - HALO, side_e, 0.0)
            value = value + jnp.where(lane < HALO, side_w, 0.0)
            state_out[f] = value
            state_out[f, 0:16] = state_out[f, 0:16] + got_s_f[f]
            state_out[f, 64:80] = state_out[f, 64:80] + got_n_f[f]
    finish_wind_send()
    finish_state_send()
    with jax.named_scope("sum_all"):
        part = end_sum()
    total = jnp.sum(jnp.broadcast_to(part, (8, LANES)), axis=1, keepdims=True)[0:1]
    entries = 2 * ROWS * LANES * nx * ny
    inv = lax.rsqrt(total / entries + NORM_EPS)
    for i in range(2):
        wind_out[i] = wind_out[i] * inv


def writer(state, wind, state_hbm, wind_hbm, sem):
    pieces = [(state, state_hbm, f) for f in range(5)] + [(wind, wind_hbm, f) for f in range(2)]
    copies = [
        pltpu.make_async_copy(src.at[f], dst.at[f], sem.at[i])
        for i, (src, dst, f) in enumerate(pieces)
    ]
    for copy in copies:
        copy.start()
    for copy in copies:
        copy.wait()


def solution(mesh):
    nx, ny = mesh.shape["gx"], mesh.shape["gy"]

    def per_device(velocity, stress, wind, strength, mass, land, region, observed, start):
        vm = lambda *shape: pltpu.VMEM(shape, F32)
        dma = pltpu.SemaphoreType.DMA
        any_spec = pl.BlockSpec(memory_space=pl.ANY)
        args = (start, velocity, stress, wind, strength, mass, land, region, observed)
        args = [args[0]] + [pltpu.with_memory_space_constraint(z, pltpu.HBM) for z in args[1:]]
        shapes = (
            jax.ShapeDtypeStruct((5, ROWS, LANES), F32),
            jax.ShapeDtypeStruct((2, ROWS, LANES), F32),
        )
        vmem_spec = pl.BlockSpec(memory_space=pltpu.VMEM)
        state, gusts = pl.pallas_call(
            functools.partial(kernel, nx, ny),
            out_shape=shapes,
            in_specs=[pl.BlockSpec(memory_space=pltpu.SMEM)] + [any_spec] * 8,
            out_specs=(vmem_spec, vmem_spec),
            scratch_shapes=[
                vm(9, LANES, LANES),
                vm(ROWS, LANES),
                pltpu.VMEM((ROWS, LANES), jnp.int32),
                pltpu.VMEM((ROWS, LANES), jnp.int32),
                vm(3, LANES, LANES),
                vm(3, LANES, LANES),
                vm(ROWS + HALO, LANES),
                vm(ROWS + HALO, LANES),
                vm(4, HALO + 8, LANES),
                vm(ROWS + HALO, LANES),
                vm(ROWS + HALO, LANES),
                vm(4, HALO + 8, LANES),
                vm(9, HALO, LANES),
                vm(2, HALO + 8, LANES),
                vm(5, TALL, LANES),
                vm(5, TALL, LANES),
                vm(STEPS, 4, TALL, LANES),
                vm(12, TALL, LANES),
                vm(5, LANES, LANES),
                vm(LANES, LANES),
                vm(LANES, LANES),
                vm(5, HALO, LANES),
                vm(5, HALO, LANES),
                vm(ROWS, LANES),
                vm(ROWS, LANES),
                vm(4, HALO, LANES),
                vm(2, TALL, LANES),
                vm(64, LANES),
                vm(2, 8, LANES),
                vm(2 * HALO, LANES),
                vm(2 * HALO, LANES),
                vm(2, HALO, LANES),
                vm(2, HALO, LANES),
                vm(4, 8, LANES),
                vm(2 * HALO, LANES),
                vm(2, 8, LANES),
                vm(nx * ny, LANES),
                dma((9,)),
                dma((8,)),
                dma((8,)),
                dma((8,)),
                dma((8,)),
                dma((8,)),
                dma((8,)),
                dma((6,)),
                dma((2,)),
                pltpu.SemaphoreType.REGULAR((3,)),
            ],
            compiler_params=pltpu.CompilerParams(
                collective_id=0, has_side_effects=True, vmem_limit_bytes=32 * 1024 * 1024
            ),
        )(*args)
        return pl.pallas_call(
            writer,
            out_shape=shapes,
            in_specs=[vmem_spec, vmem_spec],
            out_specs=(any_spec, any_spec),
            scratch_shapes=[dma((7,))],
        )(
            pltpu.with_memory_space_constraint(state, pltpu.VMEM),
            pltpu.with_memory_space_constraint(gusts, pltpu.VMEM),
        )

    tri, two = P(None, "gy", "gx"), P("gy", "gx")
    return jax.shard_map(
        per_device,
        mesh=mesh,
        in_specs=(tri, tri, tri, two, two, two, two, tri, P()),
        out_specs=(tri, tri),
        check_vma=False,
    )
```
